16 devices in a mesh: dp: 2 (over y, z), tp: 8 (over x, core).
Axes of the slice: x: 4, y: 2, z: 1, core: 2. Of those that a mesh axis runs over, the one named last changes fastest.
The devices are a block of a 4x4x8 slice.
Arguments:
- x: bfloat16 [2, 2048, 4096], P('dp', 'tp'), parts along dimension 0
- dy: bfloat16 [2, 2048, 4096], P('dp', 'tp'), parts along dimension 0
- wq: bfloat16 [4096, 4096], P(None, 'tp')
- wk: bfloat16 [4096, 1024], P(None, 'tp')
- wv: bfloat16 [4096, 1024], P(None, 'tp')
- wo: bfloat16 [4096, 4096], P('tp')
- w_gate: bfloat16 [4096, 12288], P(None, 'tp')
- w_up: bfloat16 [4096, 12288], P(None, 'tp')
- w_down: bfloat16 [12288, 4096], P('tp')
Outputs:
- output 1: bfloat16 [2, 2048, 4096], P('dp', 'tp'), parts along dimension 0
- output 2: bfloat16 [8192, 4096], P('dp', 'tp'), parts along dimension 0
- output 3: bfloat16 [8192, 1024], P('dp', 'tp'), parts along dimension 0
- output 4: bfloat16 [8192, 1024], P('dp', 'tp'), parts along dimension 0
- output 5: bfloat16 [8192, 4096], P(('dp', 'tp')), parts along dimension 0
- output 6: bfloat16 [8192, 12288], P('dp', 'tp'), parts along dimension 0
- output 7: bfloat16 [8192, 12288], P('dp', 'tp'), parts along dimension 0
- output 8: bfloat16 [24576, 4096], P(('dp', 'tp')), parts along dimension 0
There are 2 independent parts. The reference program is written for one: setup_inputs(seed, part) draws one part's arguments, and reference() takes and returns one part's arrays. A program takes and returns all parts, laid end to end along the dimension named above; an argument that names none is the same for every part.
All inputs are finite; a program needn't handle non-finite values.
Results may differ from the reference program's by a relative error of at most 0.024.
Values are sent between devices in bfloat16 or wider.
A program may use at most 768 MiB of HBM per device.

```python
import jax
import jax.numpy as jnp
from jax import lax

SEQUENCES = 1
TOKENS = 2048
D = 4096
HEADS = 32
KV_HEADS = 8
HEAD = 128
FF = 12288
THETA = 10000
NAMES = ("wq", "wk", "wv", "wo", "w_gate", "w_up", "w_down")
SHAPES = {
    "wq": (D, HEADS * HEAD),
    "wk": (D, KV_HEADS * HEAD),
    "wv": (D, KV_HEADS * HEAD),
    "wo": (HEADS * HEAD, D),
    "w_gate": (D, FF),
    "w_up": (D, FF),
    "w_down": (FF, D),
}


def bump(key, n, height):
    away = (jnp.arange(n, dtype=jnp.int32) - jax.random.randint(key, (), 0, n, jnp.int32)) % n
    return jnp.where(away < n // 8, height, 1.0)


def together(key, own, strength):
    shared = jax.random.normal(key, own.shape[1:], jnp.float32)
    return (own + strength * shared) * lax.rsqrt(1 + strength * strength)


def setup_inputs(seed: int = 0, part: int = 0) -> dict:
    kx, kdy, ka, kb, kz, kf, kh, kl, *kw = jax.random.split(jax.random.key(seed), 8 + len(NAMES))
    kx, kdy, ka, kb = (jax.random.fold_in(k, part) for k in (kx, kdy, ka, kb))
    shape = (SEQUENCES, TOKENS, D)
    much_x, much_dy = jax.random.uniform(kz, (2,), jnp.float32, 0.0, 1.0)
    loud = 2.0 ** jax.random.uniform(jax.random.fold_in(kz, 1), (), jnp.float32, -1.0, 2.0)
    halves = 2.0 ** jax.random.uniform(kl, (2,), jnp.float32, -1.0, 1.0)
    times = {"wq": 1.0, "wk": 1.0, "wv": 2.0, "wo": halves[0], "w_gate": 1.0, "w_up": bump(kh, FF, 4.0), "w_down": halves[1]}
    x = together(ka, jax.random.normal(kx, shape, jnp.float32), much_x) * bump(kf, D, 4.0)
    dy = together(kb, jax.random.normal(kdy, shape, jnp.float32), much_dy)
    drawn = {"x": x.astype(jnp.bfloat16), "dy": (loud * dy * (SEQUENCES * TOKENS) ** -0.5).astype(jnp.bfloat16)}
    for key, name in zip(kw, NAMES, strict=True):
        drawn[name] = (jax.random.normal(key, SHAPES[name], jnp.float32) * SHAPES[name][0] ** -0.5 * times[name]).astype(jnp.bfloat16)
    return drawn


def matmul(a, w):
    return jnp.dot(a, w, preferred_element_type=jnp.float32).astype(jnp.bfloat16)


def normed(h):
    wide = h.astype(jnp.float32)
    scale = lax.rsqrt(jnp.mean(wide**2, -1, keepdims=True) + 1e-6)
    return (wide * scale).astype(jnp.bfloat16)


def turned(t, theta):
    half = t.shape[-1] // 2
    angle = jnp.arange(t.shape[0], dtype=jnp.float32)[:, None] * theta ** (-jnp.arange(half, dtype=jnp.float32) / half)
    cos, sin = jnp.cos(angle)[:, None], jnp.sin(angle)[:, None]
    a, b = t[..., :half].astype(jnp.float32), t[..., half:].astype(jnp.float32)
    return jnp.concatenate([a * cos - b * sin, b * cos + a * sin], -1).astype(jnp.bfloat16)


def seen_by(q, k, v):
    tokens, kv = q.shape[0], k.shape[1]
    q = q.reshape(tokens, kv, -1, q.shape[-1])
    scores = jnp.einsum("tgsd,ugd->gstu", q.astype(jnp.float32), k.astype(jnp.float32)) * q.shape[-1] ** -0.5
    place = jnp.arange(tokens)
    weights = jax.nn.softmax(jnp.where(place[:, None] >= place, scores, -jnp.inf), -1).astype(jnp.bfloat16)
    return jnp.einsum("gstu,ugd->tgsd", weights.astype(jnp.float32), v.astype(jnp.float32)).astype(jnp.bfloat16).reshape(tokens, -1)


def layer(h, w):
    a = normed(h)
    q, k = (turned(matmul(a, w[name]).reshape(h.shape[0], -1, HEAD), THETA) for name in ("wq", "wk"))
    h = h + matmul(seen_by(q, k, matmul(a, w["wv"]).reshape(h.shape[0], -1, HEAD)), w["wo"])
    b = normed(h)
    gate = jnp.dot(b, w["w_gate"], preferred_element_type=jnp.float32)
    up = jnp.dot(b, w["w_up"], preferred_element_type=jnp.float32)
    return h + matmul((jax.nn.silu(gate) * up).astype(jnp.bfloat16), w["w_down"])


def reference(x, dy, wq, wk, wv, wo, w_gate, w_up, w_down):
    weights = dict(zip(NAMES, (wq, wk, wv, wo, w_gate, w_up, w_down), strict=True))

    def take(so_far, sequence):
        h, by_y = sequence
        _, back = jax.vjp(lambda w, h: layer(h, w), weights, h)
        by_weights, by_h = back(by_y)
        return jax.tree.map(lambda total, term: total + term.astype(jnp.float32), so_far, by_weights), by_h

    none_yet = {name: jnp.zeros(w.shape, jnp.float32) for name, w in weights.items()}
    by_weights, by_x = lax.scan(take, none_yet, (x, dy))
    return (by_x, *(by_weights[name].astype(jnp.bfloat16) for name in NAMES))
```

```python
import functools

import jax
import jax.numpy as jnp
from jax import lax
from jax.experimental import pallas as pl
from jax.experimental.pallas import tpu as pltpu
from jax.sharding import PartitionSpec as P

BF, F32 = jnp.bfloat16, jnp.float32
HEAD = 128
THETA = 10000
NEG = -1e30
HIDDEN = 2 * NEG
LOG2E = 1.4426950408889634
SCALE = HEAD**-0.5
MOST = 67_000_000
BQ, BK, STRIP = 512, 512, 512
NN, NT, TN = ((((a,), (b,)), ((), ())) for a, b in ((1, 0), (1, 1), (0, 0)))
ANY = pl.BlockSpec(memory_space=pl.ANY)
S, V, DMA = jax.ShapeDtypeStruct, pltpu.VMEM, pltpu.SemaphoreType.DMA

RA, RB, RC, RD, RE, LA, LB, LC, LD, LE, MA, MB, MC, MD, ME, MF, MG = GATHER = range(17)
R1, R2, R3, L1, L2, L3, M0, M1, M2, M3, M4, M5 = SCATTER = range(17, 29)
COPIES = 29


def dot(a, b, dims=NN, **kw):
    return lax.dot_general(a, b, dims, preferred_element_type=F32, **kw)


def norm_scale(wide):
    return lax.rsqrt(jnp.mean(wide * wide, -1, keepdims=True) + 1e-6)


def unnorm(wide, d):
    scale = norm_scale(wide)
    return d * scale - wide * (scale * scale * scale * jnp.mean(d * wide, -1, keepdims=True))


def turn(t, cos, sin):
    return t * cos + pltpu.roll(t, HEAD // 2, 1) * sin


def angles(tokens):
    half = HEAD // 2
    a = jnp.arange(tokens, dtype=F32)[:, None] * THETA ** (-jnp.arange(half, dtype=F32) / half)
    cos, sin = jnp.cos(a), jnp.sin(a)
    return jnp.concatenate([cos, cos], -1), jnp.concatenate([-sin, sin], -1)


class Ring:
    def __init__(self, n):
        self.me = lax.axis_index("tp")
        core, chips = lax.rem(self.me, 2), n // 2
        chip = [lax.rem(lax.div(self.me, 2) + k, chips) for k in range(chips)]
        self.next, self.opp, self.prev = [2 * c + core for c in chip[1:]]
        self.mate, self.nextm, self.oppm, self.prevm = [2 * c + 1 - core for c in chip]

    def barrier(self):
        b = pltpu.get_barrier_semaphore()
        near = (self.next, self.prev, self.mate)
        for d in near:
            pl.semaphore_signal(b, inc=1, device_id={"tp": d}, device_id_type=pl.DeviceIdType.MESH)
        pl.semaphore_wait(b, len(near))


class Links:
    def __init__(self, ss, rs):
        self.ss, self.rs, self.made = ss, rs, {}

    def put(self, k, src, dst, dev):
        self.made[k] = lambda: pltpu.make_async_remote_copy(src_ref=src, dst_ref=dst, send_sem=self.ss.at[k], recv_sem=self.rs.at[k],
                                                            device_id={"tp": dev}, device_id_type=pl.DeviceIdType.MESH)

    def start(self, *ks):
        for k in ks:
            self.made[k]().start()

    def got(self, *ks):
        for k in ks:
            self.made[k]().wait_recv()

    def sent(self, *ks):
        for k in ks:
            self.made[k]().wait_send()

    def passed_on(self, *ks):
        for k in ks:
            self.got(k)
            self.start(k + 2)


def begin(copies):
    for c in copies:
        c.start()


def end(copies):
    for c in copies:
        c.wait()


def pick(u, values):
    out = values[0]
    for k, v in enumerate(values):
        out = jnp.where(u == k, v, out)
    return out


def steps(u, events):
    for k, f in events.items():
        pl.when(u == k)(f)


def chunked(size, width, f):
    lax.fori_loop(0, size // width, lambda j, _: f(pl.ds(pl.multiple_of(j * width, width), width)), None)


def gather_copies(links, ring, src, dst, T):
    H, Q = T // 2, T // 4
    me, nx, pv, mt, opp = ring.me, ring.next, ring.prev, ring.mate, ring.opp
    for k, slot, a, rows, to in ((RA, me, 0, Q, nx), (RB, me, Q, Q, nx), (RC, pv, 0, Q, nx), (RD, pv, Q, Q, nx), (RE, me, H, H, nx),
                                 (LA, me, H, Q, pv), (LB, me, H + Q, Q, pv), (LC, nx, H, Q, pv), (LD, nx, H + Q, Q, pv), (LE, me, 0, H, pv),
                                 (MA, me, 0, T, mt), (MB, pv, 0, H, mt), (MC, nx, H, H, mt), (MD, opp, 0, H, mt), (ME, opp, H, H, mt),
                                 (MF, pv, H, H, mt), (MG, nx, 0, H, mt)):
        at = pl.ds(a, rows)
        links.put(k, src.at[at] if slot is me else dst.at[slot, at], dst.at[slot, at], to)


def whole(shard):
    return (shard, 0), (shard, 1)


def moves(u, units, far, near, sem, back=False):
    H = near.shape[0] // 2
    out = []
    for k in range(2):
        shard, half = (pick(u, [x[k][m] for x in units]) for m in range(2))
        ends = far.at[shard, pl.ds(pl.multiple_of(half * H, H), H)], near.at[pl.ds(k * H, H)]
        out.append(pltpu.make_async_copy(*(ends[::-1] if back else ends), sem.at[k]))
    return out


def rows_of_unit(u, units, k, H):
    shard, half = (pick(u, [x[k][m] for x in units]) for m in range(2))
    return pl.ds(pl.multiple_of((2 * shard + half) * H, H), H)


def stream(ring, links, src, tile, sin, dst, out, sout, work, events):
    units = [whole(ring.me), whole(ring.mate), ((ring.prev, 0), (ring.next, 1)), ((ring.prevm, 0), (ring.nextm, 1)), whole(ring.opp),
             whole(ring.oppm), ((ring.prev, 1), (ring.next, 0)), ((ring.prevm, 1), (ring.nextm, 0))]
    fetch = lambda u, slot: moves(u, units, src, tile.at[slot], sin.at[slot])
    store = lambda u, slot: moves(u, units, dst, out.at[slot], sout.at[slot], True)
    begin(fetch(0, 0))

    def unit(u, _):
        slot = lax.rem(u, 2)
        end(fetch(u, slot))

        @pl.when(u > 1)
        def _():
            end(store(u - 2, slot))

        work(u, units, tile.at[slot], out.at[slot])
        begin(store(u, slot))
        steps(u, events)

        @pl.when(u + 1 < len(units))
        def _():
            begin(fetch(u + 1, 1 - slot))

    lax.fori_loop(0, len(units), unit, None)
    end(store(len(units) - 2, 0) + store(len(units) - 1, 1))
    links.sent(*GATHER)


def gather_events(links):
    def far():
        links.got(RC, RD)
        links.start(MD)
        links.got(LC, LD)
        links.start(ME)

    def last():
        links.got(RE)
        links.start(MF)
        links.got(LE)
        links.start(MG)

    return {0: lambda: links.got(MA), 2: lambda: links.got(MB, MC), 3: far, 4: lambda: links.got(MD, ME), 5: last, 6: lambda: links.got(MF, MG)}


def finish(links, acc, frp, frn, last):
    H = acc.shape[0] // 2

    def each(m, half, f):
        links.got(m)
        chunked(H, 16, lambda at: f(pl.ds(half + at.start, at.size)))

    def add(fr):
        def f(at):
            acc[at, :] += fr[at, :].astype(F32)
        return f

    each(R2, H, add(frp))
    each(L2, 0, add(frn))
    each(R3, 0, lambda at: last(at, acc[at, :] + frp[at, :].astype(F32)))
    each(L3, H, lambda at: last(at, acc[at, :] + frn[at, :].astype(F32)))


def call(body, args, outs, scratch, flops, name, cid=None):
    return pl.pallas_call(
        body, in_specs=[ANY] * len(args), out_specs=[ANY] * len(outs), out_shape=outs, scratch_shapes=scratch, name=name,
        compiler_params=pltpu.CompilerParams(collective_id=cid, has_side_effects=True, vmem_limit_bytes=MOST),
        cost_estimate=pl.CostEstimate(flops=flops, bytes_accessed=sum(t.size for t in args + outs), transcendentals=0),
    )(*args)


def _qkv(x_ref, wq_ref, wk_ref, wv_ref, cos_ref, sin_ref, ag, out, w, xt, an, at, ot, cos, sin, ss, rs, sb, so, sl, *, n):
    ring, links = Ring(n), Links(ss, rs)
    T = x_ref.shape[0]
    NQ, NK = wq_ref.shape[1], wk_ref.shape[1]
    turned, Q = NQ + NK, T // 4
    gather_copies(links, ring, an, ag, T)
    pairs = ((x_ref, xt), (an, ag.at[ring.me]), (cos_ref, cos), (sin_ref, sin), (wq_ref, w.at[:, pl.ds(0, NQ)]), (wk_ref, w.at[:, pl.ds(NQ, NK)]),
             (wv_ref, w.at[:, pl.ds(turned, NK)]))
    first, keep, *rest = [pltpu.make_async_copy(a, b, sl.at[k]) for k, (a, b) in enumerate(pairs)]
    begin([first, *rest])
    ring.barrier()
    first.wait()
    for q, k in ((0, RA), (2, LA), (1, RB), (3, LB)):

        def norm(at):
            at = pl.ds(q * Q + at.start, at.size)
            wide = xt[at, :].astype(F32)
            an[at, :] = (wide * norm_scale(wide)).astype(BF)
        chunked(Q, 16, norm)
        links.start(k)
    links.start(MA)
    keep.start()
    end([*rest, keep])

    def work(u, units, x, o):
        r = dot(x[...], w[...]).astype(BF)
        for k in range(2):
            rows = slice(k * T // 2, (k + 1) * T // 2)
            place = rows_of_unit(u, units, k, T // 2)
            c, s = cos[place, :], sin[place, :]
            for a in range(0, turned, HEAD):
                o[rows, a:a + HEAD] = turn(r[rows, a:a + HEAD].astype(F32), c, s).astype(BF)
            o[rows, turned:] = r[rows, turned:]

    def near():
        links.passed_on(RA, LA, RB, LB)
        links.start(RE, LE, MB, MC)

    stream(ring, links, ag, at, sb, out, ot, so, work, {1: near, **gather_events(links)})


def gather_qkv(x, wq, wk, wv, cos, sin, n, cid):
    T, D = x.shape
    N = wq.shape[1] + wk.shape[1] + wv.shape[1]
    scratch = [V((D, N), BF), V((T, D), BF), V((T, D), BF), V((2, T, D), BF), V((2, T, N), BF), V(cos.shape, F32), V(cos.shape, F32),
               DMA((COPIES,)), DMA((COPIES,)), DMA((2, 2)), DMA((2, 2)), DMA((7,))]
    return call(functools.partial(_qkv, n=n), [x, wq, wk, wv, cos, sin], [S((n, T, D), BF), S((n, T, N), BF)], scratch, 2 * n * T * D * N, "gather_qkv", cid)


def rows_of(t):
    return jnp.concatenate([t[:, a:a + HEAD] for a in range(0, t.shape[1], HEAD)], axis=0)


def set_gap(gap):
    gap[...] = lax.rem(lax.broadcasted_iota(jnp.int32, gap.shape, 1), BQ) - lax.broadcasted_iota(jnp.int32, gap.shape, 0)


def key_blocks(iq, block):
    seen = lax.div(iq * BQ + 1, BK)
    lax.fori_loop(0, seen, lambda j, _: block(j, False), None)
    lax.fori_loop(seen, lax.div((iq + 1) * BQ + BK - 1, BK), lambda j, _: block(j, True), None)


def block_rows(i, size):
    return pl.ds(pl.multiple_of(i * size, size), size)


def attend_block(iq, qkv, o_ref, lse_ref, qs, top, mix, gap):
    NQ = o_ref.shape[1]
    cols = qs.shape[0]
    mine = block_rows(iq, BQ)
    qs[...] = rows_of(qkv[mine, :NQ])
    top[...] = jnp.full_like(top, NEG)
    mix[...] = jnp.zeros_like(mix)
    ones = jnp.ones((8, BK), BF)
    strips = [slice(a, a + STRIP) for a in range(0, cols, STRIP)]

    def block(j, masked):
        here = block_rows(j, BK)
        keys = qkv[here, NQ:NQ + HEAD]
        values = jnp.concatenate([qkv[here, NQ + HEAD:].T, ones], axis=0)
        scores = [dot(keys, qs[at, :], NT) for at in strips]
        ps, keeps = [], []
        for at, s in zip(strips, scores):
            if masked:
                s = jnp.where(gap[:, at] >= j * BK - iq * BQ, s, HIDDEN)
            old = top[:, at]
            new = jnp.maximum(old, s.max(axis=0, keepdims=True))
            top[:, at] = new
            ps.append(jnp.exp2((s - new) * (SCALE * LOG2E)).astype(BF))
            keeps.append(jnp.exp2((old - new) * (SCALE * LOG2E)))
        for at, p, keep in zip(strips, ps, keeps):
            mix[:, at] = mix[:, at] * keep + dot(values, p)

    key_blocks(iq, block)
    total = mix[HEAD:HEAD + 1, :]
    out = (mix[:HEAD, :] * (1 / total)).T.astype(BF)
    for h in range(NQ // HEAD):
        o_ref[mine, h * HEAD:(h + 1) * HEAD] = out[h * BQ:(h + 1) * BQ]
    lse_ref[iq] = top[...] * SCALE + jnp.log(total)


def _attend_bwd(qkv_ref, do_ref, o_ref, lse_ref, cos_ref, sin_ref, out_ref, qs, dos, dq, dk, dv, gap):
    NQ = do_ref.shape[1]
    tokens, cols = dk.shape[0], qs.shape[0]
    iq = pl.program_id(0)
    mine = block_rows(iq, BQ)
    qs[...] = rows_of(qkv_ref[mine, :NQ])
    dos[...] = rows_of(do_ref)
    dq[...] = jnp.zeros_like(dq)

    @pl.when(iq == 0)
    def _():
        set_gap(gap)
        dk[...] = jnp.zeros_like(dk)
        dv[...] = jnp.zeros_like(dv)

    delta = dot(jnp.ones((8, HEAD), F32), dos[...].astype(F32) * rows_of(o_ref).astype(F32), NT, precision=lax.Precision.HIGHEST)[:1]
    lse = lse_ref[0] * LOG2E
    strips = [slice(a, a + STRIP) for a in range(0, cols, STRIP)]

    def block(j, masked):
        here = block_rows(j, BK)
        keys, values = qkv_ref[here, NQ:NQ + HEAD], qkv_ref[here, NQ + HEAD:]
        scores = [dot(keys, qs[at, :], NT) for at in strips]
        dps = [dot(values, dos[at, :], NT) for at in strips]
        for at, s, dp in zip(strips, scores, dps):
            p = jnp.exp2(s * (SCALE * LOG2E) - lse[:, at])
            if masked:
                p = jnp.where(gap[:, at] >= j * BK - iq * BQ, p, 0.0)
            ds = (p * (dp - delta[:, at])).astype(BF)
            dv[here, :] += dot(p.astype(BF), dos[at, :])
            dk[here, :] += dot(ds, qs[at, :])
            dq[:, at] += dot(keys.T, ds)

    key_blocks(iq, block)
    back = (dq[...] * SCALE).T
    for h in range(NQ // HEAD):
        out_ref[mine, h * HEAD:(h + 1) * HEAD] = turn(back[h * BQ:(h + 1) * BQ], cos_ref[mine, :], -sin_ref[mine, :]).astype(BF)

    @pl.when(iq == pl.num_programs(0) - 1)
    def _():
        def rest(at):
            out_ref[at, NQ:NQ + HEAD] = turn(dk[at, :] * SCALE, cos_ref[at, :], -sin_ref[at, :]).astype(BF)
            out_ref[at, NQ + HEAD:] = dv[at, :].astype(BF)
        chunked(tokens, BQ, rest)


def attend_bwd(qkv, d_out, out, lse, cos, sin):
    tokens, NQ = out.shape
    cols = lse.shape[2]
    part = pl.BlockSpec((BQ, NQ), lambda i: (i, 0))
    all_of = lambda t: pl.BlockSpec(t.shape, lambda i: (0, 0))
    return pl.pallas_call(
        _attend_bwd, grid=(tokens // BQ,), in_specs=[all_of(qkv), part, part, pl.BlockSpec((1, 1, cols), lambda i: (i, 0, 0)), all_of(cos), all_of(sin)],
        out_specs=all_of(qkv), out_shape=S(qkv.shape, BF), name="attend_bwd",
        scratch_shapes=[V((cols, HEAD), BF), V((cols, HEAD), BF), V((HEAD, cols), F32), V((tokens, HEAD), F32), V((tokens, HEAD), F32), V((BK, cols), jnp.int32)],
        compiler_params=pltpu.CompilerParams(vmem_limit_bytes=MOST),
        cost_estimate=pl.CostEstimate(flops=5 * tokens * tokens * NQ, bytes_accessed=8 * qkv.size, transcendentals=tokens * cols),
    )(qkv, d_out, out, lse, cos, sin)


def _attend_gather(qkv_ref, dy_ref, wd_ref, ag, out, o_ref, lse_ref, w, qkv, o, lse, qs, top, mix, gap, at, ot, ss, rs, sb, so, sl, *, n):
    ring, links = Ring(n), Links(ss, rs)
    T = dy_ref.shape[0]
    gather_copies(links, ring, dy_ref, ag, T)
    pairs = ((qkv_ref, qkv), (dy_ref, at.at[1]), (wd_ref, w), (at.at[1], ag.at[ring.me]), (o, o_ref), (lse, lse_ref))
    *first, weight, keep, o_out, lse_out = [pltpu.make_async_copy(a, b, sl.at[k]) for k, (a, b) in enumerate(pairs)]
    begin([*first, weight])
    ring.barrier()
    links.start(RA, LA, RB, LB, MA)
    end(first)
    keep.start()
    set_gap(gap)
    blocks = qkv.shape[0] // BQ

    def attention(iq, _):
        attend_block(iq, qkv, o, lse, qs, top, mix, gap)
        steps(iq, {blocks - 2: lambda: links.passed_on(RA, LA)})

    lax.fori_loop(0, blocks, attention, None)
    links.passed_on(RB, LB)
    links.start(RE, LE, MB, MC)
    begin([o_out, lse_out])
    end([keep, weight])

    def work(u, units, x, o):
        o[...] = dot(x[...], w[...], NT).astype(BF)

    stream(ring, links, ag, at, sb, out, ot, so, work, gather_events(links))
    end([o_out, lse_out])


def attend_gather(qkv, dy, wd, n, cid):
    T, D = dy.shape
    F = wd.shape[0]
    tokens, N = qkv.shape
    NQ = N - 2 * HEAD
    cols = NQ // HEAD * BQ
    stat = (tokens // BQ, 1, cols)
    scratch = [V((F, D), BF), V((tokens, N), BF), V((tokens, NQ), BF), V(stat, F32), V((cols, HEAD), BF), V((1, cols), F32), V((HEAD + 8, cols), F32),
               V((BK, cols), jnp.int32), V((2, T, D), BF), V((2, T, F), BF), DMA((COPIES,)), DMA((COPIES,)), DMA((2, 2)), DMA((2, 2)), DMA((6,))]
    return call(functools.partial(_attend_gather, n=n), [qkv, dy, wd], [S((n, T, D), BF), S((n, T, F), BF), S((tokens, NQ), BF), S(stat, F32)], scratch,
                2 * n * T * D * F, "attend_gather", cid)


def _product_scatter(*refs, n, forward, parts):
    t_ref, x_ref, *refs = refs
    if not forward:
        extra_ref, *refs = refs
    w_refs, (h_ref, *refs) = refs[:parts], refs[parts:]
    if forward:
        b_ref, *refs = refs
    w, t, xt, et, ht, stg, p, s, kept, acc, tr, frp, frn, ss, rs, sl, st = refs
    ring, links = Ring(n), Links(ss, rs)
    T, D = x_ref.shape
    H, NB = T // 2, D // 4
    nx, pv, mt = ring.next, ring.prev, ring.mate
    lo, hi, every = pl.ds(0, H), pl.ds(H, H), pl.ds(0, T)
    for k, src, dst, to in ((M0, stg.at[0, lo], p.at[0, lo], mt), (M1, stg.at[0, hi], p.at[0, hi], mt), (M2, stg.at[1], p.at[1], mt),
                            (M3, stg.at[2], p.at[2], mt), (M4, stg.at[3], p.at[3], mt),
                            (R1, s.at[0, lo], tr.at[0], nx), (L1, s.at[0, hi], tr.at[1], pv),
                            (R2, s.at[1, hi], frp.at[hi], nx), (L2, s.at[2, lo], frn.at[lo], pv),
                            (R3, s.at[1, lo], frp.at[lo], nx), (L3, s.at[2, hi], frn.at[hi], pv)):
        links.put(k, src, dst, to)
    at, pairs = 0, [(x_ref, xt)] if forward else [(x_ref, xt), (extra_ref, et)]
    for r in w_refs:
        pairs.append((r, w if forward else w.at[:, pl.ds(at, r.shape[1])]))
        at += r.shape[1]
    loads = [pltpu.make_async_copy(a, b, sl.at[k]) for k, (a, b) in enumerate(pairs)]
    rows_in, weights = loads[:-parts], loads[-parts:]
    order = (ring.oppm, ring.nextm, ring.prevm, mt, ring.opp, nx, pv, ring.me)
    ts = [pltpu.make_async_copy(t_ref.at[d], t.at[d], st.at[k]) for k, d in enumerate(order)]
    begin(weights + ts + rows_in)
    ring.barrier()
    end(weights)

    def product(k, rows, then):
        def part(c):
            a = t[order[k], rows, :]
            then(c, dot(a, w[:, c]) if forward else dot(a, w[c, :], NT))
        chunked(D, NB, part)

    def for_mate(k, *copies):
        def then(c, v):
            stg[k, :, c] = v.astype(BF)
        ts[k].wait()
        product(k, every, then)
        links.start(*copies)

    def own(k, rows, then):
        def summed(c, v):
            then(c, v + p[k, rows, c].astype(F32))
        product(k + 4, rows, summed)

    for_mate(0, M0, M1)
    for_mate(1, M2)
    for_mate(2, M3)
    ts[4].wait()
    for rows, m, on in ((lo, M0, R1), (hi, M1, L1)):
        def then(c, v):
            s[0, rows, c] = v.astype(BF)
        links.got(m)
        own(0, rows, then)
        links.start(on)
    for k, m, ready, on in ((1, M2, hi, R2), (2, M3, lo, L2)):
        def then(c, v):
            a, b = (v[:H], v[H:]) if ready is lo else (v[H:], v[:H])
            s[k, ready, c] = a.astype(BF)
            kept[k - 1, :, c] = b
        ts[k + 4].wait()
        links.got(m)
        own(k, every, then)
        links.start(on)
    for_mate(3, M4)

    def keep(c, v):
        acc[:, c] = v
    ts[7].wait()
    links.got(M4)
    own(3, every, keep)
    for k, m, half, on in ((1, R1, 0, R3), (2, L1, H, L3)):
        def add(at):
            s[k, pl.ds(half + at.start, at.size), :] = (kept[k - 1, at, :] + tr[k - 1, at, :].astype(F32)).astype(BF)
        links.got(m)
        chunked(H, 16, add)
        links.start(on)
    end(rows_in)

    def last(at, total):
        x = xt[at, :].astype(F32)
        if forward:
            h = (x + total).astype(BF)
            ht[at, :] = h
            wide = h.astype(F32)
            et[at, :] = (wide * norm_scale(wide)).astype(BF)
        else:
            ht[at, :] = (et[at, :].astype(F32) + unnorm(x, total)).astype(BF)

    finish(links, acc, frp, frn, last)
    outs = [pltpu.make_async_copy(a, b, sl.at[k]) for k, (a, b) in enumerate(((ht, h_ref), (et, b_ref)) if forward else ((ht, h_ref),))]
    begin(outs)
    end(outs)
    links.sent(*SCATTER[:-1])


def product_scatter(t, ws, x, n, cid, extra=None):
    T, D = x.shape
    K = t.shape[2]
    forward = extra is None
    row = V((T, D), BF)
    scratch = [V((K, D) if forward else (D, K), BF), V(t.shape, BF), row, row, row, V((4, T, D), BF), V((4, T, D), BF), V((3, T, D), BF),
               V((2, T // 2, D), F32), V((T, D), F32), V((2, T // 2, D), BF), row, row, DMA((COPIES,)), DMA((COPIES,)), DMA((8,)), DMA((8,))]
    return call(functools.partial(_product_scatter, n=n, forward=forward, parts=len(ws)), [t, x, *([] if forward else [extra]), *ws],
                [S((T, D), BF)] * (1 + forward), scratch, 2 * n * T * D * K, "product_scatter", cid)


def _mlp(b_ref, dhid_ref, wg_ref, wu_ref, h_ref, dy_ref, bg, hid, dgo, duo, dh, own, frm,
         wg, wu, bt, dht, st, acc, stg, s3, s1, p1, p3, tr, frp, frn, ss, rs, sw, sb, sd, so, sl, *, n):
    ring, links = Ring(n), Links(ss, rs)
    T, D = b_ref.shape
    F = wg_ref.shape[1]
    H, NC, NB = T // 2, F // 3, D // 4
    me, nx, pv, mt = ring.me, ring.next, ring.prev, ring.mate
    lo, hi = pl.ds(0, H), pl.ds(H, H)
    gather_copies(links, ring, b_ref, bg, T)
    for k, src, dst, to in ((M5, stg.at[0], frm, mt), (M0, stg.at[1, hi], p1.at[0], mt), (M1, stg.at[0], p3, mt), (M2, stg.at[1, hi], p1.at[1], mt),
                            (M3, stg.at[0, hi], p1.at[2], mt), (M4, stg.at[1, hi], p1.at[3], mt),
                            (R1, s3.at[lo], tr.at[0], nx), (L1, s3.at[hi], tr.at[1], pv), (R2, s1.at[1], frp.at[hi], nx), (L2, s1.at[0], frn.at[lo], pv),
                            (R3, s1.at[2], frp.at[lo], nx), (L3, s1.at[3], frn.at[hi], pv)):
        links.put(k, src, dst, to)
    units = [whole(me), whole(mt), ((pv, 0), (ring.prevm, 0)), whole(ring.oppm), whole(ring.opp), ((nx, 1), (ring.nextm, 1)),
             ((nx, 0), (ring.nextm, 0)), ((pv, 1), (ring.prevm, 1))]
    count = len(units)

    def fetch(u, slot):
        return moves(u, units, bg, bt.at[slot], sb.at[slot]) + moves(u, units, dhid_ref, dht.at[slot], sd.at[slot])

    def fetching(u):
        return lambda: begin(fetch(u, u % 2))

    def store(u, slot):
        return [c for m, ref in enumerate((hid, dgo, duo)) for c in moves(u, units, ref, st.at[slot, m], so.at[slot, m], True)]

    def weights(j):
        s = block_rows(j, NC)
        return [pltpu.make_async_copy(a.at[:, s], b.at[:, s], sw.at[k, j]) for k, (a, b) in enumerate(((wg_ref, wg), (wu_ref, wu)))]

    pairs = ((b_ref, bt.at[0]), (dhid_ref.at[me], dht.at[0]), (bt.at[0], bg.at[me]), (acc, own), (own, acc), (frm, bt.at[0]), (h_ref, bt.at[1]), (dy_ref, s3), (stg.at[0], dh))
    *first, keep, own_out, own_in, frm_in, h_in, dy_in, dh_out = [pltpu.make_async_copy(a, b, sl.at[k]) for k, (a, b) in enumerate(pairs)]
    begin(first)
    for j in range(F // NC):
        begin(weights(j))
    ring.barrier()
    links.start(RA, LA, RB, LB, MA)
    end(first)
    keep.start()

    def pair(k, more=None):
        def add(at):
            v = acc[at, :] + p1[k, at, :].astype(F32)
            if more is not None:
                v = v + tr[more, at, :].astype(F32)
            s1[k, at, :] = v.astype(BF)
        chunked(H, 16, add)

    def mid0():
        keep.wait()
        links.passed_on(RA, LA)
        links.got(MA)
        begin(fetch(1, 1))

    def mid1():
        links.passed_on(RB)
        links.start(RE)
        links.passed_on(LB)
        links.start(LE, MB, MC)
        own_out.start()

    def mid3():
        links.got(M0)
        pair(0)
        links.start(L2)
        links.sent(M5)

    def mid6():
        links.got(M2)
        pair(1)
        links.start(R2)
        links.sent(M1)

    def mid7():
        links.got(M3, R1)
        pair(2, 0)
        links.start(R3)
        links.sent(M2)

    def late1():
        links.got(MB)
        begin(fetch(2, 0))

    def late2():
        links.got(RC, RD)
        links.start(MD)
        links.got(LC, LD)
        links.start(ME)

    def late4():
        links.got(MC)
        begin(fetch(5, 1))
        links.got(LE)
        links.start(MG)
        links.got(RE)
        links.start(MF)

    def late5():
        links.got(MG)
        begin(fetch(6, 0))

    def late6():
        links.got(MF)
        begin(fetch(7, 1))

    def post2():
        links.start(M0)
        links.got(MD, ME)
        begin(fetch(3, 1))

    def post7():
        links.start(M4)
        links.got(M4, L1)
        pair(3, 1)
        links.start(L3)

    mids = {0: mid0, 1: mid1, 2: own_out.wait, 3: mid3, 4: lambda: links.got(M1), 5: lambda: links.sent(M0), 6: mid6, 7: mid7}
    lates = {1: late1, 2: late2, 3: fetching(4), 4: late4, 5: late5, 6: late6}
    posts = {1: lambda: links.start(M5), 2: post2, 3: lambda: links.start(M1), 4: lambda: links.start(R1, L1), 5: lambda: links.start(M2),
             6: lambda: links.start(M3), 7: post7}

    def unit(u, _):
        slot = lax.rem(u, 2)

        @pl.when(u > 0)
        def _():
            end(fetch(u, slot))

        @pl.when(u > 1)
        def _():
            end(store(u - 2, slot))

        def forth(j, _):
            @pl.when(u == 0)
            def _():
                end(weights(j))
            s = block_rows(j, NC)
            x = bt[slot]
            gate, up = dot(x, wg[:, s]), dot(x, wu[:, s])
            d = dht[slot, :, s].astype(F32)
            sig = jax.nn.sigmoid(gate)
            act = gate * sig
            for m, v in enumerate((act * up, d * up * (sig + act * (1 - sig)), d * act)):
                st[slot, m, :, s] = v.astype(BF)

        lax.fori_loop(0, F // NC, forth, None)
        begin(store(u, slot))
        steps(u, mids)
        mate_only = (u == 1) | (u == 3)
        halved = (u == 2) | (u > 4)
        side = jnp.where(u == 6, 0, 1)

        def back(c):
            v = dot(st[slot, 1], wg[c, :], NT) + dot(st[slot, 2], wu[c, :], NT)

            @pl.when(u == 0)
            def _():
                acc[:, c] = v

            @pl.when(mate_only)
            def _():
                stg[0, :, c] = v.astype(BF)

            @pl.when(u == 4)
            def _():
                s3[:, c] = (v + p3[:, c].astype(F32)).astype(BF)

            @pl.when(halved)
            def _():
                acc[:H, c] = v[:H]
                stg[side, H:, c] = v[H:].astype(BF)

        lax.fori_loop(0, 2, lambda j, _: back(block_rows(j, NB)), None)
        steps(u, lates)
        lax.fori_loop(2, 4, lambda j, _: back(block_rows(j, NB)), None)
        steps(u, posts)

    lax.fori_loop(0, count, unit, None)
    own_in.start()
    links.got(M5)
    links.sent(M3, R1, L1)
    end(store(count - 2, 0) + store(count - 1, 1))
    begin([frm_in, h_in, dy_in])
    end([own_in, frm_in, h_in, dy_in])

    def add(at):
        acc[at, :] += bt[0, at, :].astype(F32)
    chunked(T, 16, add)

    def last(at, total):
        stg[0, at, :] = (s3[at, :].astype(F32) + unnorm(bt[1, at, :].astype(F32), total)).astype(BF)

    finish(links, acc, frp, frn, last)
    dh_out.start()
    dh_out.wait()
    links.sent(*GATHER, R2, R3, L2, L3, M4)


def mlp(b, dhid, wg, wu, h, dy, n, cid):
    T, D = b.shape
    F = wg.shape[1]
    H = T // 2
    row, weight, halves = V((T, D), BF), V((D, F), BF), V((4, H, D), BF)
    scratch = [weight, weight, V((2, T, D), BF), V((2, T, F), BF), V((2, 3, T, F), BF), V((T, D), F32), V((2, T, D), BF), row, halves, halves, row,
               V((2, H, D), BF), row, row, DMA((COPIES,)), DMA((COPIES,)), DMA((2, 3)), DMA((2, 2)), DMA((2, 2)), DMA((2, 3, 2)), DMA((9,))]
    wide = S((n, T, F), BF)
    got = call(functools.partial(_mlp, n=n), [b, dhid, wg, wu, h, dy], [S((n, T, D), BF), wide, wide, wide, S((T, D), BF), S((T, D), F32), S((T, D), BF)],
               scratch, 8 * n * T * D * F, "mlp", cid)
    return got[:5]


def solution(mesh):
    n = mesh.shape["tp"]

    def step(x, dy, wq, wk, wv, wo, wg, wu, wd):
        x, dy = x[0], dy[0]
        flat = lambda t: t.reshape(-1, t.shape[2])
        blocks = lambda t: t.reshape(n, -1, t.shape[1])
        by = lambda a, b: dot(a, b, TN).astype(BF)
        cos, sin = angles(n * x.shape[0])
        a, qkv = map(flat, gather_qkv(x, wq, wk, wv, cos, sin, n, 0))
        dy_all, dhid, heads, lse = attend_gather(qkv, dy, wd, n, 1)
        h, b = product_scatter(blocks(heads), [wo], x, n, 2)
        b, hid, dg, du, dh = mlp(b, dhid, wg, wu, h, dy, n, 3)
        b, hid, dg, du = map(flat, (b, hid, dg, du))
        dh_all = lax.all_gather(dh, "tp", axis=0, tiled=True)
        by_down, by_gate, by_up = by(hid, flat(dy_all)), by(b, dg), by(b, du)
        (dh_all, by_down, by_gate, by_up) = lax.optimization_barrier((dh_all, by_down, by_gate, by_up))
        dqkv = attend_bwd(qkv, dot(dh_all, wo, NT).astype(BF), heads, lse, cos, sin)
        (dx,) = product_scatter(blocks(dqkv), [wq, wk, wv], x, n, 4, dh)
        by_q, by_k, by_v = jnp.split(by(a, dqkv), (wq.shape[1], wq.shape[1] + wk.shape[1]), axis=1)
        return dx[None], by_q, by_k, by_v, by(heads, dh_all), by_gate, by_up, by_down

    states, by_columns, by_rows = P("dp", "tp", None), P(None, "tp"), P("tp", None)
    weights = (by_columns, by_columns, by_columns, by_rows, by_columns, by_columns, by_rows)
    own = tuple(P("dp", "tp") if spec == by_columns else P(("dp", "tp"), None) for spec in weights)
    return jax.shard_map(step, mesh=mesh, in_specs=(states, states, *weights), out_specs=(states, *own), check_vma=False)
```

```python
import functools

import jax
import jax.numpy as jnp
from jax import lax
from jax.experimental import pallas as pl
from jax.experimental.pallas import tpu as pltpu
from jax.sharding import PartitionSpec as P

BF, F32 = jnp.bfloat16, jnp.float32
HEAD = 128
THETA = 10000
NEG = -1e30
HIDDEN = 2 * NEG
LOG2E = 1.4426950408889634
SCALE = HEAD**-0.5
MOST = 67_000_000
BQ = BK = 512
TILE = 512
NN, NT, TN = ((((a,), (b,)), ((), ())) for a, b in ((1, 0), (1, 1), (0, 0)))
ANY = pl.BlockSpec(memory_space=pl.ANY)
S, V, DMA = jax.ShapeDtypeStruct, pltpu.VMEM, pltpu.SemaphoreType.DMA

RA, RB, RC, RD, RE, LA, LB, LC, LD, LE, MA, MB, MC, MD, ME, MF, MG = GATHER = range(17)
R1, R2, R3, L1, L2, L3, M0, M1, M2, M3, M4, M5 = SCATTER = range(17, 29)
COPIES = 29
LO, HI = range(2)


def dot(a, b, dims=NN, **kw):
    return lax.dot_general(a, b, dims, preferred_element_type=F32, **kw)


def norm_scale(wide):
    return lax.rsqrt(jnp.mean(wide * wide, -1, keepdims=True) + 1e-6)


def unnorm(wide, d):
    scale = norm_scale(wide)
    return d * scale - wide * (scale * scale * scale * jnp.mean(d * wide, -1, keepdims=True))


def turn(t, cos, sin):
    return t * cos + pltpu.roll(t, HEAD // 2, 1) * sin


def angles(places):
    half = HEAD // 2
    a = places.astype(F32)[:, None] * THETA ** (-jnp.arange(half, dtype=F32) / half)
    cos, sin = jnp.cos(a), jnp.sin(a)
    return jnp.concatenate([cos, cos], -1), jnp.concatenate([-sin, sin], -1)


class Ring:
    def __init__(self, n):
        self.me = lax.axis_index("tp")
        core, chips = lax.rem(self.me, 2), n // 2
        chip = [lax.rem(lax.div(self.me, 2) + k, chips) for k in range(chips)]
        self.next, self.opp, self.prev = [2 * c + core for c in chip[1:]]
        self.mate, self.nextm, self.oppm, self.prevm = [2 * c + 1 - core for c in chip]

    def barrier(self):
        b = pltpu.get_barrier_semaphore()
        near = (self.next, self.prev, self.mate)
        for d in near:
            pl.semaphore_signal(b, inc=1, device_id={"tp": d}, device_id_type=pl.DeviceIdType.MESH)
        pl.semaphore_wait(b, len(near))


class Links:
    def __init__(self, ss, rs, base=0):
        self.ss, self.rs, self.base, self.made = ss, rs, base, {}

    def put(self, k, src, dst, dev):
        self.made[k] = lambda: pltpu.make_async_remote_copy(src_ref=src, dst_ref=dst, send_sem=self.ss.at[self.base + k], recv_sem=self.rs.at[self.base + k],
                                                            device_id={"tp": dev}, device_id_type=pl.DeviceIdType.MESH)

    def start(self, *ks):
        for k in ks:
            self.made[k]().start()

    def got(self, *ks):
        for k in ks:
            self.made[k]().wait_recv()

    def sent(self, *ks):
        for k in ks:
            self.made[k]().wait_send()

    def passed_on(self, *ks):
        for k in ks:
            self.got(k)
            self.start(k + 2)


def flat(t):
    return t.reshape(-1, t.shape[-1])


def begin(copies):
    for c in copies:
        c.start()


def end(copies):
    for c in copies:
        c.wait()


def pick(u, values):
    out = values[0]
    for k, v in enumerate(values):
        out = jnp.where(u == k, v, out)
    return out


def steps(u, events):
    for k, f in events.items() if isinstance(events, dict) else enumerate(events):
        def run(f=f):
            f()
        if f is not None:
            pl.when(u == k)(run)


def loop(count, f, first=0):
    def body(k, _):
        f(k)
    lax.fori_loop(first, count, body, None)


def block_rows(i, size):
    return pl.ds(pl.multiple_of(i * size, size), size)


def chunked(size, width, f):
    loop(size // width, lambda j: f(block_rows(j, width)))


def gather_copies(links, ring, src, dst, T):
    H, Q = T // 2, T // 4
    me, nx, pv, mt, opp = ring.me, ring.next, ring.prev, ring.mate, ring.opp
    for k, slot, a, rows, to in ((RA, me, 0, Q, nx), (RB, me, Q, Q, nx), (RC, pv, 0, Q, nx), (RD, pv, Q, Q, nx), (RE, me, H, H, nx),
                                 (LA, me, H, Q, pv), (LB, me, H + Q, Q, pv), (LC, nx, H, Q, pv), (LD, nx, H + Q, Q, pv), (LE, me, 0, H, pv),
                                 (MA, me, 0, T, mt), (MB, pv, 0, H, mt), (MC, nx, H, H, mt), (MD, opp, 0, H, mt), (ME, opp, H, H, mt),
                                 (MF, pv, H, H, mt), (MG, nx, 0, H, mt)):
        at = pl.ds(a, rows)
        links.put(k, src.at[at] if slot is me else dst.at[slot, at], dst.at[slot, at], to)


def whole(shard):
    return (shard, LO), (shard, HI)


def moves(u, units, far, near, sem, back=False):
    H = near.shape[0] // 2
    out = []
    for k in range(2):
        shard, half = (pick(u, [x[k][m] for x in units]) for m in range(2))
        ends = far.at[shard, pl.ds(pl.multiple_of(half * H, H), H)], near.at[pl.ds(k * H, H)]
        out.append(pltpu.make_async_copy(*(ends[::-1] if back else ends), sem.at[k]))
    return out


def rows_of_unit(u, units, k, H):
    shard, half = (pick(u, [x[k][m] for x in units]) for m in range(2))
    return pl.ds(pl.multiple_of((2 * shard + half) * H, H), H)


def stream(ring, links, src, tile, sin, dst, out, sout, work, events, schedule=range(8), beside=None):
    units = [whole(ring.me), whole(ring.mate), ((ring.prev, LO), (ring.next, HI)), ((ring.prevm, LO), (ring.nextm, HI)), whole(ring.opp),
             whole(ring.oppm), ((ring.prev, HI), (ring.next, LO)), ((ring.prevm, HI), (ring.nextm, LO))]
    fetch = lambda u, slot: moves(u, units, src, tile.at[slot], sin.at[slot])
    store = lambda u, slot: moves(u, units, dst, out.at[slot], sout.at[slot], True)
    latest = lambda k: sum(jnp.where(k < s, 0, 1) for s in schedule) - 1

    def fetch_for(k):
        u = latest(k)

        @pl.when(latest(k - 1) < u)
        def _():
            begin(fetch(u, lax.rem(u, 2)))

    fetch_for(0)

    def step(k):
        if beside is not None:
            beside(k)
        u = latest(k)

        @pl.when(latest(k - 1) < u)
        def _():
            slot = lax.rem(u, 2)
            end(fetch(u, slot))

            if dst is None:
                work(u, units, tile.at[slot])
            else:
                pl.when(u > 1)(lambda: end(store(u - 2, slot)))
                work(u, units, tile.at[slot], out.at[slot])
                begin(store(u, slot))

        steps(k, events)
        fetch_for(k + 1)

    loop(schedule[-1] + 1, step)
    if dst is not None:
        end(store(len(units) - 2, 0) + store(len(units) - 1, 1))
    links.sent(*GATHER)


class Fill:
    def __init__(self, jobs, tile, sin, sout):
        self.jobs, self.tile, self.sin, self.sout = jobs, tile, sin, sout
        self.per = [src.shape[2] // TILE for src, *_ in jobs]
        self.steps = sum(self.per)

    def fetch(self, k):
        at = 0
        for (src, *_), per in zip(self.jobs, self.per):
            @pl.when((k >= at) & (k < at + per))
            def _():
                begin([self.load(src, k - at, lax.rem(k, 2))])
            at += per

    def load(self, src, j, slot):
        return pltpu.make_async_copy(src.at[:, :, block_rows(j, TILE)], self.tile.at[slot], self.sin.at[slot])

    def step(self, k):
        slot = lax.rem(k, 2)
        at = 0
        end([self.load(self.jobs[0][0], 0, slot)])
        self.fetch(k + 1)
        for (src, fixed, out, right, ends), per in zip(self.jobs, self.per):
            @pl.when((k >= at) & (k < at + per))
            def _():
                j = k - at
                store = lambda j, slot: [pltpu.make_async_copy(out.at[slot, :, a], b, self.sout.at[slot, m]) for m, (a, b) in enumerate(ends(j))]

                @pl.when(j > 1)
                def _():
                    end(store(j - 2, slot))

                t = self.tile[slot].reshape(-1, TILE)
                r = dot(flat(fixed[...]), t, TN) if right else dot(t, flat(fixed[...]), TN)
                out[slot, :, :r.shape[1]] = r.astype(BF)
                begin(store(j, slot))

                @pl.when(j == per - 1)
                def _():
                    end(store(j, slot) + store(j - 1, 1 - slot))
            at += per


def gather_events(links, near=None):
    def far():
        links.got(RC, RD)
        links.start(MD)
        links.got(LC, LD)
        links.start(ME)

    def last():
        links.got(RE)
        links.start(MF)
        links.got(LE)
        links.start(MG)

    got = lambda *ks: lambda: links.got(*ks)
    return [got(MA), near, got(MB, MC), far, got(MD, ME), last, got(MF, MG)]


def finish(links, acc, frp, frn, last):
    H = acc.shape[0] // 2

    def each(m, half, f):
        links.got(m)
        chunked(H, 16, lambda at: f(pl.ds(half + at.start, at.size)))

    def add(fr):
        def f(at):
            acc[at, :] += fr[at, :].astype(F32)
        return f

    each(R2, H, add(frp))
    each(L2, 0, add(frn))
    each(R3, 0, lambda at: last(at, acc[at, :] + frp[at, :].astype(F32)))
    each(L3, H, lambda at: last(at, acc[at, :] + frn[at, :].astype(F32)))


class Scatter:
    def __init__(self, ring, links, product, stg, p, s, acc, tr, fr):
        self.ring, self.links, self.product, self.stg, self.p, self.s, self.acc, self.tr, self.fr = ring, links, product, stg, p, s, acc, tr, fr
        T = acc.shape[0]
        H = T // 2
        nx, pv, mt = ring.next, ring.prev, ring.mate
        self.every, self.lo, self.hi = every, lo, hi = pl.ds(0, T), pl.ds(0, H), pl.ds(H, H)
        at = lambda ref: [ref.at[k] for k in range(ref.shape[0])]
        even, odd, pa, pb, pc, pd, so, sn, sp, on, off, fp, fn = [*at(stg), *at(p), *at(s), *at(tr), *at(fr)]
        for k, src, dst, to in ((M0, even.at[lo], pa.at[lo], mt), (M1, even.at[hi], pa.at[hi], mt), (M2, odd, pb, mt), (M3, even, pc, mt), (M4, odd, pd, mt),
                                (R1, so.at[lo], on, nx), (L1, so.at[hi], off, pv), (R2, sn.at[hi], fp.at[hi], nx), (L2, sp.at[lo], fn.at[lo], pv),
                                (R3, sn.at[lo], fp.at[lo], nx), (L3, sp.at[hi], fn.at[hi], pv)):
            links.put(k, src, dst, to)

    def for_mate(self, k, shard, *on):
        def then(c, v):
            self.stg[k % 2, :, c] = v.astype(BF)
        self.product(shard, self.every, then)
        self.links.start(*on)

    def own(self, k, shard, rows, wait, on, more=None):
        def then(c, v):
            v = v + self.p[k, rows, c].astype(F32)
            if more is not None:
                v = v + self.tr[more, :, c].astype(F32)
            self.s[k, rows, c] = v.astype(BF)
        self.links.got(wait)
        self.product(shard, rows, then)
        self.links.start(on)

    def send(self):
        links, ring = self.links, self.ring
        self.for_mate(0, ring.oppm, M0, M1)
        self.for_mate(1, ring.nextm, M2)
        self.own(0, ring.opp, self.lo, M0, R1)
        self.own(0, ring.opp, self.hi, M1, L1)
        links.sent(M0, M1)
        self.for_mate(2, ring.prevm, M3)
        self.own(1, ring.next, self.hi, M2, R2)
        self.own(2, ring.prev, self.lo, M3, L2)
        links.sent(M2)
        self.for_mate(3, ring.mate, M4)

        def keep(c, v):
            self.acc[:, c] = v + self.p[3, :, c].astype(F32)
        links.got(M4)
        self.product(ring.me, self.every, keep)
        links.sent(M3, M4)

    def pass_on(self):
        self.own(1, self.ring.next, self.lo, R1, R3, 0)
        self.own(2, self.ring.prev, self.hi, L1, L3, 1)

    def finish(self, last):
        self.links.sent(R1, L1)
        finish(self.links, self.acc, self.fr.at[0], self.fr.at[1], last)


def scatter_scratch(T, D):
    return [V((2, T, D), BF), V((4, T, D), BF), V((3, T, D), BF), V((T, D), F32), V((2, T // 2, D), BF), V((2, T, D), BF)]


def call(body, args, outs, scratch, flops, name, cid=None):
    return pl.pallas_call(
        body, in_specs=[ANY] * len(args), out_specs=[ANY] * len(outs), out_shape=outs, scratch_shapes=scratch, name=name,
        compiler_params=pltpu.CompilerParams(collective_id=cid, has_side_effects=True, vmem_limit_bytes=MOST),
        cost_estimate=pl.CostEstimate(flops=flops, bytes_accessed=sum(t.size for t in (*args, *outs)), transcendentals=0),
    )(*args)


def rows_of(t):
    return jnp.concatenate([t[:, a:a + HEAD] for a in range(0, t.shape[1], HEAD)], axis=0)


def set_gap(gap):
    gap[...] = lax.broadcasted_iota(jnp.int32, gap.shape, 1) - lax.broadcasted_iota(jnp.int32, gap.shape, 0)


def key_blocks(iq, block):
    seen = lax.div(iq * BQ + 1, BK)
    loop(seen, lambda j: block(j, False))
    loop(lax.div((iq + 1) * BQ + BK - 1, BK), lambda j: block(j, True), seen)


def attend_block(iq, qkv, o_ref, lse_ref, qs, top, mix, gap):
    NQ = o_ref.shape[1]
    cols = qs.shape[0]
    mine = block_rows(iq, BQ)
    qs[...] = rows_of(qkv[mine, :NQ])
    top[...] = jnp.full_like(top, NEG)
    mix[...] = jnp.zeros_like(mix)
    ones = jnp.ones((8, BK), BF)
    strips = [slice(a, a + BQ) for a in range(0, cols, BQ)]

    def block(j, masked):
        here = block_rows(j, BK)
        keys = qkv[here, NQ:NQ + HEAD]
        values = jnp.concatenate([qkv[here, NQ + HEAD:].T, ones], axis=0)
        scores = [dot(keys, qs[at, :], NT) for at in strips]
        ps, keeps = [], []
        for at, s in zip(strips, scores):
            if masked:
                s = jnp.where(gap[...] >= j * BK - iq * BQ, s, HIDDEN)
            old = top[:, at]
            new = jnp.maximum(old, s.max(axis=0, keepdims=True))
            top[:, at] = new
            ps.append(jnp.exp2((s - new) * (SCALE * LOG2E)).astype(BF))
            keeps.append(jnp.exp2((old - new) * (SCALE * LOG2E)))
        for at, p, keep in zip(strips, ps, keeps):
            mix[:, at] = mix[:, at] * keep + dot(values, p)

    key_blocks(iq, block)
    total = mix[HEAD:HEAD + 1, :]
    out = (mix[:HEAD, :] * (1 / total)).T.astype(BF)
    for h in range(NQ // HEAD):
        o_ref[mine, h * HEAD:(h + 1) * HEAD] = out[h * BQ:(h + 1) * BQ]
    lse_ref[iq] = top[...] * SCALE + jnp.log(total)


def _attend_bwd(qkv_ref, do_ref, o_ref, lse_ref, cos_ref, sin_ref, one, two, out_ref, one_out, two_out, qs, dos, dq, dk, dv, gap, one_tile, two_tile, sem):
    NQ = do_ref.shape[1]
    tokens, cols = dk.shape[0], qs.shape[0]
    iq = pl.program_id(0)
    mine = block_rows(iq, BQ)
    come, go = [[pltpu.make_async_copy(x, y, sem.at[k]) for k, (x, y) in enumerate(ends)]
                for ends in (((one, one_tile), (two, two_tile)), ((one_tile, one_out), (two_tile, two_out)))]
    steps(iq, {0: lambda: begin(come), 1: lambda: (come[0].wait(), go[0].start()), 2: lambda: (come[1].wait(), go[1].start())})
    qs[...] = rows_of(qkv_ref[mine, :NQ])
    dos[...] = rows_of(do_ref)
    dq[...] = jnp.zeros_like(dq)

    @pl.when(iq == 0)
    def _():
        set_gap(gap)
        dk[...] = jnp.zeros_like(dk)
        dv[...] = jnp.zeros_like(dv)

    delta = dot(jnp.ones((8, HEAD), F32), dos[...].astype(F32) * rows_of(o_ref).astype(F32), NT, precision=lax.Precision.HIGHEST)[:1]
    lse = lse_ref[0] * LOG2E
    strips = [slice(a, a + BQ) for a in range(0, cols, BQ)]

    def block(j, masked):
        here = block_rows(j, BK)
        keys, values = qkv_ref[here, NQ:NQ + HEAD], qkv_ref[here, NQ + HEAD:]
        scores = [dot(keys, qs[at, :], NT) for at in strips]
        dps = [dot(values, dos[at, :], NT) for at in strips]
        for at, s, dp in zip(strips, scores, dps):
            p = jnp.exp2(s * (SCALE * LOG2E) - lse[:, at])
            if masked:
                p = jnp.where(gap[...] >= j * BK - iq * BQ, p, 0.0)
            ds = (p * (dp - delta[:, at])).astype(BF)
            dv[here, :] += dot(p.astype(BF), dos[at, :])
            dk[here, :] += dot(ds, qs[at, :])
            dq[:, at] += dot(keys.T, ds)

    key_blocks(iq, block)
    back = (dq[...] * SCALE).T
    for h in range(NQ // HEAD):
        out_ref[mine, h * HEAD:(h + 1) * HEAD] = turn(back[h * BQ:(h + 1) * BQ], cos_ref[mine, :], -sin_ref[mine, :]).astype(BF)

    @pl.when(iq == pl.num_programs(0) - 1)
    def _():
        end(go)

        def rest(at):
            out_ref[at, NQ:NQ + HEAD] = turn(dk[at, :] * SCALE, cos_ref[at, :], -sin_ref[at, :]).astype(BF)
            out_ref[at, NQ + HEAD:] = dv[at, :].astype(BF)
        chunked(tokens, BQ, rest)


def attend_bwd(qkv, d_out, out, lse, cos, sin, one, two):
    tokens, NQ = out.shape
    cols = lse.shape[2]
    part = pl.BlockSpec((BQ, NQ), lambda i: (i, 0))
    all_of = lambda t: pl.BlockSpec(t.shape, lambda i: (0, 0))
    shape = lambda t: S(t.shape, BF)
    return pl.pallas_call(
        _attend_bwd, grid=(tokens // BQ,), name="attend_bwd",
        in_specs=[all_of(qkv), part, part, pl.BlockSpec((1, 1, cols), lambda i: (i, 0, 0)), all_of(cos), all_of(sin), ANY, ANY],
        out_specs=[all_of(qkv), ANY, ANY], out_shape=[shape(qkv), shape(one), shape(two)],
        scratch_shapes=[V((cols, HEAD), BF), V((cols, HEAD), BF), V((HEAD, cols), F32), V((tokens, HEAD), F32), V((tokens, HEAD), F32), V((BK, BQ), jnp.int32),
                        V(one.shape, BF), V(two.shape, BF), DMA((2,))],
        compiler_params=pltpu.CompilerParams(vmem_limit_bytes=MOST),
        cost_estimate=pl.CostEstimate(flops=5 * tokens * tokens * NQ, bytes_accessed=8 * qkv.size, transcendentals=tokens * cols),
    )(qkv, d_out, out, lse, cos, sin, one, two)


def _front(x_ref, dy_ref, wq_ref, wk_ref, wv_ref, wo_ref, wd_ref, c_ref, s_ref, a_all, qkv_ref, dy_all, dhid, o_ref, lse_ref, cos_ref, sin_ref, h_ref, b_ref,
           an, tile, small, qkv, o, lse, qs, top, mix, gap, wo, dt, stg, p, s, acc, tr, fr, ss, rs, sb, so, sl, *, n):
    T, D = x_ref.shape
    NQ, NK = wq_ref.shape[1], wk_ref.shape[1]
    turned, Q = NQ + NK, T // 4

    def links():
        ring = Ring(n)
        of_a, of_dy, of_o = (Links(ss, rs, k * COPIES) for k in range(3))
        gather_copies(of_a, ring, an, a_all, T)
        gather_copies(of_dy, ring, dy_ref, dy_all, T)
        return ring, of_a, of_dy, of_o

    pairs = ((x_ref, stg.at[0]), (dy_ref, stg.at[1]), (c_ref, small.at[0]), (s_ref, small.at[1]), (wo_ref, wo),
             (x_ref, stg.at[0]), (qkv, qkv_ref), (o, o_ref), (lse, lse_ref), (s.at[0], h_ref), (stg.at[1], b_ref))
    copies = [pltpu.make_async_copy(a, b, sl.at[k]) for k, (a, b) in enumerate(pairs)]
    x_in, dy_in, c_in, s_in, wo_in, x_again, *outs = copies
    x_in.start()

    def products(w, cos, sin):
        tables = [pltpu.make_async_copy(a, b, so.at[0, k]) for k, (a, b) in enumerate(((cos, cos_ref), (sin, sin_ref)))]
        ring, of_a, of_dy, _ = links()
        keep, keep_dy = (pltpu.make_async_copy(a, b.at[ring.me], so.at[1, k]) for k, (a, b) in enumerate(((an, a_all), (stg.at[1], dy_all))))
        place = [pl.ds(0, NQ), pl.ds(NQ, NK), pl.ds(turned, NK)]
        loads = [dy_in, c_in, s_in, wo_in] + [pltpu.make_async_copy(r, w.at[:, c], sb.at[0, k]) for k, (r, c) in enumerate(zip((wq_ref, wk_ref, wv_ref), place))]
        begin(loads)
        ring.barrier()
        x_in.wait()
        for q, k in ((0, RA), (2, LA), (1, RB), (3, LB)):

            def norm(at):
                at = pl.ds(q * Q + at.start, at.size)
                wide = stg[0, at, :].astype(F32)
                an[at, :] = (wide * norm_scale(wide)).astype(BF)
            chunked(Q, 16, norm)
            of_a.start(k)
        of_a.start(MA)
        keep.start()
        end(loads)
        keep_dy.start()

        def table(at):
            row = pl.ds(HEAD + lax.div(at.start, HEAD), 1)
            c0, s0, c1, s1 = small[0, row, :], small[1, row, :], small[0, :HEAD, :], small[1, :HEAD, :]
            cos[at, :] = c0 * c1 - s0 * s1
            sin[at, :] = s0 * c1 + c0 * s1
        chunked(n * T, HEAD, table)
        begin(tables)
        end([keep, keep_dy])

        def work(u, units, x):
            r = dot(x[...], w[...]).astype(BF)
            for k in range(2):
                rows = slice(k * T // 2, (k + 1) * T // 2)
                place = rows_of_unit(u, units, k, T // 2)
                c, s = cos[place, :], sin[place, :]
                for a in range(0, turned, HEAD):
                    qkv[place, a:a + HEAD] = turn(r[rows, a:a + HEAD].astype(F32), c, s).astype(BF)
                qkv[place, turned:] = r[rows, turned:]

        def near():
            of_a.passed_on(RA, LA, RB, LB)
            of_a.start(RE, LE, MB, MC)
            of_dy.start(RA, LA, RB, LB, MA)

        stream(ring, of_a, a_all, tile, sb, None, None, None, work, gather_events(of_a, near))
        end(tables)

    pl.run_scoped(products, V((D, turned + NK), BF), *[V((n * T, HEAD), F32)] * 2)
    outs[0].start()
    set_gap(gap)

    def rest(wd):
        ring, _, of_dy, of_o = links()
        wd_in = pltpu.make_async_copy(wd_ref, wd, so.at[0, 0])
        wd_in.start()
        blocks = n * T // BQ

        def attention(iq):
            attend_block(iq, qkv, o, lse, qs, top, mix, gap)
            steps(iq, {blocks - 2: lambda: of_dy.passed_on(RA, LA)})

        loop(blocks, attention)
        begin(outs[1:3])
        of_dy.passed_on(RB, LB)
        of_dy.start(RE, LE, MB, MC)

        def product(shard, rows, then):
            at = pl.ds(pl.multiple_of(shard * T + rows.start, T // 2), rows.size)
            chunked(D, D // 4, lambda c: then(c, dot(o[at, :], wo[:, c])))

        scatter = Scatter(ring, of_o, product, stg, p, s, acc, tr, fr)
        scatter.send()
        x_again.start()
        wd_in.wait()

        def work(u, units, x, o):
            o[...] = dot(x[...], wd[...], NT).astype(BF)

        stream(ring, of_dy, dy_all, tile, sb, dhid, dt, so, work, gather_events(of_dy))
        scatter.pass_on()
        x_again.wait()

        def last(at, total):
            h = (stg[0, at, :].astype(F32) + total).astype(BF)
            s[0, at, :] = h
            h = h.astype(F32)
            stg[1, at, :] = (h * norm_scale(h)).astype(BF)

        scatter.finish(last)
        begin(outs[3:])
        end(outs)
        of_o.sent(R2, L2, R3, L3)

    pl.run_scoped(rest, V(wd_ref.shape, BF))


def front(x, dy, wq, wk, wv, wo, wd, n, cid):
    T, D = x.shape
    NQ, F, tokens = wo.shape[0], wd.shape[0], n * T
    N, cols = NQ + 2 * HEAD, NQ // HEAD * BQ
    stat = (tokens // BQ, 1, cols)
    table, row = S((tokens, HEAD), F32), S((T, D), BF)
    small = angles(jnp.concatenate([jnp.arange(HEAD), jnp.arange(0, tokens, HEAD)]))
    outs = [S((n, T, D), BF), S((tokens, N), BF), S((n, T, D), BF), S((n, T, F), BF), S((tokens, NQ), BF), S(stat, F32), table, table, row, row]
    scratch = [V((T, D), BF), V((2, T, D), BF), V((2, *small[0].shape), F32), V((tokens, N), BF), V((tokens, NQ), BF),
               V(stat, F32), V((cols, HEAD), BF), V((1, cols), F32), V((HEAD + 8, cols), F32), V((BK, BQ), jnp.int32), V((NQ, D), BF), V((2, T, F), BF),
               *scatter_scratch(T, D), DMA((3 * COPIES,)), DMA((3 * COPIES,)), DMA((2, 3)), DMA((2, 3)), DMA((15,))]
    return call(functools.partial(_front, n=n), [x, dy, wq, wk, wv, wo, wd, *small], outs, scratch, 2 * tokens * D * (N + F + NQ), "front", cid)


def _gather_fill(dh_ref, wo_ref, b_ref, dg_ref, hid_ref, dy_ref, ag, out, by_gate, by_down, w, dg, hid, left, right, ft, at, ot, ss, rs, sb, so, sf, sg, sl, *, n):
    ring, links = Ring(n), Links(ss, rs)
    T = dh_ref.shape[0]
    gather_copies(links, ring, dh_ref, ag, T)
    pairs = ((dh_ref, at.at[1]), (dg_ref, dg), (wo_ref, w), (hid_ref, hid), (at.at[1], ag.at[ring.me]))
    first, fixed, *later, keep = [pltpu.make_async_copy(a, b, sl.at[k]) for k, (a, b) in enumerate(pairs)]
    wide = pl.ds(0, dg.shape[2])
    fill = Fill(((b_ref, dg, left, False, lambda j: ((wide, by_gate.at[block_rows(j, TILE)]),)),
                 (dy_ref, hid, right, True, lambda j: ((pl.ds(0, TILE), by_down.at[:, block_rows(j, TILE)]),))), ft, sf, sg)
    begin([first, fixed])
    fill.fetch(0)
    begin(later)
    ring.barrier()
    links.start(RA, LA, RB, LB, MA)
    first.wait()
    keep.start()
    end([fixed, keep, *later])

    def work(u, units, x, o):
        o[...] = dot(x[...], w[...], NT).astype(BF)

    def near():
        links.passed_on(RB, LB)
        links.start(RE, LE, MB, MC)

    def beside(k):
        pl.when(k < fill.steps)(lambda: fill.step(k))

    mate, _, mates, far, fars, last, lasts = gather_events(links)
    schedule = (1, 3, 7, 8, 13, 14, fill.steps, fill.steps + 1)
    events = {1: mate, 2: lambda: links.passed_on(RA, LA), 5: near, 7: mates, 11: far, 13: fars, 15: last, 16: lasts}
    stream(ring, links, ag, at, sb, out, ot, so, work, events, schedule, beside)


def gather_fill(dh, wo, b, dg, hid, dy, n, cid):
    T, D = dh.shape
    NQ, F = wo.shape[0], dg.shape[2]
    scratch = [V((NQ, D), BF), V((n, T, F), BF), V((n, T, F), BF), V((2, TILE, F), BF), V((2, F, TILE), BF), V((2, n, T, TILE), BF), V((2, T, D), BF),
               V((2, T, NQ), BF), DMA((COPIES,)), DMA((COPIES,)), DMA((2, 2)), DMA((2, 2)), DMA((2,)), DMA((2, 1)), DMA((5,))]
    return call(functools.partial(_gather_fill, n=n), [dh, wo, b, dg, hid, dy],
                [S((n, T, D), BF), S((n, T, NQ), BF), S((D, F), BF), S((F, D), BF)], scratch, 6 * n * T * D * F, "gather_fill", cid)


def _back(t_ref, x_ref, dh_ref, wq_ref, wk_ref, wv_ref, b_ref, du_ref, a_ref, dh_all, heads_ref, dx_ref, by_up, by_q, by_k, by_v, by_o,
          w, t, du, heads, out, ft, stg, p, s, acc, tr, fr, ss, rs, sl, sf, sg, *, n):
    ring, links = Ring(n), Links(ss, rs)
    T, D = x_ref.shape
    NQ, NK = wq_ref.shape[1], wk_ref.shape[1]
    columns = [pl.ds(0, NQ), pl.ds(NQ, NK), pl.ds(NQ + NK, NK)]
    pairs = ((t_ref, t), *((r, w.at[:, c]) for r, c in zip((wq_ref, wk_ref, wv_ref), columns)), (du_ref, du), (heads_ref, heads), (x_ref, stg.at[0]), (dh_ref, stg.at[1]),
             (s.at[0], dx_ref))
    *first, du_in, heads_in, x_in, dh_in, dx_out = [pltpu.make_async_copy(a, b, sl.at[k]) for k, (a, b) in enumerate(pairs)]
    begin([*first, du_in, heads_in])
    ring.barrier()
    end(first)

    def product(shard, rows, then):
        chunked(D, D // 4, lambda c: then(c, dot(t[shard, rows, :], w[c, :], NT)))

    scatter = Scatter(ring, links, product, stg, p, s, acc, tr, fr)
    scatter.send()
    begin([x_in, dh_in])
    end([du_in, heads_in])
    fill = Fill(((b_ref, du, out, False, lambda j: ((pl.ds(0, du.shape[2]), by_up.at[block_rows(j, TILE)]),)),
                 (a_ref, t, out, False, lambda j: [(c, r.at[block_rows(j, TILE)]) for c, r in zip(columns, (by_q, by_k, by_v))]),
                 (dh_all, heads, out, True, lambda j: ((pl.ds(0, TILE), by_o.at[:, block_rows(j, TILE)]),))), ft, sf, sg)
    fill.fetch(0)

    def beside(k):
        fill.step(k)
        steps(k, {4: scatter.pass_on})
    loop(fill.steps, beside)
    end([x_in, dh_in])

    def last(at, total):
        s[0, at, :] = (stg[1, at, :].astype(F32) + unnorm(stg[0, at, :].astype(F32), total)).astype(BF)

    scatter.finish(last)
    dx_out.start()
    dx_out.wait()
    links.sent(R2, L2, R3, L3)


def back(dqkv, x, dh, ws, b, du, a, dh_all, heads, n, cid):
    T, D = x.shape
    K, F = dqkv.shape[2], du.shape[2]
    scratch = [V((D, K), BF), *(V(t.shape, BF) for t in (dqkv, du, heads)), V((2, TILE, F), BF), V((2, n, T, TILE), BF), *scatter_scratch(T, D),
               DMA((COPIES,)), DMA((COPIES,)), DMA((9,)), DMA((2,)), DMA((2, 3))]
    outs = [S((T, D), BF), S((D, F), BF), *(S(w.shape, BF) for w in ws), S((heads.shape[2], D), BF)]
    return call(functools.partial(_back, n=n), [dqkv, x, dh, *ws, b, du, a, dh_all, heads], outs, scratch, 2 * n * T * D * (F + 3 * K), "back", cid)


def _land(*refs):
    m = len(refs) // 3
    ins, outs, tiles, sem = refs[:m], refs[m:2 * m], refs[2 * m:-1], refs[-1]
    come = [pltpu.make_async_copy(a, b, sem.at[k]) for k, (a, b) in enumerate(zip(ins, tiles))]
    go = [pltpu.make_async_copy(a, b, sem.at[k]) for k, (a, b) in enumerate(zip(tiles, outs))]
    begin(come)
    for a, b in zip(come, go):
        a.wait()
        b.start()
    end(go)


def land(arrays):
    shapes = [S(t.shape, BF) for t in arrays]
    return call(_land, arrays, shapes, [*(V(t.shape, BF) for t in arrays), DMA((len(arrays),))], 0, "land")


def _mlp(b_ref, dhid_ref, wg_ref, wu_ref, h_ref, dy_ref, bg, hid, dgo, duo, dh, own, frm,
         wg, wu, bt, dht, st, acc, stg, s3, s1, p1, p3, tr, frp, frn, ss, rs, sw, sb, sd, so, sl, *, n):
    ring, links = Ring(n), Links(ss, rs)
    T, D = b_ref.shape
    F = wg_ref.shape[1]
    H, NC, NB = T // 2, F // 3, D // 4
    me, nx, pv, mt = ring.me, ring.next, ring.prev, ring.mate
    lo, hi = pl.ds(0, H), pl.ds(H, H)
    gather_copies(links, ring, b_ref, bg, T)
    at = lambda ref: [ref.at[k] for k in range(ref.shape[0])]
    pa, pb, pc, pd, sa, sb1, sc, sd1, even, odd, on, off = [*at(p1), *at(s1), *at(stg), *at(tr)]
    for k, src, dst, to in ((M5, even, frm, mt), (M0, odd.at[hi], pa, mt), (M1, even, p3, mt), (M2, odd.at[hi], pb, mt), (M3, even.at[hi], pc, mt), (M4, odd.at[hi], pd, mt),
                            (R1, s3.at[lo], on, nx), (L1, s3.at[hi], off, pv), (R2, sb1, frp.at[hi], nx), (L2, sa, frn.at[lo], pv),
                            (R3, sc, frp.at[lo], nx), (L3, sd1, frn.at[hi], pv)):
        links.put(k, src, dst, to)
    units = [whole(me), whole(mt), ((pv, LO), (ring.prevm, LO)), whole(ring.oppm), whole(ring.opp), ((nx, HI), (ring.nextm, HI)),
             ((nx, LO), (ring.nextm, LO)), ((pv, HI), (ring.prevm, HI))]
    count = len(units)

    def fetch(u, slot):
        return moves(u, units, bg, bt.at[slot], sb.at[slot]) + moves(u, units, dhid_ref, dht.at[slot], sd.at[slot])

    def fetching(u):
        return lambda: begin(fetch(u, u % 2))

    def store(u, slot):
        return [c for m, ref in enumerate((hid, dgo, duo)) for c in moves(u, units, ref, st.at[slot, m], so.at[slot, m], True)]

    def weights(j):
        s = block_rows(j, NC)
        return [pltpu.make_async_copy(a.at[:, s], b.at[:, s], sw.at[k, j]) for k, (a, b) in enumerate(((wg_ref, wg), (wu_ref, wu)))]

    pairs = ((b_ref, bt.at[0]), (dhid_ref.at[me], dht.at[0]), (bt.at[0], bg.at[me]), (acc, own), (own, acc), (frm, bt.at[0]), (h_ref, bt.at[1]), (dy_ref, s3), (stg.at[0], dh))
    *first, keep, own_out, own_in, frm_in, h_in, dy_in, dh_out = [pltpu.make_async_copy(a, b, sl.at[k]) for k, (a, b) in enumerate(pairs)]
    begin(first)
    for j in range(F // NC):
        begin(weights(j))
    ring.barrier()
    links.start(RA, LA, RB, LB, MA)
    end(first)
    keep.start()

    def pair(k, more=None):
        def add(at):
            v = acc[at, :] + p1[k, at, :].astype(F32)
            if more is not None:
                v = v + tr[more, at, :].astype(F32)
            s1[k, at, :] = v.astype(BF)
        chunked(H, 16, add)

    def mid0():
        keep.wait()
        links.passed_on(RA, LA)
        links.got(MA)
        begin(fetch(1, 1))

    def mid1():
        links.passed_on(RB)
        links.start(RE)
        links.passed_on(LB)
        links.start(LE, MB, MC)
        own_out.start()

    def mid3():
        links.got(M0)
        pair(0)
        links.start(L2)
        links.sent(M5)

    def mid6():
        links.got(M2)
        pair(1)
        links.start(R2)
        links.sent(M1)

    def mid7():
        links.got(M3, R1)
        pair(2, 0)
        links.start(R3)
        links.sent(M2)

    def late1():
        links.got(MB)
        begin(fetch(2, 0))

    def late2():
        links.got(RC, RD)
        links.start(MD)
        links.got(LC, LD)
        links.start(ME)

    def late4():
        links.got(MC)
        begin(fetch(5, 1))
        links.got(LE)
        links.start(MG)
        links.got(RE)
        links.start(MF)

    def late5():
        links.got(MG)
        begin(fetch(6, 0))

    def late6():
        links.got(MF)
        begin(fetch(7, 1))

    def post2():
        links.start(M0)
        links.got(MD, ME)
        begin(fetch(3, 1))

    def post7():
        links.start(M4)
        links.got(M4, L1)
        pair(3, 1)
        links.start(L3)

    starting = lambda *ks: lambda: links.start(*ks)
    mids = [mid0, mid1, own_out.wait, mid3, lambda: links.got(M1), lambda: links.sent(M0), mid6, mid7]
    lates = [None, late1, late2, fetching(4), late4, late5, late6]
    posts = [None, starting(M5), post2, starting(M1), starting(R1, L1), starting(M2), starting(M3), post7]

    def unit(u):
        slot = lax.rem(u, 2)

        @pl.when(u > 0)
        def _():
            end(fetch(u, slot))

        @pl.when(u > 1)
        def _():
            end(store(u - 2, slot))

        def forth(j):
            @pl.when(u == 0)
            def _():
                end(weights(j))
            s = block_rows(j, NC)
            x = bt[slot]
            gate, up = dot(x, wg[:, s]), dot(x, wu[:, s])
            d = dht[slot, :, s].astype(F32)
            sig = jax.nn.sigmoid(gate)
            act = gate * sig
            for m, v in enumerate((act * up, d * up * (sig + act * (1 - sig)), d * act)):
                st[slot, m, :, s] = v.astype(BF)

        loop(F // NC, forth)
        begin(store(u, slot))
        steps(u, mids)
        mate_only = (u == 1) | (u == 3)
        halved = (u == 2) | (u > 4)
        side = jnp.where(u == 6, 0, 1)

        def back(c):
            v = dot(st[slot, 1], wg[c, :], NT) + dot(st[slot, 2], wu[c, :], NT)

            @pl.when(u == 0)
            def _():
                acc[:, c] = v

            @pl.when(mate_only)
            def _():
                stg[0, :, c] = v.astype(BF)

            @pl.when(u == 4)
            def _():
                s3[:, c] = (v + p3[:, c].astype(F32)).astype(BF)

            @pl.when(halved)
            def _():
                acc[:H, c] = v[:H]
                stg[side, H:, c] = v[H:].astype(BF)

        half = D // NB // 2
        loop(half, lambda j: back(block_rows(j, NB)))
        steps(u, lates)
        loop(D // NB, lambda j: back(block_rows(j, NB)), half)
        steps(u, posts)

    loop(count, unit)
    own_in.start()
    links.got(M5)
    links.sent(M3, R1, L1)
    end(store(count - 2, 0) + store(count - 1, 1))
    begin([frm_in, h_in, dy_in])
    end([own_in, frm_in, h_in, dy_in])

    def add(at):
        acc[at, :] += bt[0, at, :].astype(F32)
    chunked(T, 16, add)

    def last(at, total):
        stg[0, at, :] = (s3[at, :].astype(F32) + unnorm(bt[1, at, :].astype(F32), total)).astype(BF)

    finish(links, acc, frp, frn, last)
    dh_out.start()
    dh_out.wait()
    links.sent(*GATHER, R2, R3, L2, L3, M4)


def mlp(b, dhid, wg, wu, h, dy, n, cid):
    T, D = b.shape
    F = wg.shape[1]
    H = T // 2
    row, weight, halves = V((T, D), BF), V((D, F), BF), V((4, H, D), BF)
    scratch = [weight, weight, V((2, T, D), BF), V((2, T, F), BF), V((2, 3, T, F), BF), V((T, D), F32), V((2, T, D), BF), row, halves, halves, row,
               V((2, H, D), BF), row, row, DMA((COPIES,)), DMA((COPIES,)), DMA((2, 3)), DMA((2, 2)), DMA((2, 2)), DMA((2, 3, 2)), DMA((9,))]
    wide = S((n, T, F), BF)
    got = call(functools.partial(_mlp, n=n), [b, dhid, wg, wu, h, dy], [S((n, T, D), BF), wide, wide, wide, S((T, D), BF), S((T, D), F32), S((T, D), BF)],
               scratch, 8 * n * T * D * F, "mlp", cid)
    return got[:5]


def solution(mesh):
    n = mesh.shape["tp"]

    def step(x, dy, wq, wk, wv, wo, wg, wu, wd):
        x, dy = x[0], dy[0]
        blocks = lambda t: t.reshape(n, -1, t.shape[1])
        a, qkv, dy_all, dhid, heads, lse, cos, sin, h, b = front(x, dy, wq, wk, wv, wo, wd, n, 0)
        b, hid, dg, du, dh = mlp(b, dhid, wg, wu, h, dy, n, 1)
        dh_all, d_heads, by_gate, by_down = gather_fill(dh, wo, b, dg, hid, dy_all, n, 2)
        dqkv, by_gate, by_down = attend_bwd(qkv, flat(d_heads), heads, lse, cos, sin, by_gate, by_down)
        dx, by_up, *by_qkvo = land(back(blocks(dqkv), x, dh, [wq, wk, wv], b, du, a, dh_all, blocks(heads), n, 3))
        return dx[None], *by_qkvo, by_gate, by_up, by_down

    states, by_columns, by_rows = P("dp", "tp", None), P(None, "tp"), P("tp", None)
    weights = (by_columns, by_columns, by_columns, by_rows, by_columns, by_columns, by_rows)
    own = tuple(P("dp", "tp") if spec == by_columns else P(("dp", "tp"), None) for spec in weights)
    return jax.shard_map(step, mesh=mesh, in_specs=(states, states, *weights), out_specs=(states, *own), check_vma=False)
```

```python
import functools

import jax
import jax.numpy as jnp
from jax import lax
from jax.experimental import pallas as pl
from jax.experimental.pallas import tpu as pltpu
from jax.sharding import PartitionSpec as P

BF, F32 = jnp.bfloat16, jnp.float32
HEAD = 128
THETA = 10000
NEG = -1e30
HIDDEN = 2 * NEG
LOG2E = 1.4426950408889634
SCALE = HEAD**-0.5
MOST = 67_000_000
BQ = BK = 512
TILE = 512
NN, NT, TN = ((((a,), (b,)), ((), ())) for a, b in ((1, 0), (1, 1), (0, 0)))
ANY = pl.BlockSpec(memory_space=pl.ANY)
S, V, DMA = jax.ShapeDtypeStruct, pltpu.VMEM, pltpu.SemaphoreType.DMA

RA, RB, RC, RD, RE, LA, LB, LC, LD, LE, MA, MB, MC, MD, ME, MF, MG = GATHER = range(17)
R1, R2, R3, L1, L2, L3, M0, M1, M2, M3, M4, M5 = SCATTER = range(17, 29)
COPIES = 29
LO, HI = range(2)


def dot(a, b, dims=NN, **kw):
    return lax.dot_general(a, b, dims, preferred_element_type=F32, **kw)


def norm_scale(wide):
    return lax.rsqrt(jnp.mean(wide * wide, -1, keepdims=True) + 1e-6)


def unnorm(wide, d):
    scale = norm_scale(wide)
    return d * scale - wide * (scale * scale * scale * jnp.mean(d * wide, -1, keepdims=True))


def turn(t, cos, sin):
    return t * cos + pltpu.roll(t, HEAD // 2, 1) * sin


def angles(places):
    half = HEAD // 2
    a = places.astype(F32)[:, None] * THETA ** (-jnp.arange(half, dtype=F32) / half)
    cos, sin = jnp.cos(a), jnp.sin(a)
    return jnp.concatenate([cos, cos], -1), jnp.concatenate([-sin, sin], -1)


class Ring:
    def __init__(self, n):
        self.me = lax.axis_index("tp")
        core, chips = lax.rem(self.me, 2), n // 2
        chip = [lax.rem(lax.div(self.me, 2) + k, chips) for k in range(chips)]
        self.next, self.opp, self.prev = [2 * c + core for c in chip[1:]]
        self.mate, self.nextm, self.oppm, self.prevm = [2 * c + 1 - core for c in chip]

    def barrier(self):
        b = pltpu.get_barrier_semaphore()
        near = (self.next, self.prev, self.mate)
        for d in near:
            pl.semaphore_signal(b, inc=1, device_id={"tp": d}, device_id_type=pl.DeviceIdType.MESH)
        pl.semaphore_wait(b, len(near))


class Links:
    def __init__(self, ss, rs, base=0):
        self.ss, self.rs, self.base, self.made = ss, rs, base, {}

    def put(self, k, src, dst, dev):
        self.made[k] = lambda: pltpu.make_async_remote_copy(src_ref=src, dst_ref=dst, send_sem=self.ss.at[self.base + k], recv_sem=self.rs.at[self.base + k],
                                                            device_id={"tp": dev}, device_id_type=pl.DeviceIdType.MESH)

    def start(self, *ks):
        for k in ks:
            self.made[k]().start()

    def got(self, *ks):
        for k in ks:
            self.made[k]().wait_recv()

    def sent(self, *ks):
        for k in ks:
            self.made[k]().wait_send()

    def passed_on(self, *ks):
        for k in ks:
            self.got(k)
            self.start(k + 2)


def flat(t):
    return t.reshape(-1, t.shape[-1])


def begin(copies):
    for c in copies:
        c.start()


def end(copies):
    for c in copies:
        c.wait()


def pick(u, values):
    out = values[0]
    for k, v in enumerate(values):
        out = jnp.where(u == k, v, out)
    return out


def steps(u, events):
    for k, f in events.items() if isinstance(events, dict) else enumerate(events):
        def run(f=f):
            f()
        if f is not None:
            pl.when(u == k)(run)


def loop(count, f, first=0):
    def body(k, _):
        f(k)
    lax.fori_loop(first, count, body, None)


def block_rows(i, size):
    return pl.ds(pl.multiple_of(i * size, size), size)


def chunked(size, width, f):
    loop(size // width, lambda j: f(block_rows(j, width)))


def gather_copies(links, ring, src, dst, T):
    H, Q = T // 2, T // 4
    me, nx, pv, mt, opp = ring.me, ring.next, ring.prev, ring.mate, ring.opp
    for k, slot, a, rows, to in ((RA, me, 0, Q, nx), (RB, me, Q, Q, nx), (RC, pv, 0, Q, nx), (RD, pv, Q, Q, nx), (RE, me, H, H, nx),
                                 (LA, me, H, Q, pv), (LB, me, H + Q, Q, pv), (LC, nx, H, Q, pv), (LD, nx, H + Q, Q, pv), (LE, me, 0, H, pv),
                                 (MA, me, 0, T, mt), (MB, pv, 0, H, mt), (MC, nx, H, H, mt), (MD, opp, 0, H, mt), (ME, opp, H, H, mt),
                                 (MF, pv, H, H, mt), (MG, nx, 0, H, mt)):
        at = pl.ds(a, rows)
        links.put(k, src.at[at] if slot is me else dst.at[slot, at], dst.at[slot, at], to)


def whole(shard):
    return (shard, LO), (shard, HI)


def moves(u, units, far, near, sem, back=False):
    H = near.shape[0] // 2
    out = []
    for k in range(2):
        shard, half = (pick(u, [x[k][m] for x in units]) for m in range(2))
        ends = far.at[shard, pl.ds(pl.multiple_of(half * H, H), H)], near.at[pl.ds(k * H, H)]
        out.append(pltpu.make_async_copy(*(ends[::-1] if back else ends), sem.at[k]))
    return out


def rows_of_unit(u, units, k, H):
    shard, half = (pick(u, [x[k][m] for x in units]) for m in range(2))
    return pl.ds(pl.multiple_of((2 * shard + half) * H, H), H)


def stream(ring, links, src, tile, sin, dst, out, sout, work, events, schedule=range(8), beside=None):
    units = [whole(ring.me), whole(ring.mate), ((ring.prev, LO), (ring.next, HI)), ((ring.prevm, LO), (ring.nextm, HI)), whole(ring.opp),
             whole(ring.oppm), ((ring.prev, HI), (ring.next, LO)), ((ring.prevm, HI), (ring.nextm, LO))]
    fetch = lambda u, slot: moves(u, units, src, tile.at[slot], sin.at[slot])
    store = lambda u, slot: moves(u, units, dst, out.at[slot], sout.at[slot], True)
    latest = lambda k: sum(jnp.where(k < s, 0, 1) for s in schedule) - 1

    def fetch_for(k):
        u = latest(k)

        @pl.when(latest(k - 1) < u)
        def _():
            begin(fetch(u, lax.rem(u, 2)))

    fetch_for(0)

    def step(k):
        if beside is not None:
            beside(k)
        u = latest(k)

        @pl.when(latest(k - 1) < u)
        def _():
            slot = lax.rem(u, 2)
            end(fetch(u, slot))

            if dst is None:
                work(u, units, tile.at[slot])
            else:
                pl.when(u > 1)(lambda: end(store(u - 2, slot)))
                work(u, units, tile.at[slot], out.at[slot])
                begin(store(u, slot))

        steps(k, events)
        fetch_for(k + 1)

    loop(schedule[-1] + 1, step)
    if dst is not None:
        end(store(len(units) - 2, 0) + store(len(units) - 1, 1))
    links.sent(*GATHER)


class Fill:
    def __init__(self, jobs, tile, sin, sout):
        self.tile, self.sin, self.sout, self.jobs, at = tile, sin, sout, [], 0
        for srcs, fixed, out, right, ends in jobs:
            per = srcs[0].shape[2] // TILE
            self.jobs.append((at, per, srcs, fixed, out, right, ends))
            at += per * len(srcs)
        self.steps = at

    def load(self, src, j, slot):
        return pltpu.make_async_copy(src.at[:, :, block_rows(j, TILE)], self.tile.at[slot], self.sin.at[slot])

    def fetch(self, k):
        for at, per, srcs, *_ in self.jobs:
            for m, src in enumerate(srcs):
                first = at + m * per
                pl.when((k >= first) & (k < first + per))(lambda: begin([self.load(src, k - first, lax.rem(k, 2))]))

    def step(self, k):
        slot = lax.rem(k, 2)
        end([self.load(self.jobs[0][2][0], 0, slot)])
        self.fetch(k + 1)
        for at, per, srcs, fixed, out, right, ends in self.jobs:
            @pl.when((k >= at) & (k < at + per * len(srcs)))
            def _():
                which, j = lax.div(k - at, per), lax.rem(k - at, per)
                store = lambda m, j, slot: [pltpu.make_async_copy(out.at[slot, :, a], b, self.sout.at[slot, i]) for i, (a, b) in enumerate(ends[m](j))]
                pl.when(j > 1)(lambda: end(store(0, j, slot)))
                t = self.tile[slot].reshape(-1, TILE)
                f = flat(fixed[which] if len(srcs) > 1 else fixed[...])
                r = dot(f, t, TN) if right else dot(t, f, TN)
                for a in range(0, r.shape[0], TILE):
                    out[slot, :, (a if right else 0):(a if right else 0) + r.shape[1]] = r[a:a + TILE].astype(BF)
                for m in range(len(srcs)):
                    pl.when(which == m)(lambda: begin(store(m, j, slot)))
                pl.when(j == per - 1)(lambda: end(store(0, j, slot) + store(0, j, 1 - slot)))


def gather_events(links, near=None):
    def far():
        links.got(RC, RD)
        links.start(MD)
        links.got(LC, LD)
        links.start(ME)

    def last():
        links.got(RE)
        links.start(MF)
        links.got(LE)
        links.start(MG)

    got = lambda *ks: lambda: links.got(*ks)
    return [got(MA), near, got(MB, MC), far, got(MD, ME), last, got(MF, MG)]


def finish(links, acc, frp, frn, last):
    H = acc.shape[0] // 2

    def each(m, half, f):
        links.got(m)
        chunked(H, 16, lambda at: f(pl.ds(half + at.start, at.size)))

    def add(fr):
        def f(at):
            acc[at, :] += fr[at, :].astype(F32)
        return f

    each(R2, H, add(frp))
    each(L2, 0, add(frn))
    each(R3, 0, lambda at: last(at, acc[at, :] + frp[at, :].astype(F32)))
    each(L3, H, lambda at: last(at, acc[at, :] + frn[at, :].astype(F32)))


class Scatter:
    def __init__(self, ring, links, product, stg, p, s, acc, tr, fr):
        self.ring, self.links, self.product, self.stg, self.p, self.s, self.acc, self.tr, self.fr = ring, links, product, stg, p, s, acc, tr, fr
        T = acc.shape[0]
        H = T // 2
        nx, pv, mt = ring.next, ring.prev, ring.mate
        self.every, self.lo, self.hi = every, lo, hi = pl.ds(0, T), pl.ds(0, H), pl.ds(H, H)
        at = lambda ref: [ref.at[k] for k in range(ref.shape[0])]
        even, odd, pa, pb, pc, pd, so, sn, sp, on, off, fp, fn = [*at(stg), *at(p), *at(s), *at(tr), *at(fr)]
        for k, src, dst, to in ((M0, even.at[lo], pa.at[lo], mt), (M1, even.at[hi], pa.at[hi], mt), (M2, odd, pb, mt), (M3, even, pc, mt), (M4, odd, pd, mt),
                                (R1, so.at[lo], on, nx), (L1, so.at[hi], off, pv), (R2, sn.at[hi], fp.at[hi], nx), (L2, sp.at[lo], fn.at[lo], pv),
                                (R3, sn.at[lo], fp.at[lo], nx), (L3, sp.at[hi], fn.at[hi], pv)):
            links.put(k, src, dst, to)

    def send(self):
        links, ring, stg, p, s, acc = self.links, self.ring, self.stg, self.p, self.s, self.acc
        shards = (ring.oppm, ring.nextm, ring.opp, ring.prevm, ring.next, ring.prev, ring.mate, ring.me)
        got, sent, start = ((lambda f: lambda *ks: lambda: f(*ks))(f) for f in (links.got, links.sent, links.start))
        before = [None, None, got(M0, M1), sent(M0, M1), got(M2), got(M3), sent(M2), got(M4)]
        after = [start(M0, M1), start(M2), start(R1, L1), start(M3), start(R2), start(L2), start(M4)]

        def step(i):
            steps(i, before)

            def then(c, v):
                def to_mate(k):
                    def f():
                        stg[k, :, c] = v.astype(BF)
                    return f

                def to_chip(k, rows):
                    def f():
                        s[k, rows, c] = (v[rows.start:rows.start + rows.size] + p[k, rows, c].astype(F32)).astype(BF)
                    return f

                def keep():
                    acc[:, c] = v + p[3, :, c].astype(F32)

                steps(i, [to_mate(0), to_mate(1), to_chip(0, self.every), to_mate(0), to_chip(1, self.hi), to_chip(2, self.lo), to_mate(1), keep])

            self.product(pick(i, shards), self.every, then)
            steps(i, after)

        loop(len(shards), step)
        links.sent(M3, M4)

    def pass_on(self):
        H = self.lo.size

        def step(i):
            rows = block_rows(i, H)
            steps(i, [lambda: self.links.got(R1), lambda: self.links.got(L1)])

            def then(c, v):
                self.s[1 + i, rows, c] = (v + self.p[1 + i, rows, c].astype(F32) + self.tr[i, :, c].astype(F32)).astype(BF)
            self.product(pick(i, (self.ring.next, self.ring.prev)), rows, then)
            steps(i, [lambda: self.links.start(R3), lambda: self.links.start(L3)])

        loop(2, step)

    def finish(self, last):
        self.links.sent(R1, L1)
        finish(self.links, self.acc, self.fr.at[0], self.fr.at[1], last)


def scatter_scratch(T, D):
    return [V((2, T, D), BF), V((4, T, D), BF), V((3, T, D), BF), V((T, D), F32), V((2, T // 2, D), BF), V((2, T, D), BF)]


def call(body, args, outs, scratch, flops, name, cid=None):
    return pl.pallas_call(
        body, in_specs=[ANY] * len(args), out_specs=[ANY] * len(outs), out_shape=outs, scratch_shapes=scratch, name=name,
        compiler_params=pltpu.CompilerParams(collective_id=cid, has_side_effects=True, vmem_limit_bytes=MOST),
        cost_estimate=pl.CostEstimate(flops=flops, bytes_accessed=sum(t.size for t in (*args, *outs)), transcendentals=0),
    )(*args)


def rows_of(t):
    return jnp.concatenate([t[:, a:a + HEAD] for a in range(0, t.shape[1], HEAD)], axis=0)


def set_gap(gap):
    gap[...] = lax.broadcasted_iota(jnp.int32, gap.shape, 1) - lax.broadcasted_iota(jnp.int32, gap.shape, 0)


def key_blocks(iq, block):
    seen = lax.div(iq * BQ + 1, BK)
    loop(seen, lambda j: block(j, False))
    loop(lax.div((iq + 1) * BQ + BK - 1, BK), lambda j: block(j, True), seen)


def attend_block(iq, qkv, o_ref, lse_ref, qs, top, mix, gap):
    NQ = o_ref.shape[1]
    cols = qs.shape[0]
    mine = block_rows(iq, BQ)
    qs[...] = rows_of(qkv[mine, :NQ])
    top[...] = jnp.full_like(top, NEG)
    mix[...] = jnp.zeros_like(mix)
    ones = jnp.ones((8, BK), BF)
    strips = [slice(a, a + BQ) for a in range(0, cols, BQ)]

    def block(j, masked):
        here = block_rows(j, BK)
        keys = qkv[here, NQ:NQ + HEAD]
        values = jnp.concatenate([qkv[here, NQ + HEAD:].T, ones], axis=0)
        scores = [dot(keys, qs[at, :], NT) for at in strips]
        ps, keeps = [], []
        for at, s in zip(strips, scores):
            if masked:
                s = jnp.where(gap[...] >= j * BK - iq * BQ, s, HIDDEN)
            old = top[:, at]
            new = jnp.maximum(old, s.max(axis=0, keepdims=True))
            top[:, at] = new
            ps.append(jnp.exp2((s - new) * (SCALE * LOG2E)).astype(BF))
            keeps.append(jnp.exp2((old - new) * (SCALE * LOG2E)))
        for at, p, keep in zip(strips, ps, keeps):
            mix[:, at] = mix[:, at] * keep + dot(values, p)

    key_blocks(iq, block)
    total = mix[HEAD:HEAD + 1, :]
    out = (mix[:HEAD, :] * (1 / total)).T.astype(BF)
    for h in range(NQ // HEAD):
        o_ref[mine, h * HEAD:(h + 1) * HEAD] = out[h * BQ:(h + 1) * BQ]
    lse_ref[iq] = top[...] * SCALE + jnp.log(total)


def _attend_bwd(qkv_ref, do_ref, o_ref, lse_ref, cos_ref, sin_ref, *refs):
    ins, (out_ref, *outs), (qs, dos, dq, dk, dv, gap, *tiles, sem) = refs[:3], refs[3:7], refs[7:]
    NQ = do_ref.shape[1]
    tokens, cols = dk.shape[0], qs.shape[0]
    iq = pl.program_id(0)
    mine = block_rows(iq, BQ)
    come, go = [[pltpu.make_async_copy(x, y, sem.at[k]) for k, (x, y) in enumerate(zip(*ends))] for ends in ((ins, tiles), (tiles, outs))]

    def landed(*ks):
        def f():
            for k in ks:
                come[k].wait()
                go[k].start()
        return f

    steps(iq, [lambda: begin(come), landed(0), landed(1, 2)])
    qs[...] = rows_of(qkv_ref[mine, :NQ])
    dos[...] = rows_of(do_ref)
    dq[...] = jnp.zeros_like(dq)

    @pl.when(iq == 0)
    def _():
        set_gap(gap)
        dk[...] = jnp.zeros_like(dk)
        dv[...] = jnp.zeros_like(dv)

    delta = dot(jnp.ones((8, HEAD), F32), dos[...].astype(F32) * rows_of(o_ref).astype(F32), NT, precision=lax.Precision.HIGHEST)[:1]
    lse = lse_ref[0] * LOG2E
    strips = [slice(a, a + BQ) for a in range(0, cols, BQ)]

    def block(j, masked):
        here = block_rows(j, BK)
        keys, values = qkv_ref[here, NQ:NQ + HEAD], qkv_ref[here, NQ + HEAD:]
        scores = [dot(keys, qs[at, :], NT) for at in strips]
        dps = [dot(values, dos[at, :], NT) for at in strips]
        for at, s, dp in zip(strips, scores, dps):
            p = jnp.exp2(s * (SCALE * LOG2E) - lse[:, at])
            if masked:
                p = jnp.where(gap[...] >= j * BK - iq * BQ, p, 0.0)
            ds = (p * (dp - delta[:, at])).astype(BF)
            dv[here, :] += dot(p.astype(BF), dos[at, :])
            dk[here, :] += dot(ds, qs[at, :])
            dq[:, at] += dot(keys.T, ds)

    key_blocks(iq, block)
    back = (dq[...] * SCALE).T
    for h in range(NQ // HEAD):
        out_ref[mine, h * HEAD:(h + 1) * HEAD] = turn(back[h * BQ:(h + 1) * BQ], cos_ref[mine, :], -sin_ref[mine, :]).astype(BF)

    @pl.when(iq == pl.num_programs(0) - 1)
    def _():
        end(go)

        def rest(at):
            out_ref[at, NQ:NQ + HEAD] = turn(dk[at, :] * SCALE, cos_ref[at, :], -sin_ref[at, :]).astype(BF)
            out_ref[at, NQ + HEAD:] = dv[at, :].astype(BF)
        chunked(tokens, BQ, rest)


def attend_bwd(qkv, d_out, out, lse, cos, sin, others):
    tokens, NQ = out.shape
    cols = lse.shape[2]
    part = pl.BlockSpec((BQ, NQ), lambda i: (i, 0))
    all_of = lambda t, **kw: pl.BlockSpec(t.shape, lambda i: (0, 0), **kw)
    once = pl.Buffered(1)
    return pl.pallas_call(
        _attend_bwd, grid=(tokens // BQ,), name="attend_bwd",
        in_specs=[all_of(qkv, pipeline_mode=once), part, part, pl.BlockSpec((1, 1, cols), lambda i: (i, 0, 0)), all_of(cos, pipeline_mode=once),
                  all_of(sin, pipeline_mode=once), *[ANY] * len(others)],
        out_specs=[all_of(qkv), *[ANY] * len(others)], out_shape=[S(t.shape, BF) for t in (qkv, *others)],
        scratch_shapes=[V((cols, HEAD), BF), V((cols, HEAD), BF), V((HEAD, cols), F32), V((tokens, HEAD), F32), V((tokens, HEAD), F32), V((BK, BQ), jnp.int32),
                        *(V(t.shape, BF) for t in others), DMA((len(others),))],
        compiler_params=pltpu.CompilerParams(vmem_limit_bytes=MOST),
        cost_estimate=pl.CostEstimate(flops=5 * tokens * tokens * NQ, bytes_accessed=8 * qkv.size, transcendentals=tokens * cols),
    )(qkv, d_out, out, lse, cos, sin, *others)


def _front(x_ref, dy_ref, wq_ref, wk_ref, wv_ref, wo_ref, wd_ref, c_ref, s_ref, a_all, qkv_ref, dy_all, dhid, o_ref, lse_ref, cos_ref, sin_ref, h_ref, b_ref,
           an, tile, small, qkv, o, lse, qs, top, mix, gap, wo, dt, stg, p, s, acc, tr, fr, ss, rs, sb, so, sl, *, n):
    T, D = x_ref.shape
    NQ, NK = wq_ref.shape[1], wk_ref.shape[1]
    turned, Q = NQ + NK, T // 4

    def links():
        ring = Ring(n)
        of_a, of_dy, of_o = (Links(ss, rs, k * COPIES) for k in range(3))
        gather_copies(of_a, ring, an, a_all, T)
        gather_copies(of_dy, ring, dy_ref, dy_all, T)
        return ring, of_a, of_dy, of_o

    pairs = ((x_ref, stg.at[0]), (dy_ref, stg.at[1]), (c_ref, small.at[0]), (s_ref, small.at[1]), (wo_ref, wo),
             (x_ref, stg.at[0]), (qkv, qkv_ref), (o, o_ref), (lse, lse_ref), (s.at[0], h_ref), (stg.at[1], b_ref))
    copies = [pltpu.make_async_copy(a, b, sl.at[k]) for k, (a, b) in enumerate(pairs)]
    x_in, dy_in, c_in, s_in, wo_in, x_again, *outs = copies
    x_in.start()

    def products(w, cos, sin):
        tables = [pltpu.make_async_copy(a, b, so.at[0, k]) for k, (a, b) in enumerate(((cos, cos_ref), (sin, sin_ref)))]
        ring, of_a, of_dy, _ = links()
        keep, keep_dy = (pltpu.make_async_copy(a, b.at[ring.me], so.at[1, k]) for k, (a, b) in enumerate(((an, a_all), (stg.at[1], dy_all))))
        place = [pl.ds(0, NQ), pl.ds(NQ, NK), pl.ds(turned, NK)]
        loads = [dy_in, c_in, s_in, wo_in] + [pltpu.make_async_copy(r, w.at[:, c], sb.at[0, k]) for k, (r, c) in enumerate(zip((wq_ref, wk_ref, wv_ref), place))]
        begin(loads)
        ring.barrier()
        x_in.wait()
        for q, k in ((0, RA), (2, LA), (1, RB), (3, LB)):

            def norm(at):
                at = pl.ds(q * Q + at.start, at.size)
                wide = stg[0, at, :].astype(F32)
                an[at, :] = (wide * norm_scale(wide)).astype(BF)
            chunked(Q, 16, norm)
            of_a.start(k)
        of_a.start(MA)
        keep.start()
        end(loads)
        keep_dy.start()

        def table(at):
            row = pl.ds(HEAD + lax.div(at.start, HEAD), 1)
            c0, s0, c1, s1 = small[0, row, :], small[1, row, :], small[0, :HEAD, :], small[1, :HEAD, :]
            cos[at, :] = c0 * c1 - s0 * s1
            sin[at, :] = s0 * c1 + c0 * s1
        chunked(n * T, HEAD, table)
        begin(tables)
        end([keep, keep_dy])

        def work(u, units, x):
            r = dot(x[...], w[...]).astype(BF)
            for k in range(2):
                rows = slice(k * T // 2, (k + 1) * T // 2)
                place = rows_of_unit(u, units, k, T // 2)
                c, s = cos[place, :], sin[place, :]
                for a in range(0, turned, HEAD):
                    qkv[place, a:a + HEAD] = turn(r[rows, a:a + HEAD].astype(F32), c, s).astype(BF)
                qkv[place, turned:] = r[rows, turned:]

        def near():
            of_a.passed_on(RA, LA, RB, LB)
            of_a.start(RE, LE, MB, MC)
            of_dy.start(RA, LA, RB, LB, MA)

        stream(ring, of_a, a_all, tile, sb, None, None, None, work, gather_events(of_a, near))
        end(tables)

    pl.run_scoped(products, V((D, turned + NK), BF), *[V((n * T, HEAD), F32)] * 2)
    outs[0].start()
    set_gap(gap)

    def rest(wd):
        ring, _, of_dy, of_o = links()
        wd_in = pltpu.make_async_copy(wd_ref, wd, so.at[0, 0])
        wd_in.start()
        blocks = n * T // BQ

        def attention(iq):
            attend_block(iq, qkv, o, lse, qs, top, mix, gap)
            steps(iq, {blocks - 2: lambda: of_dy.passed_on(RA, LA)})

        loop(blocks, attention)
        begin(outs[1:3])
        of_dy.passed_on(RB, LB)
        of_dy.start(RE, LE, MB, MC)

        def product(shard, rows, then):
            at = pl.ds(pl.multiple_of(shard * T + rows.start, T // 2), rows.size)
            chunked(D, D // 4, lambda c: then(c, dot(o[at, :], wo[:, c])))

        scatter = Scatter(ring, of_o, product, stg, p, s, acc, tr, fr)
        scatter.send()
        x_again.start()
        wd_in.wait()

        def work(u, units, x, o):
            def run(c):
                o[:, c] = dot(x[...], wd[c, :], NT).astype(BF)
            chunked(wd.shape[0], TILE, run)

        stream(ring, of_dy, dy_all, tile, sb, dhid, dt, so, work, gather_events(of_dy))
        scatter.pass_on()
        x_again.wait()

        def last(at, total):
            h = (stg[0, at, :].astype(F32) + total).astype(BF)
            s[0, at, :] = h
            h = h.astype(F32)
            stg[1, at, :] = (h * norm_scale(h)).astype(BF)

        scatter.finish(last)
        begin(outs[3:])
        end(outs)
        of_o.sent(R2, L2, R3, L3)

    pl.run_scoped(rest, V(wd_ref.shape, BF))


def front(x, dy, wq, wk, wv, wo, wd, n, cid):
    T, D = x.shape
    NQ, F, tokens = wo.shape[0], wd.shape[0], n * T
    N, cols = NQ + 2 * HEAD, NQ // HEAD * BQ
    stat = (tokens // BQ, 1, cols)
    table, row = S((tokens, HEAD), F32), S((T, D), BF)
    small = angles(jnp.concatenate([jnp.arange(HEAD), jnp.arange(0, tokens, HEAD)]))
    outs = [S((n, T, D), BF), S((tokens, N), BF), S((n, T, D), BF), S((n, T, F), BF), S((tokens, NQ), BF), S(stat, F32), table, table, row, row]
    scratch = [V((T, D), BF), V((2, T, D), BF), V((2, *small[0].shape), F32), V((tokens, N), BF), V((tokens, NQ), BF),
               V(stat, F32), V((cols, HEAD), BF), V((1, cols), F32), V((HEAD + 8, cols), F32), V((BK, BQ), jnp.int32), V((NQ, D), BF), V((2, T, F), BF),
               *scatter_scratch(T, D), DMA((3 * COPIES,)), DMA((3 * COPIES,)), DMA((2, 3)), DMA((2, 3)), DMA((15,))]
    return call(functools.partial(_front, n=n), [x, dy, wq, wk, wv, wo, wd, *small], outs, scratch, 2 * tokens * D * (N + F + NQ), "front", cid)


def _back(t_ref, x_ref, wq_ref, wk_ref, wv_ref, a_ref, dh_all, heads_ref, dx_ref, by_q, by_k, by_v, by_o,
          w, t, heads, out, ft, stg, p, s, acc, tr, fr, ss, rs, sl, sf, sg, *, n):
    ring, links = Ring(n), Links(ss, rs)
    T, D = x_ref.shape
    NQ, NK = wq_ref.shape[1], wk_ref.shape[1]
    columns = [pl.ds(0, NQ), pl.ds(NQ, NK), pl.ds(NQ + NK, NK)]
    pairs = ((t_ref, t), *((r, w.at[:, c]) for r, c in zip((wq_ref, wk_ref, wv_ref), columns)), (heads_ref, heads), (x_ref, stg.at[0]), (dh_all.at[ring.me], stg.at[1]),
             (s.at[0], dx_ref))
    *first, heads_in, x_in, dh_in, dx_out = [pltpu.make_async_copy(a, b, sl.at[k]) for k, (a, b) in enumerate(pairs)]
    begin([*first, heads_in])
    ring.barrier()
    end(first)

    def product(shard, rows, then):
        chunked(D, D // 4, lambda c: then(c, dot(t[shard, rows, :], w[c, :], NT)))

    scatter = Scatter(ring, links, product, stg, p, s, acc, tr, fr)
    scatter.send()
    begin([x_in, dh_in])
    heads_in.wait()
    fill = Fill((([a_ref], t, out, False, [lambda j: [(c, r.at[block_rows(j, TILE)]) for c, r in zip(columns, (by_q, by_k, by_v))]]),
                 ([dh_all], heads, out, True, [lambda j: [(pl.ds(0, TILE), by_o.at[:, block_rows(j, TILE)])]])), ft, sf, sg)
    fill.fetch(0)

    def beside(k):
        fill.step(k)
        steps(k, {6: scatter.pass_on})
    loop(fill.steps, beside)
    end([x_in, dh_in])

    def last(at, total):
        s[0, at, :] = (stg[1, at, :].astype(F32) + unnorm(stg[0, at, :].astype(F32), total)).astype(BF)

    scatter.finish(last)
    dx_out.start()
    dx_out.wait()
    links.sent(R2, L2, R3, L3)


def back(dqkv, x, ws, a, dh_all, heads, n, cid):
    T, D = x.shape
    K, NQ = dqkv.shape[2], heads.shape[2]
    scratch = [V((D, K), BF), V(dqkv.shape, BF), V(heads.shape, BF), V((2, TILE, K), BF), V((2, n, T, TILE), BF), *scatter_scratch(T, D),
               DMA((COPIES,)), DMA((COPIES,)), DMA((8,)), DMA((2,)), DMA((2, 3))]
    outs = [S((T, D), BF), *(S(w.shape, BF) for w in ws), S((NQ, D), BF)]
    return call(functools.partial(_back, n=n), [dqkv, x, *ws, a, dh_all, heads], outs, scratch, 6 * n * T * D * K, "back", cid)


def _land(*refs):
    m = len(refs) // 3
    ins, outs, tiles, sem = refs[:m], refs[m:2 * m], refs[2 * m:-1], refs[-1]
    come = [pltpu.make_async_copy(a, b, sem.at[k]) for k, (a, b) in enumerate(zip(ins, tiles))]
    go = [pltpu.make_async_copy(a, b, sem.at[k]) for k, (a, b) in enumerate(zip(tiles, outs))]
    begin(come)
    for a, b in zip(come, go):
        a.wait()
        b.start()
    end(go)


def land(arrays):
    shapes = [S(t.shape, BF) for t in arrays]
    return call(_land, arrays, shapes, [*(V(t.shape, BF) for t in arrays), DMA((len(arrays),))], 0, "land")


def mlp_links(b_ref, bg, frm, stg, s3, s1, p1, p3, tr, frp, frn, ss, rs, n):
    ring, links = Ring(n), Links(ss, rs)
    T = b_ref.shape[0]
    H = T // 2
    nx, pv, mt = ring.next, ring.prev, ring.mate
    lo, hi = pl.ds(0, H), pl.ds(H, H)
    gather_copies(links, ring, b_ref, bg, T)
    at = lambda ref: [ref.at[k] for k in range(ref.shape[0])]
    pa, pb, pc, pd, sa, sb1, sc, sd1, even, odd, on, off = [*at(p1), *at(s1), *at(stg), *at(tr)]
    for k, src, dst, to in ((M5, even, frm, mt), (M0, odd.at[hi], pa, mt), (M1, even, p3, mt), (M2, odd.at[hi], pb, mt), (M3, even.at[hi], pc, mt), (M4, odd.at[hi], pd, mt),
                            (R1, s3.at[lo], on, nx), (L1, s3.at[hi], off, pv), (R2, sb1, frp.at[hi], nx), (L2, sa, frn.at[lo], pv),
                            (R3, sc, frp.at[lo], nx), (L3, sd1, frn.at[hi], pv)):
        links.put(k, src, dst, to)
    return ring, links


def pair_sum(acc, p1, s1, tr, k, more=None):
    def add(at):
        v = acc[at, :] + p1[k, at, :].astype(F32)
        if more is not None:
            v = v + tr[more, at, :].astype(F32)
        s1[k, at, :] = v.astype(BF)
    chunked(s1.shape[1], 16, add)


def _units(b_ref, dhid_ref, wg_ref, wu_ref, bg, hid, dgo, duo, own, frm, bt, acc, stg, s3, s1, p1, p3, tr, frp, frn, ss, rs, sw, sb, sd, so, sl, n, wg, wu, dht, st):
    ring, links = mlp_links(b_ref, bg, frm, stg, s3, s1, p1, p3, tr, frp, frn, ss, rs, n)
    T, D = b_ref.shape
    F = wg_ref.shape[1]
    H, NC, NB = T // 2, F // 3, D // 4
    me, nx, pv, mt = ring.me, ring.next, ring.prev, ring.mate
    units = [whole(me), whole(mt), ((pv, LO), (ring.prevm, LO)), whole(ring.oppm), whole(ring.opp), ((nx, HI), (ring.nextm, HI)),
             ((nx, LO), (ring.nextm, LO)), ((pv, HI), (ring.prevm, HI))]
    count = len(units)

    def fetch(u, slot):
        return moves(u, units, bg, bt.at[slot], sb.at[slot]) + moves(u, units, dhid_ref, dht.at[slot], sd.at[slot])

    def fetching(u):
        return lambda: begin(fetch(u, u % 2))

    def store(u):
        return [c for m, ref in enumerate((hid, dgo, duo)) for c in moves(u, units, ref, st.at[m], so.at[m], True)]

    def weights(j):
        s = block_rows(j, NC)
        return [pltpu.make_async_copy(a.at[:, s], b.at[:, s], sw.at[k, j]) for k, (a, b) in enumerate(((wg_ref, wg), (wu_ref, wu)))]

    pairs = ((b_ref, bt.at[0]), (dhid_ref.at[me], dht.at[0]), (bt.at[0], bg.at[me]), (acc, own))
    *first, keep, own_out = [pltpu.make_async_copy(a, b, sl.at[k]) for k, (a, b) in enumerate(pairs)]
    begin(first)
    for j in range(F // NC):
        begin(weights(j))
    ring.barrier()
    links.start(RA, LA, RB, LB, MA)
    end(first)
    keep.start()

    pair = functools.partial(pair_sum, acc, p1, s1, tr)

    def mid0():
        keep.wait()
        links.passed_on(RA, LA)
        links.got(MA)
        begin(fetch(1, 1))

    def mid1():
        links.passed_on(RB)
        links.start(RE)
        links.passed_on(LB)
        links.start(LE, MB, MC)
        own_out.start()

    def mid3():
        links.got(M0)
        pair(0)
        links.start(L2)
        links.sent(M5)

    def mid6():
        links.got(M2)
        pair(1)
        links.start(R2)
        links.sent(M1)

    def mid7():
        links.got(M3, R1)
        pair(2, 0)
        links.start(R3)
        links.sent(M2)

    def late1():
        links.got(MB)
        begin(fetch(2, 0))

    def late2():
        links.got(RC, RD)
        links.start(MD)
        links.got(LC, LD)
        links.start(ME)

    def late4():
        links.got(MC)
        begin(fetch(5, 1))
        links.got(LE)
        links.start(MG)
        links.got(RE)
        links.start(MF)

    def late5():
        links.got(MG)
        begin(fetch(6, 0))

    def late6():
        links.got(MF)
        begin(fetch(7, 1))

    def post2():
        links.start(M0)
        links.got(MD, ME)
        begin(fetch(3, 1))

    starting = lambda *ks: lambda: links.start(*ks)
    mids = [mid0, mid1, own_out.wait, mid3, lambda: links.got(M1), lambda: links.sent(M0), mid6, mid7]
    lates = [None, late1, late2, fetching(4), late4, late5, late6]
    posts = [None, starting(M5), post2, starting(M1), starting(R1, L1), starting(M2), starting(M3), starting(M4)]

    def unit(u):
        slot = lax.rem(u, 2)

        @pl.when(u > 0)
        def _():
            end(fetch(u, slot))
            end(store(u - 1))

        def forth(j):
            @pl.when(u == 0)
            def _():
                end(weights(j))
            s = block_rows(j, NC)
            x = bt[slot]
            gate, up = dot(x, wg[:, s]), dot(x, wu[:, s])
            d = dht[slot, :, s].astype(F32)
            sig = jax.nn.sigmoid(gate)
            act = gate * sig
            for m, v in enumerate((act * up, d * up * (sig + act * (1 - sig)), d * act)):
                st[m, :, s] = v.astype(BF)

        loop(F // NC, forth)
        begin(store(u))
        steps(u, mids)
        mate_only = (u == 1) | (u == 3)
        halved = (u == 2) | (u > 4)
        side = jnp.where(u == 6, 0, 1)

        def back(c):
            v = dot(st[1], wg[c, :], NT) + dot(st[2], wu[c, :], NT)

            @pl.when(u == 0)
            def _():
                acc[:, c] = v

            @pl.when(mate_only)
            def _():
                stg[0, :, c] = v.astype(BF)

            @pl.when(u == 4)
            def _():
                s3[:, c] = (v + p3[:, c].astype(F32)).astype(BF)

            @pl.when(halved)
            def _():
                acc[:H, c] = v[:H]
                stg[side, H:, c] = v[H:].astype(BF)

        half = D // NB // 2
        loop(half, lambda j: back(block_rows(j, NB)))
        steps(u, lates)
        loop(D // NB, lambda j: back(block_rows(j, NB)), half)
        steps(u, posts)

    loop(count, unit)
    end(store(count - 1))


def _middle(b_ref, dhid_ref, wg_ref, wu_ref, h_ref, dy_ref, wo_ref, dy_all, bg, hid, dgo, duo, dh_all, out, by_down, by_gate, by_up, own, frm,
            bt, acc, stg, s3, s1, p1, p3, tr, frp, frn, ot, ss, rs, sw, sb, sd, so, sl, sf, sg, *, n):
    T, D = b_ref.shape
    F, NQ = wg_ref.shape[1], wo_ref.shape[0]
    shared = (bt, acc, stg, s3, s1, p1, p3, tr, frp, frn, ss, rs)
    pl.run_scoped(functools.partial(_units, b_ref, dhid_ref, wg_ref, wu_ref, bg, hid, dgo, duo, own, frm, *shared, sw, sb, sd, so, sl, n),
                  V((D, F), BF), V((D, F), BF), V((2, T, F), BF), V((3, T, F), BF))

    def rest(fixed, left, tile, wo):
        ring, links = mlp_links(b_ref, bg, frm, *shared[2:], n)
        of_dh = Links(ss, rs, COPIES)
        gather_copies(of_dh, ring, stg.at[0], dh_all, T)
        pairs = ((hid, fixed.at[1]), (dgo, fixed.at[0]), (duo, fixed.at[1]), (wo_ref, wo), (own, acc), (frm, bt.at[0]), (h_ref, bt.at[1]), (dy_ref, s3),
                 (stg.at[0], dh_all.at[ring.me]))
        hid_in, dg_in, du_in, wo_in, own_in, *rows_in, keep = [pltpu.make_async_copy(a, b, sl.at[k]) for k, (a, b) in enumerate(pairs)]
        side = lambda ref: lambda j: [(pl.ds(0, F), ref.at[block_rows(j, TILE)])]
        fill = Fill((([dy_all], fixed.at[1], left, True, [lambda j: [(pl.ds(a, TILE), by_down.at[pl.ds(a, TILE), block_rows(j, TILE)]) for a in range(0, F, TILE)]]),
                     ([bg, bg], fixed, left, False, [side(by_gate), side(by_up)])), tile, sf, sg)
        hid_in.start()
        fill.fetch(0)
        begin([dg_in, wo_in])
        links.got(M4, L1)
        pair_sum(acc, p1, s1, tr, 3, 1)
        links.start(L3)
        own_in.start()
        links.got(M5)
        links.sent(M3, R1, L1)
        begin(rows_in)
        hid_in.wait()

        def scattered():
            end([dg_in, wo_in, own_in, *rows_in])

            def add(at):
                acc[at, :] += bt[0, at, :].astype(F32)
            chunked(T, 16, add)

            def last(at, total):
                stg[0, at, :] = (s3[at, :].astype(F32) + unnorm(bt[1, at, :].astype(F32), total)).astype(BF)

            finish(links, acc, frp, frn, last)
            of_dh.start(RA, LA, RB, LB, MA)
            keep.start()

        def near():
            of_dh.passed_on(RB, LB)
            of_dh.start(RE, LE, MB, MC)

        def work(u, units, x, o):
            o[...] = dot(x[...], wo[...], NT).astype(BF)

        mate, _, mates, far, fars, last, lasts = gather_events(of_dh)
        events = {5: scattered, 7: du_in.start, 8: lambda: (mate(), keep.wait(), of_dh.passed_on(RA, LA)), 11: near, 13: mates, 15: du_in.wait, 17: far, 18: fars, 22: last, 23: lasts}
        schedule = (9, 10, 14, 15, 19, 20, fill.steps - 1, fill.steps)
        stream(ring, of_dh, dh_all, bt, sb, out, ot, sd, work, events, schedule, lambda k: pl.when(k < fill.steps)(lambda: fill.step(k)))
        links.sent(*GATHER, R2, R3, L2, L3, M4)

    pl.run_scoped(rest, V((2, n, T, F), BF), V((2, TILE, F), BF), V((2, n, T, TILE), BF), V((NQ, D), BF))


def middle(b, dhid, wg, wu, h, dy, wo, dy_all, n, cid):
    T, D = b.shape
    F, NQ = wg.shape[1], wo.shape[0]
    H = T // 2
    row, halves = V((T, D), BF), V((4, H, D), BF)
    scratch = [V((2, T, D), BF), V((T, D), F32), V((2, T, D), BF), row, halves, halves, row, V((2, H, D), BF), row, row, V((2, T, NQ), BF),
               DMA((2 * COPIES,)), DMA((2 * COPIES,)), DMA((2, 3)), DMA((2, 2)), DMA((2, 2)), DMA((3, 2)), DMA((9,)), DMA((2,)), DMA((2, 3))]
    wide, full, narrow = S((n, T, F), BF), S((n, T, D), BF), S((D, F), BF)
    outs = [full, wide, wide, wide, full, S((n, T, NQ), BF), S((F, D), BF), narrow, narrow, S((T, D), F32), S((T, D), BF)]
    got = call(functools.partial(_middle, n=n), [b, dhid, wg, wu, h, dy, wo, dy_all], outs, scratch, 14 * n * T * D * F, "middle", cid)
    return got[4:9]


def solution(mesh):
    n = mesh.shape["tp"]

    def step(x, dy, wq, wk, wv, wo, wg, wu, wd):
        x, dy = x[0], dy[0]
        blocks = lambda t: t.reshape(n, -1, t.shape[1])
        a, qkv, dy_all, dhid, heads, lse, cos, sin, h, b = front(x, dy, wq, wk, wv, wo, wd, n, 0)
        dh_all, d_heads, *by_mlp = middle(b, dhid, wg, wu, h, dy, wo, dy_all, n, 1)
        dqkv, by_down, by_gate, by_up = attend_bwd(qkv, flat(d_heads), heads, lse, cos, sin, by_mlp)
        dx, *by_qkvo = land(back(blocks(dqkv), x, [wq, wk, wv], a, dh_all, blocks(heads), n, 2))
        return dx[None], *by_qkvo, by_gate, by_up, by_down

    states, by_columns, by_rows = P("dp", "tp", None), P(None, "tp"), P("tp", None)
    weights = (by_columns, by_columns, by_columns, by_rows, by_columns, by_columns, by_rows)
    own = tuple(P("dp", "tp") if spec == by_columns else P(("dp", "tp"), None) for spec in weights)
    return jax.shard_map(step, mesh=mesh, in_specs=(states, states, *weights), out_specs=(states, *own), check_vma=False)
```

```python
import functools

import jax
import jax.numpy as jnp
from jax import lax
from jax.experimental import pallas as pl
from jax.experimental.pallas import tpu as pltpu
from jax.sharding import PartitionSpec as P

BF, F32 = jnp.bfloat16, jnp.float32
HEAD = 128
THETA = 10000
NEG = -1e30
HIDDEN = 2 * NEG
LOG2E = 1.4426950408889634
SCALE = HEAD**-0.5
MOST = 67_000_000
BQ = BK = 512
TILE = 512
EARLY = 4
NN, NT, TN = ((((a,), (b,)), ((), ())) for a, b in ((1, 0), (1, 1), (0, 0)))
ANY = pl.BlockSpec(memory_space=pl.ANY)
S, V, DMA = jax.ShapeDtypeStruct, pltpu.VMEM, pltpu.SemaphoreType.DMA

RA, RB, RC, RD, RE, LA, LB, LC, LD, LE, MA, MB, MC, MD, ME, MF, MG = GATHER = range(17)
R1, R2, R3, R4, L1, L2, L3, L4, M0, M1, M2, M3, M4, M5, M6, M7 = range(17, 33)
COPIES = 33
RUNS = 4
LO, HI = range(2)


def dot(a, b, dims=NN, **kw):
    return lax.dot_general(a, b, dims, preferred_element_type=F32, **kw)


def norm_scale(wide):
    return lax.rsqrt(jnp.mean(wide * wide, -1, keepdims=True) + 1e-6)


def unnorm(wide, d):
    scale = norm_scale(wide)
    return d * scale - wide * (scale * scale * scale * jnp.mean(d * wide, -1, keepdims=True))


def turn(t, cos, sin):
    return t * cos + pltpu.roll(t, HEAD // 2, 1) * sin


def angles(places):
    half = HEAD // 2
    a = places.astype(F32)[:, None] * THETA ** (-jnp.arange(half, dtype=F32) / half)
    cos, sin = jnp.cos(a), jnp.sin(a)
    return jnp.concatenate([cos, cos], -1), jnp.concatenate([-sin, sin], -1)


class Ring:
    def __init__(self, n):
        self.me = lax.axis_index("tp")
        core, chips = lax.rem(self.me, 2), n // 2
        chip = [lax.rem(lax.div(self.me, 2) + k, chips) for k in range(chips)]
        self.next, self.opp, self.prev = [2 * c + core for c in chip[1:]]
        self.mate, self.nextm, self.oppm, self.prevm = [2 * c + 1 - core for c in chip]

    def barrier(self):
        b = pltpu.get_barrier_semaphore()
        near = (self.next, self.prev, self.mate)
        for d in near:
            pl.semaphore_signal(b, inc=1, device_id={"tp": d}, device_id_type=pl.DeviceIdType.MESH)
        pl.semaphore_wait(b, len(near))


class Links:
    def __init__(self, ss, rs, base=0):
        self.ss, self.rs, self.base, self.made = ss, rs, base, {}

    def put(self, k, src, dst, dev):
        self.made[k] = lambda: pltpu.make_async_remote_copy(src_ref=src, dst_ref=dst, send_sem=self.ss.at[self.base + k], recv_sem=self.rs.at[self.base + k],
                                                            device_id={"tp": dev}, device_id_type=pl.DeviceIdType.MESH)

    def start(self, *ks):
        for k in ks:
            self.made[k]().start()

    def got(self, *ks):
        for k in ks:
            self.made[k]().wait_recv()

    def sent(self, *ks):
        for k in ks:
            self.made[k]().wait_send()

    def passed_on(self, *ks):
        for k in ks:
            self.got(k)
            self.start(k + 2)


def flat(t):
    return t.reshape(-1, t.shape[-1])


def begin(copies):
    for c in copies:
        c.start()


def end(copies):
    for c in copies:
        c.wait()


def pick(u, values):
    out = values[0]
    for k, v in enumerate(values):
        out = jnp.where(u == k, v, out)
    return out


def steps(u, events):
    for k, f in events.items() if isinstance(events, dict) else enumerate(events):
        def run(f=f):
            f()
        if f is not None:
            pl.when(u == k)(run)


def loop(count, f, first=0):
    def body(k, _):
        f(k)
    lax.fori_loop(first, count, body, None)


def block_rows(i, size):
    return pl.ds(pl.multiple_of(i * size, size), size)


def chunked(size, width, f):
    loop(size // width, lambda j: f(block_rows(j, width)))


def gather_copies(links, ring, src, dst, T):
    H, Q = T // 2, T // 4
    me, nx, pv, mt, opp = ring.me, ring.next, ring.prev, ring.mate, ring.opp
    for k, slot, a, rows, to in ((RA, me, 0, Q, nx), (RB, me, Q, Q, nx), (RC, pv, 0, Q, nx), (RD, pv, Q, Q, nx), (RE, me, H, H, nx),
                                 (LA, me, H, Q, pv), (LB, me, H + Q, Q, pv), (LC, nx, H, Q, pv), (LD, nx, H + Q, Q, pv), (LE, me, 0, H, pv),
                                 (MA, me, 0, T, mt), (MB, pv, 0, H, mt), (MC, nx, H, H, mt), (MD, opp, 0, H, mt), (ME, opp, H, H, mt),
                                 (MF, pv, H, H, mt), (MG, nx, 0, H, mt)):
        at = pl.ds(a, rows)
        links.put(k, src.at[at] if slot is me else dst.at[slot, at], dst.at[slot, at], to)


def whole(shard):
    return (shard, LO), (shard, HI)


def moves(u, units, far, near, sem, back=False):
    parts = len(units[0])
    size = near.shape[0] // parts
    out = []
    for k in range(parts):
        shard, place = (pick(u, [x[k][m] for x in units]) for m in range(2))
        ends = far.at[shard, block_rows(place, size)], near.at[pl.ds(k * size, size)]
        out.append(pltpu.make_async_copy(*(ends[::-1] if back else ends), sem.at[k]))
    return out


def rows_of_unit(u, units, k, H):
    shard, half = (pick(u, [x[k][m] for x in units]) for m in range(2))
    return pl.ds(pl.multiple_of((2 * shard + half) * H, H), H)


def stream(ring, links, src, tile, sin, dst, out, sout, work, events, schedule=range(8), beside=None):
    units = [whole(ring.me), whole(ring.mate), ((ring.prev, LO), (ring.next, HI)), ((ring.prevm, LO), (ring.nextm, HI)), whole(ring.opp),
             whole(ring.oppm), ((ring.prev, HI), (ring.next, LO)), ((ring.prevm, HI), (ring.nextm, LO))]
    fetch = lambda u, slot: moves(u, units, src, tile.at[slot], sin.at[slot])
    store = lambda u, slot: moves(u, units, dst, out.at[slot], sout.at[slot], True)
    latest = lambda k: sum(jnp.where(k < s, 0, 1) for s in schedule) - 1

    def fetch_for(k):
        u = latest(k)

        @pl.when(latest(k - 1) < u)
        def _():
            begin(fetch(u, lax.rem(u, 2)))

    fetch_for(0)

    def step(k):
        if beside is not None:
            beside(k)
        u = latest(k)

        @pl.when(latest(k - 1) < u)
        def _():
            slot = lax.rem(u, 2)
            end(fetch(u, slot))

            if dst is None:
                work(u, units, tile.at[slot])
            else:
                pl.when(u > 1)(lambda: end(store(u - 2, slot)))
                work(u, units, tile.at[slot], out.at[slot])
                begin(store(u, slot))

        steps(k, events)
        fetch_for(k + 1)

    loop(schedule[-1] + 1, step)
    if dst is not None:
        end(store(len(units) - 2, 0) + store(len(units) - 1, 1))
    links.sent(*GATHER)


class Fill:
    def __init__(self, jobs, tile, sin, sout):
        self.tile, self.sin, self.sout, self.jobs, at = tile, sin, sout, [], 0
        for srcs, fixed, out, right, ends, *tiles in jobs:
            per = srcs[0].shape[2] // TILE
            first, last = tiles or (0, per * len(srcs))
            self.jobs.append((at, last - first, first, per, srcs, fixed, out, right, ends))
            at += last - first
        self.steps = at

    def load(self, src, j, slot):
        return pltpu.make_async_copy(src.at[:, :, block_rows(j, TILE)], self.tile.at[slot], self.sin.at[slot])

    def fetch(self, k):
        for at, count, first, per, srcs, *_ in self.jobs:
            i = k - at + first
            for m, src in enumerate(srcs):
                mine = (k >= at) & (k < at + count) & (lax.div(i, per) == m)
                pl.when(mine)(lambda: begin([self.load(src, i - m * per, lax.rem(k, 2))]))

    def step(self, k):
        slot = lax.rem(k, 2)
        end([self.load(self.jobs[0][4][0], 0, slot)])
        self.fetch(k + 1)
        for at, count, first, per, srcs, fixed, out, right, ends in self.jobs:
            @pl.when((k >= at) & (k < at + count))
            def _():
                which, j = lax.div(k - at + first, per), lax.rem(k - at + first, per)
                store = lambda m, j, slot: [pltpu.make_async_copy(out.at[slot, :, a], b, self.sout.at[slot, i]) for i, (a, b) in enumerate(ends[m](j))]
                pl.when(k > at + 1)(lambda: end(store(0, j, slot)))
                t = self.tile[slot].reshape(-1, TILE)
                f = flat(fixed[which] if len(srcs) > 1 else fixed[...])
                r = dot(f, t, TN) if right else dot(t, f, TN)
                for a in range(0, r.shape[0], TILE):
                    out[slot, :, (a if right else 0):(a if right else 0) + r.shape[1]] = r[a:a + TILE].astype(BF)
                for m in range(len(srcs)):
                    pl.when(which == m)(lambda: begin(store(m, j, slot)))
                pl.when(k == at + count - 1)(lambda: end(store(0, j, slot) + store(0, j, 1 - slot)))


def gather_events(links, near=None):
    def far():
        links.got(RC, RD)
        links.start(MD)
        links.got(LC, LD)
        links.start(ME)

    def last():
        links.got(RE)
        links.start(MF)
        links.got(LE)
        links.start(MG)

    got = lambda *ks: lambda: links.got(*ks)
    return [got(MA), near, got(MB, MC), far, got(MD, ME), last, got(MF, MG)]


def finish(links, acc, frp, frn, last, rs=(R3,), ls=(L3,)):
    H = acc.shape[0] // 2

    def each(ms, half, f):
        links.got(*ms)
        chunked(H, 16, lambda at: f(pl.ds(half + at.start, at.size)))

    def add(fr):
        def f(at):
            acc[at, :] += fr[at, :].astype(F32)
        return f

    each([R2], H, add(frp))
    each([L2], 0, add(frn))
    each(rs, 0, lambda at: last(at, acc[at, :] + frp[at, :].astype(F32)))
    each(ls, H, lambda at: last(at, acc[at, :] + frn[at, :].astype(F32)))


class Scatter:
    def __init__(self, ring, links, product, stg, p, s, acc, tr, fr):
        self.ring, self.links, self.product, self.stg, self.p, self.s, self.acc, self.tr, self.fr = ring, links, product, stg, p, s, acc, tr, fr
        T = acc.shape[0]
        H = T // 2
        nx, pv, mt = ring.next, ring.prev, ring.mate
        self.every, self.lo, self.hi = every, lo, hi = pl.ds(0, T), pl.ds(0, H), pl.ds(H, H)
        at = lambda ref: [ref.at[k] for k in range(ref.shape[0])]
        even, odd, pa, pb, pc, pd, so, sn, sp, on, off, fp, fn = [*at(stg), *at(p), *at(s), *at(tr), *at(fr)]
        NB = acc.shape[1] // RUNS
        for j, k in enumerate((M0, M5, M6, M7)):
            links.put(k, even.at[:, pl.ds(j * NB, NB)], pa.at[:, pl.ds(j * NB, NB)], mt)
        for k, src, dst, to in ((M2, odd, pb, mt), (M3, even, pc, mt), (M4, odd, pd, mt),
                                (R1, so.at[lo], on, nx), (L1, so.at[hi], off, pv), (R2, sn.at[hi], fp.at[hi], nx), (L2, sp.at[lo], fn.at[lo], pv),
                                (R3, sn.at[lo], fp.at[lo], nx), (L3, sp.at[hi], fn.at[hi], pv)):
            links.put(k, src, dst, to)

    def send(self):
        links, ring, stg, p, s, acc = self.links, self.ring, self.stg, self.p, self.s, self.acc
        runs = (M0, M5, M6, M7)
        shards = (ring.oppm, ring.opp, ring.nextm, ring.prevm, ring.next, ring.prev, ring.mate, ring.me)
        got, sent, start = ((lambda f: lambda *ks: lambda: f(*ks))(f) for f in (links.got, links.sent, links.start))
        before = [None, None, None, sent(*runs), got(M2), got(M3), sent(M2), got(M4)]
        after = [None, start(R1, L1), start(M2), start(M3), start(R2), start(L2), start(M4)]

        def step(i):
            steps(i, before)

            def then(c, v):
                j = lax.div(c.start, c.size)

                def to_mate(k, on=()):
                    def f():
                        stg[k, :, c] = v.astype(BF)
                        steps(j, on)
                    return f

                def to_chip(k, rows, wait=()):
                    def f():
                        steps(j, wait)
                        s[k, rows, c] = (v[rows.start:rows.start + rows.size] + p[k, rows, c].astype(F32)).astype(BF)
                    return f

                def keep():
                    acc[:, c] = v + p[3, :, c].astype(F32)

                steps(i, [to_mate(0, [start(k) for k in runs]), to_chip(0, self.every, [got(k) for k in runs]), to_mate(1), to_mate(0), to_chip(1, self.hi),
                          to_chip(2, self.lo), to_mate(1), keep])

            self.product(pick(i, shards), self.every, then)
            steps(i, after)

        loop(len(shards), step)
        links.sent(M3, M4)

    def pass_on(self):
        H = self.lo.size

        def step(i):
            rows = block_rows(i, H)
            steps(i, [lambda: self.links.got(R1), lambda: self.links.got(L1)])

            def then(c, v):
                self.s[1 + i, rows, c] = (v + self.p[1 + i, rows, c].astype(F32) + self.tr[i, :, c].astype(F32)).astype(BF)
            self.product(pick(i, (self.ring.next, self.ring.prev)), rows, then)
            steps(i, [lambda: self.links.start(R3), lambda: self.links.start(L3)])

        loop(2, step)

    def finish(self, last):
        self.links.sent(R1, L1)
        finish(self.links, self.acc, self.fr.at[0], self.fr.at[1], last)


def scatter_scratch(T, D):
    return [V((2, T, D), BF), V((4, T, D), BF), V((3, T, D), BF), V((T, D), F32), V((2, T // 2, D), BF), V((2, T, D), BF)]


def call(body, args, outs, scratch, flops, name, cid=None, aliases=()):
    return pl.pallas_call(
        body, in_specs=[ANY] * len(args), out_specs=[ANY] * len(outs), out_shape=outs, scratch_shapes=scratch, name=name, input_output_aliases=dict(aliases),
        compiler_params=pltpu.CompilerParams(collective_id=cid, has_side_effects=True, vmem_limit_bytes=MOST),
        cost_estimate=pl.CostEstimate(flops=flops, bytes_accessed=sum(t.size for t in (*args, *outs)), transcendentals=0),
    )(*args)


def rows_of(t):
    return jnp.concatenate([t[:, a:a + HEAD] for a in range(0, t.shape[1], HEAD)], axis=0)


def set_gap(gap):
    gap[...] = lax.broadcasted_iota(jnp.int32, gap.shape, 1) - lax.broadcasted_iota(jnp.int32, gap.shape, 0)


def key_blocks(iq, block):
    seen = lax.div(iq * BQ + 1, BK)
    loop(seen, lambda j: block(j, False))
    loop(lax.div((iq + 1) * BQ + BK - 1, BK), lambda j: block(j, True), seen)


def attend_block(iq, qkv, o_ref, lse_ref, qs, top, mix, gap):
    NQ = o_ref.shape[1]
    cols = qs.shape[0]
    mine = block_rows(iq, BQ)
    qs[...] = rows_of(qkv[mine, :NQ])
    top[...] = jnp.full_like(top, NEG)
    mix[...] = jnp.zeros_like(mix)
    ones = jnp.ones((8, BK), BF)
    strips = [slice(a, a + BQ) for a in range(0, cols, BQ)]

    def block(j, masked):
        here = block_rows(j, BK)
        keys = qkv[here, NQ:NQ + HEAD]
        values = jnp.concatenate([qkv[here, NQ + HEAD:].T, ones], axis=0)
        scores = [dot(keys, qs[at, :], NT) for at in strips]
        ps, keeps = [], []
        for at, s in zip(strips, scores):
            if masked:
                s = jnp.where(gap[...] >= j * BK - iq * BQ, s, HIDDEN)
            old = top[:, at]
            new = jnp.maximum(old, s.max(axis=0, keepdims=True))
            top[:, at] = new
            ps.append(jnp.exp2((s - new) * (SCALE * LOG2E)).astype(BF))
            keeps.append(jnp.exp2((old - new) * (SCALE * LOG2E)))
        for at, p, keep in zip(strips, ps, keeps):
            mix[:, at] = mix[:, at] * keep + dot(values, p)

    key_blocks(iq, block)
    total = mix[HEAD:HEAD + 1, :]
    out = (mix[:HEAD, :] * (1 / total)).T.astype(BF)
    for h in range(NQ // HEAD):
        o_ref[mine, h * HEAD:(h + 1) * HEAD] = out[h * BQ:(h + 1) * BQ]
    lse_ref[iq] = top[...] * SCALE + jnp.log(total)


def _attend_bwd(qkv_ref, do_ref, o_ref, lse_ref, cos_ref, sin_ref, *refs):
    ins, (out_ref, *outs), (qkv, do, o, lse, cos, sin, out, qs, dos, dq, dk, dv, gap, *tiles, sem, sl) = refs[:3], refs[3:7], refs[7:]
    NQ = do.shape[1]
    tokens, cols = dk.shape[0], qs.shape[0]
    blocks = tokens // BQ
    ins, outs = ([*x[:-1], x[-1].at[pl.ds(0, EARLY * TILE)]] for x in (ins, outs))
    come, go = [[pltpu.make_async_copy(x, y, sl.at[k]) for k, (x, y) in enumerate(zip(*ends))] for ends in ((ins, tiles), (tiles, outs))]

    def loads(i):
        at = block_rows(i, BQ)
        pairs = [(x.at[at], y.at[at]) for x, y in ((qkv_ref, qkv), (do_ref, do), (o_ref, o), (cos_ref, cos), (sin_ref, sin))]
        return [pltpu.make_async_copy(x, y, sem.at[i, k]) for k, (x, y) in enumerate([*pairs, (lse_ref.at[i], lse.at[i])])]

    def store(i, columns, k):
        at = block_rows(i, BQ), columns
        return pltpu.make_async_copy(out.at[at], out_ref.at[at], sem.at[i, k])

    part, rest = pl.ds(0, NQ), pl.ds(NQ, 2 * HEAD)
    for i in range(blocks):
        begin(loads(i))
    begin(come)
    set_gap(gap)
    dk[...] = jnp.zeros_like(dk)
    dv[...] = jnp.zeros_like(dv)

    def landed(k):
        def f():
            come[k].wait()
            go[k].start()
        return f

    def queries(iq):
        end(loads(iq))
        steps(iq, [None, *[landed(k) for k in range(len(come))]])
        mine = block_rows(iq, BQ)
        qs[...] = rows_of(qkv[mine, :NQ])
        dos[...] = rows_of(do[mine, :])
        dq[...] = jnp.zeros_like(dq)
        delta = (dos[...].astype(F32) * rows_of(o[mine, :]).astype(F32)).T.sum(axis=0, keepdims=True)
        lses = lse[iq] * LOG2E

        def piece(j, masked, first, size):
            here = pl.ds(pl.multiple_of(j * BK + first, size), size)
            keys, values = qkv[here, NQ:NQ + HEAD], qkv[here, NQ + HEAD:]
            strips = [slice(a + (first if masked else 0), a + BQ) for a in range(0, cols, BQ)]
            scores = [dot(keys, qs[at, :], NT) for at in strips]
            dps = [dot(values, dos[at, :], NT) for at in strips]
            for at, s, dp in zip(strips, scores, dps):
                p = jnp.exp2(s * (SCALE * LOG2E) - lses[:, at])
                if masked:
                    p = jnp.where(gap[first:first + size, first:] >= j * BK - iq * BQ, p, 0.0)
                ds = (p * (dp - delta[:, at])).astype(BF)
                dv[here, :] += dot(p.astype(BF), dos[at, :])
                dk[here, :] += dot(ds, qs[at, :])
                dq[:, at] += dot(keys.T, ds)

        def block(j, masked):
            size = BK // 2 if masked else BK
            for first in range(0, BK, size):
                piece(j, masked, first, size)

        key_blocks(iq, block)
        back = (dq[...] * SCALE).T
        for h in range(NQ // HEAD):
            out[mine, h * HEAD:(h + 1) * HEAD] = turn(back[h * BQ:(h + 1) * BQ], cos[mine, :], -sin[mine, :]).astype(BF)
        store(iq, part, 0).start()

    loop(blocks, queries)

    def keys(at):
        out[at, NQ:NQ + HEAD] = turn(dk[at, :] * SCALE, cos[at, :], -sin[at, :]).astype(BF)
        out[at, NQ + HEAD:] = dv[at, :].astype(BF)
    chunked(tokens, BQ, keys)
    for i in range(blocks):
        store(i, rest, 1).start()
    end([*go, *(store(i, part, 0) for i in range(blocks)), *(store(i, rest, 1) for i in range(blocks))])


def attend_bwd(qkv, d_out, out, lse, cos, sin, others):
    tokens, NQ = out.shape
    cols = lse.shape[2]
    table, key = V(cos.shape, F32), V((tokens, HEAD), F32)
    scratch = [V(qkv.shape, BF), V(out.shape, BF), V(out.shape, BF), V(lse.shape, F32), table, table, V(qkv.shape, BF), V((cols, HEAD), BF), V((cols, HEAD), BF),
               V((HEAD, cols), F32), key, key, V((BK, BQ), jnp.int32), *(V(t.shape, BF) for t in others[:-1]), V((EARLY * TILE, others[-1].shape[1]), BF),
               DMA((tokens // BQ, 6)), DMA((len(others),))]
    return call(_attend_bwd, [qkv, d_out, out, lse, cos, sin, *others], [S(t.shape, BF) for t in (qkv, *others)], scratch, 5 * tokens * tokens * NQ, "attend_bwd")


def _front(x_ref, dy_ref, wq_ref, wk_ref, wv_ref, wo_ref, wd_ref, c_ref, s_ref, a_all, qkv_ref, dy_all, dhid, o_ref, lse_ref, cos_ref, sin_ref, h_ref, b_ref, wt_ref,
           an, tile, small, qkv, o, lse, qs, top, mix, gap, wo, dt, stg, p, s, acc, tr, fr, ss, rs, sb, so, sl, *, n):
    T, D = x_ref.shape
    NQ, NK = wq_ref.shape[1], wk_ref.shape[1]
    turned, Q = NQ + NK, T // 4

    def links():
        ring = Ring(n)
        of_a, of_dy, of_o = (Links(ss, rs, k * COPIES) for k in range(3))
        gather_copies(of_a, ring, an, a_all, T)
        gather_copies(of_dy, ring, dy_ref, dy_all, T)
        return ring, of_a, of_dy, of_o

    pairs = ((x_ref, stg.at[0]), (dy_ref, stg.at[1]), (c_ref, small.at[0]), (s_ref, small.at[1]), (wo_ref, wo),
             (x_ref, stg.at[0]), (qkv, qkv_ref), (o, o_ref), (lse, lse_ref), (s.at[0], h_ref), (stg.at[1], b_ref))
    copies = [pltpu.make_async_copy(a, b, sl.at[k]) for k, (a, b) in enumerate(pairs)]
    x_in, dy_in, c_in, s_in, wo_in, x_again, *outs = copies
    x_in.start()

    def products(w, cos, sin, wt):
        tables = [pltpu.make_async_copy(a, b, so.at[0, k]) for k, (a, b) in enumerate(((cos, cos_ref), (sin, sin_ref)))]
        ring, of_a, of_dy, _ = links()
        keep, keep_dy = (pltpu.make_async_copy(a, b.at[ring.me], so.at[1, k]) for k, (a, b) in enumerate(((an, a_all), (stg.at[1], dy_all))))
        place = [pl.ds(0, NQ), pl.ds(NQ, NK), pl.ds(turned, NK)]
        loads = [dy_in, c_in, s_in, wo_in] + [pltpu.make_async_copy(r, w.at[:, c], sb.at[0, k]) for k, (r, c) in enumerate(zip((wq_ref, wk_ref, wv_ref), place))]
        begin(loads)
        ring.barrier()
        x_in.wait()
        for q, k in ((0, RA), (2, LA), (1, RB), (3, LB)):

            def norm(at):
                at = pl.ds(q * Q + at.start, at.size)
                wide = stg[0, at, :].astype(F32)
                an[at, :] = (wide * norm_scale(wide)).astype(BF)
            chunked(Q, 16, norm)
            of_a.start(k)
        of_a.start(MA)
        keep.start()
        end(loads)
        keep_dy.start()

        def table(at):
            row = pl.ds(HEAD + lax.div(at.start, HEAD), 1)
            c0, s0, c1, s1 = small[0, row, :], small[1, row, :], small[0, :HEAD, :], small[1, :HEAD, :]
            cos[at, :] = c0 * c1 - s0 * s1
            sin[at, :] = s0 * c1 + c0 * s1
        chunked(n * T, HEAD, table)
        begin(tables)
        end([keep, keep_dy])

        def work(u, units, x):
            r = dot(x[...], w[...]).astype(BF)
            for k in range(2):
                rows = slice(k * T // 2, (k + 1) * T // 2)
                place = rows_of_unit(u, units, k, T // 2)
                c, s = cos[place, :], sin[place, :]
                for a in range(0, turned, HEAD):
                    qkv[place, a:a + HEAD] = turn(r[rows, a:a + HEAD].astype(F32), c, s).astype(BF)
                qkv[place, turned:] = r[rows, turned:]

        def turned_round(j):
            slot = lax.rem(j, 2)
            put = lambda j: pltpu.make_async_copy(wt.at[slot], wt_ref.at[:, block_rows(j, TILE)], so.at[1, slot])
            pl.when(j > 1)(lambda: put(j - 2).wait())
            wt[slot] = w[block_rows(j, TILE), :].T
            put(j).start()

        def near():
            of_a.passed_on(RA, LA)
            loop(D // TILE, turned_round)
            of_a.passed_on(RB, LB)
            of_a.start(RE, LE, MB, MC)
            of_dy.start(RA, LA, RB, LB, MA)

        stream(ring, of_a, a_all, tile, sb, None, None, None, work, gather_events(of_a, near))
        end([*tables, *[pltpu.make_async_copy(wt.at[k], wt_ref.at[:, pl.ds(0, TILE)], so.at[1, k]) for k in range(2)]])

    pl.run_scoped(products, V((D, turned + NK), BF), *[V((n * T, HEAD), F32)] * 2, V((2, turned + NK, TILE), BF))
    outs[0].start()
    set_gap(gap)

    def rest(wd):
        ring, _, of_dy, of_o = links()
        wd_in = pltpu.make_async_copy(wd_ref, wd, so.at[0, 0])
        wd_in.start()
        blocks = n * T // BQ

        def attention(iq):
            attend_block(iq, qkv, o, lse, qs, top, mix, gap)
            steps(iq, {blocks - 2: lambda: of_dy.passed_on(RA, LA)})

        loop(blocks, attention)
        begin(outs[1:3])
        of_dy.passed_on(RB, LB)
        of_dy.start(RE, LE, MB, MC)

        def product(shard, rows, then):
            at = pl.ds(pl.multiple_of(shard * T + rows.start, T // 2), rows.size)
            chunked(D, D // RUNS, lambda c: then(c, dot(o[at, :], wo[:, c])))

        scatter = Scatter(ring, of_o, product, stg, p, s, acc, tr, fr)
        scatter.send()
        x_again.start()
        wd_in.wait()

        def work(u, units, x, o):
            def run(c):
                o[:, c] = dot(x[...], wd[c, :], NT).astype(BF)
            chunked(wd.shape[0], TILE, run)

        stream(ring, of_dy, dy_all, tile, sb, dhid, dt, so, work, gather_events(of_dy))
        scatter.pass_on()
        x_again.wait()

        def last(at, total):
            h = (stg[0, at, :].astype(F32) + total).astype(BF)
            s[0, at, :] = h
            h = h.astype(F32)
            stg[1, at, :] = (h * norm_scale(h)).astype(BF)

        scatter.finish(last)
        begin(outs[3:])
        end(outs)
        of_o.sent(R2, L2, R3, L3)

    pl.run_scoped(rest, V(wd_ref.shape, BF))


def front(x, dy, wq, wk, wv, wo, wd, n, cid):
    T, D = x.shape
    NQ, F, tokens = wo.shape[0], wd.shape[0], n * T
    N, cols = NQ + 2 * HEAD, NQ // HEAD * BQ
    stat = (tokens // BQ, 1, cols)
    table, row = S((tokens, HEAD), F32), S((T, D), BF)
    small = angles(jnp.concatenate([jnp.arange(HEAD), jnp.arange(0, tokens, HEAD)]))
    outs = [S((n, T, D), BF), S((tokens, N), BF), S((n, T, D), BF), S((n, T, F), BF), S((tokens, NQ), BF), S(stat, F32), table, table, row, row, S((N, D), BF)]
    scratch = [V((T, D), BF), V((2, T, D), BF), V((2, *small[0].shape), F32), V((tokens, N), BF), V((tokens, NQ), BF),
               V(stat, F32), V((cols, HEAD), BF), V((1, cols), F32), V((HEAD + 8, cols), F32), V((BK, BQ), jnp.int32), V((NQ, D), BF), V((2, T, F), BF),
               *scatter_scratch(T, D), DMA((3 * COPIES,)), DMA((3 * COPIES,)), DMA((2, 3)), DMA((2, 3)), DMA((15,))]
    return call(functools.partial(_front, n=n), [x, dy, wq, wk, wv, wo, wd, *small], outs, scratch, 2 * tokens * D * (N + F + NQ), "front", cid)


def _back(t_ref, x_ref, wt_ref, a_ref, dh_all, heads_ref, b_ref, du_ref, dx_ref, by_q, by_k, by_v, by_o, by_up,
          w, t, heads, du, out, ft, stg, p, s, acc, tr, fr, ss, rs, sl, sf, sg, *, n):
    ring, links = Ring(n), Links(ss, rs)
    T, D = x_ref.shape
    NQ, NK = by_q.shape[1], by_k.shape[1]
    columns = [pl.ds(0, NQ), pl.ds(NQ, NK), pl.ds(NQ + NK, NK)]
    pairs = ((t_ref, t), (wt_ref, w), (du_ref, du), (heads_ref, heads), (x_ref, stg.at[0]), (dh_all.at[ring.me], stg.at[1]),
             (s.at[0], dx_ref))
    *first, du_in, heads_in, x_in, dh_in, dx_out = [pltpu.make_async_copy(a, b, sl.at[k]) for k, (a, b) in enumerate(pairs)]
    begin([*first, du_in, heads_in])
    ring.barrier()
    end(first)

    def product(shard, rows, then):
        chunked(D, D // RUNS, lambda c: then(c, dot(t[shard, rows, :], w[:, c])))

    scatter = Scatter(ring, links, product, stg, p, s, acc, tr, fr)
    scatter.send()
    begin([x_in, dh_in])
    end([du_in, heads_in])
    late = lambda j: [(pl.ds(0, du.shape[2]), by_up.at[block_rows(j - EARLY, TILE)])]
    fill = Fill((([b_ref], du, out, False, [late], EARLY, D // TILE),
                 ([a_ref], t, out, False, [lambda j: [(c, r.at[block_rows(j, TILE)]) for c, r in zip(columns, (by_q, by_k, by_v))]]),
                 ([dh_all], heads, out, True, [lambda j: [(pl.ds(0, TILE), by_o.at[:, block_rows(j, TILE)])]])), ft, sf, sg)
    fill.fetch(0)

    def beside(k):
        fill.step(k)
        steps(k, {1: scatter.pass_on})
    loop(fill.steps, beside)
    end([x_in, dh_in])

    def last(at, total):
        s[0, at, :] = (stg[1, at, :].astype(F32) + unnorm(stg[0, at, :].astype(F32), total)).astype(BF)

    scatter.finish(last)
    dx_out.start()
    dx_out.wait()
    links.sent(R2, L2, R3, L3)


def back(dqkv, x, wt, ws, a, dh_all, heads, b, du, n, cid):
    T, D = x.shape
    K, NQ, F = dqkv.shape[2], heads.shape[2], du.shape[2]
    scratch = [V((K, D), BF), V(dqkv.shape, BF), V(heads.shape, BF), V(du.shape, BF), V((2, TILE, F), BF), V((2, n, T, TILE), BF), *scatter_scratch(T, D),
               DMA((COPIES,)), DMA((COPIES,)), DMA((8,)), DMA((2,)), DMA((2, 3))]
    outs = [S((T, D), BF), *(S(w.shape, BF) for w in ws), S((NQ, D), BF), S((D - EARLY * TILE, F), BF)]
    return call(functools.partial(_back, n=n), [dqkv, x, wt, a, dh_all, heads, b, du], outs, scratch, 6 * n * T * D * K, "back", cid)


def _land(*refs):
    m = (len(refs) - 2) // 3
    ins, outs, tiles, sem = refs[:m], refs[m + 1:2 * m + 1], refs[2 * m + 1:-1], refs[-1]
    outs = [*outs[:-1], outs[-1].at[pl.ds(EARLY * TILE, ins[-1].shape[0])]]
    come = [pltpu.make_async_copy(a, b, sem.at[k]) for k, (a, b) in enumerate(zip(ins, tiles))]
    go = [pltpu.make_async_copy(a, b, sem.at[k]) for k, (a, b) in enumerate(zip(tiles, outs))]
    begin(come)
    for a, b in zip(come, go):
        a.wait()
        b.start()
    end(go)


def land(arrays, whole):
    shapes = [S(t.shape, BF) for t in (*arrays[:-1], whole)]
    return call(_land, [*arrays, whole], shapes, [*(V(t.shape, BF) for t in arrays), DMA((len(arrays),))], 0, "land", aliases={len(arrays): len(arrays) - 1})


def mlp_links(b_ref, bg, frm, stg, s3, s1, p1, p3, tr, frp, frn, ss, rs, n):
    ring, links = Ring(n), Links(ss, rs)
    T = b_ref.shape[0]
    H, Q = T // 2, T // 4
    first = pl.ds(0, Q)
    nx, pv, mt = ring.next, ring.prev, ring.mate
    lo, hi = pl.ds(0, H), pl.ds(H, H)
    gather_copies(links, ring, b_ref, bg, T)
    at = lambda ref: [ref.at[k] for k in range(ref.shape[0])]
    pa, pb, pc, pd, sa, sb1, sc, sd1, even, odd, on, off = [*at(p1), *at(s1), *at(stg), *at(tr)]
    for k, src, dst, to in ((M5, odd, frm, mt), (M0, odd.at[hi], pa, mt), (M1, even, p3, mt), (M2, even.at[hi], pb, mt), (M3, odd.at[hi], pc, mt), (M4, even.at[hi], pd, mt),
                            (R1, s3.at[lo], on, nx), (L1, s3.at[hi], off, pv), (R2, sb1, frp.at[hi], nx), (L2, sa, frn.at[lo], pv),
                            (R3, sc.at[first], frp.at[first], nx), (R4, sd1.at[first], frp.at[pl.ds(Q, Q)], nx),
                            (L3, sc.at[pl.ds(Q, Q)], frn.at[pl.ds(H, Q)], pv), (L4, sd1.at[pl.ds(Q, Q)], frn.at[pl.ds(H + Q, Q)], pv)):
        links.put(k, src, dst, to)
    return ring, links


def pair_sum(acc, p1, s1, tr, k, base=0, first=None):
    H = s1.shape[1]

    def add(at, *further):
        v = acc[pl.ds(base + at.start, at.size), :] + p1[k, at, :].astype(F32)
        s1[k, at, :] = sum([tr[t].astype(F32) for t in further], v).astype(BF)

    if first is None:
        chunked(H, 16, add)
    else:
        for side in range(2):
            chunked(H // 2, 16, lambda at: add(pl.ds(side * (H // 2) + at.start, at.size), (side, pl.ds(first + at.start, at.size))))


def _units(b_ref, dhid_ref, wg_ref, wu_ref, bg, hid, dgo, duo, own, frm, bt, acc, stg, s3, s1, p1, p3, tr, frp, frn, ss, rs, sw, sb, sd, so, sl, n, wg, wu, dht, st):
    ring, links = mlp_links(b_ref, bg, frm, stg, s3, s1, p1, p3, tr, frp, frn, ss, rs, n)
    T, D = b_ref.shape
    F = wg_ref.shape[1]
    H, NC, NB = T // 2, F // 3, D // 4
    me, nx, pv, mt = ring.me, ring.next, ring.prev, ring.mate
    Q0, Q1, Q2, Q3 = range(4)
    quarters = lambda *shards: tuple((shard, q) for shard in shards for q in range(4))
    pvm, nxm = ring.prevm, ring.nextm
    units = [quarters(me), quarters(mt), ((pv, Q0), (pv, Q1), (pvm, Q0), (pvm, Q1)), ((nx, Q2), (nx, Q3), (nxm, Q2), (nxm, Q3)),
             quarters(ring.oppm), quarters(ring.opp), ((nx, Q0), (pv, Q2), (nxm, Q0), (pvm, Q2)), ((nx, Q1), (pv, Q3), (nxm, Q1), (pvm, Q3))]
    count = len(units)

    def fetch(u, slot):
        return moves(u, units, bg, bt.at[slot], sb.at[slot]) + moves(u, units, dhid_ref, dht.at[slot], sd.at[slot])

    def store(u):
        return [c for m, ref in enumerate((hid, dgo, duo)) for c in moves(u, units, ref, st.at[m], so.at[m], True)]

    def weights(j):
        s = block_rows(j, NC)
        return [pltpu.make_async_copy(a.at[:, s], b.at[:, s], sw.at[k, j]) for k, (a, b) in enumerate(((wg_ref, wg), (wu_ref, wu)))]

    pairs = ((b_ref, bt.at[0]), (dhid_ref.at[me], dht.at[0]), (bt.at[0], bg.at[me]), (acc, own))
    *first, keep, own_out = [pltpu.make_async_copy(a, b, sl.at[k]) for k, (a, b) in enumerate(pairs)]
    begin(first)
    for j in range(F // NC):
        begin(weights(j))
    ring.barrier()
    links.start(RA, LA, RB, LB, MA)
    end(first)
    keep.start()

    pair = functools.partial(pair_sum, acc, p1, s1, tr)

    again = [c for m, ref in enumerate((dgo, duo)) for c in moves(HI, units, ref, st.at[1 + m], so.at[1 + m])]

    def mid0():
        keep.wait()
        links.got(MA)
        begin(fetch(1, 1))

    def mid1():
        own_out.start()
        links.passed_on(RB)
        links.start(RE)
        links.passed_on(LB)
        links.start(LE, MB, MC)
        links.got(MB)
        begin(fetch(2, 0))

    def late2():
        links.got(MC)
        begin(fetch(3, 1))

    def mid3():
        links.got(M0)
        pair(0)
        links.start(L2)
        far()

    def late3():
        links.got(MD, ME)
        begin(fetch(4, 0))

    def mid4():
        links.got(M2)
        pair(1)
        links.start(R2)
        links.sent(M2)
        begin(fetch(5, 1))

    def late5():
        links.got(MG, MF)
        begin(fetch(6, 0))

    def late7():
        links.got(M3, R1, L1)
        pair(2, 0, 0)
        links.start(R3, L3)
        links.sent(M3)

    def post7():
        links.start(M4)
        end(store(7))
        begin(again)
        end(again)

    def late8():
        links.got(M4)
        pair(3, H, H // 2)
        links.start(R4, L4)

    _, _, _, far, _, last, _ = gather_events(links)
    starting = lambda *ks: lambda: links.start(*ks)
    mids = [mid0, mid1, own_out.wait, mid3, mid4, lambda: links.got(M1), lambda: links.sent(M0), lambda: links.sent(M1)]
    lates = [lambda: links.passed_on(RA, LA), None, late2, late3, last, late5, lambda: begin(fetch(7, 1)), late7, late8]
    posts = [None, None, starting(M0), starting(M2), starting(M1), starting(R1, L1), starting(M3), post7, starting(M5)]

    def forth_unit(u, slot):
        @pl.when(u > 0)
        def _():
            end(fetch(u, slot))
            end(store(u - 1))

        def forth(j):
            @pl.when(u == 0)
            def _():
                end(weights(j))
            s = block_rows(j, NC)
            x = bt[slot]
            gate, up = dot(x, wg[:, s]), dot(x, wu[:, s])
            d = dht[slot, :, s].astype(F32)
            sig = jax.nn.sigmoid(gate)
            act = gate * sig
            for m, v in enumerate((act * up, d * up * (sig + act * (1 - sig)), d * act)):
                st[m, :, s] = v.astype(BF)

        loop(F // NC, forth)
        begin(store(u))

    def unit(u):
        slot = lax.rem(u, 2)
        pl.when(u < count)(lambda: forth_unit(u, slot))
        steps(u, mids)
        mate_only = (u == 4) | (u == count)
        halved = (u == 2) | (u == 3) | (u == 6) | (u == 7)
        side = jnp.where((u == 2) | (u == 6) | (u == count), 1, 0)

        def back(c):
            v = dot(st[1], wg[c, :], NT) + dot(st[2], wu[c, :], NT)

            @pl.when(u == 0)
            def _():
                acc[:, c] = v

            @pl.when(mate_only)
            def _():
                stg[side, :, c] = v.astype(BF)

            @pl.when(u == 5)
            def _():
                s3[:, c] = (v + p3[:, c].astype(F32)).astype(BF)

            @pl.when(halved)
            def _():
                acc[pl.ds(pl.multiple_of(jnp.where(u == 7, H, 0), H), H), c] = v[:H]
                stg[side, H:, c] = v[H:].astype(BF)

        half = D // NB // 2

        @pl.when(u != 1)
        def _():
            loop(half, lambda j: back(block_rows(j, NB)))
            steps(u, lates)
            loop(D // NB, lambda j: back(block_rows(j, NB)), half)

        steps(u, posts)

    loop(count + 1, unit)


def _middle(b_ref, dhid_ref, wg_ref, wu_ref, h_ref, dy_ref, wo_ref, dy_all, bg, hid, dgo, duo, dh_all, out, by_down, by_gate, by_up, own, frm,
            bt, acc, stg, s3, s1, p1, p3, tr, frp, frn, ot, ss, rs, sw, sb, sd, so, sl, sf, sg, *, n):
    T, D = b_ref.shape
    F, NQ = wg_ref.shape[1], wo_ref.shape[0]
    shared = (bt, acc, stg, s3, s1, p1, p3, tr, frp, frn, ss, rs)
    pl.run_scoped(functools.partial(_units, b_ref, dhid_ref, wg_ref, wu_ref, bg, hid, dgo, duo, own, frm, *shared, sw, sb, sd, so, sl, n),
                  V((D, F), BF), V((D, F), BF), V((2, T, F), BF), V((3, T, F), BF))

    def rest(fixed, left, tile, wo):
        ring, links = mlp_links(b_ref, bg, frm, *shared[2:], n)
        of_dh = Links(ss, rs, COPIES)
        gather_copies(of_dh, ring, stg.at[0], dh_all, T)
        pairs = ((hid, fixed.at[1]), (dgo, fixed.at[0]), (duo, fixed.at[1]), (wo_ref, wo), (own, acc), (frm, bt.at[0]), (h_ref, bt.at[1]), (dy_ref, s3),
                 (stg.at[0], dh_all.at[ring.me]))
        hid_in, dg_in, du_in, wo_in, own_in, frm_in, *rows_in, keep = [pltpu.make_async_copy(a, b, sl.at[k]) for k, (a, b) in enumerate(pairs)]
        side = lambda ref: lambda j: [(pl.ds(0, F), ref.at[block_rows(j, TILE)])]
        fill = Fill((([dy_all], fixed.at[1], left, True, [lambda j: [(pl.ds(a, TILE), by_down.at[pl.ds(a, TILE), block_rows(j, TILE)]) for a in range(0, F, TILE)]]),
                     ([bg, bg], fixed, left, False, [side(by_gate), side(by_up)], 0, D // TILE + EARLY)), tile, sf, sg)
        hid_in.start()
        fill.fetch(0)
        links.sent(R1, L1)
        begin([own_in, *rows_in])
        hid_in.wait()

        def loads():
            links.got(M5)
            begin([frm_in, dg_in, wo_in])

        def scattered():
            end([dg_in, wo_in, own_in, frm_in, *rows_in])
            links.sent(M4)

            def add(at):
                acc[at, :] += bt[0, at, :].astype(F32)
            chunked(T, 16, add)

            def last(at, total):
                stg[0, at, :] = (s3[at, :].astype(F32) + unnorm(bt[1, at, :].astype(F32), total)).astype(BF)

            finish(links, acc, frp, frn, last, (R3, R4), (L3, L4))
            of_dh.start(RA, LA, RB, LB, MA)
            keep.start()

        def near():
            of_dh.passed_on(RB, LB)
            of_dh.start(RE, LE, MB, MC)

        def work(u, units, x, o):
            o[...] = dot(x[...], wo[...], NT).astype(BF)

        mate, _, mates, far, fars, last, lasts = gather_events(of_dh)
        events = {0: loads, 3: scattered, 7: lambda: (du_in.start(), mate(), keep.wait(), of_dh.passed_on(RA, LA)), 10: near, 12: mates, 15: lambda: (du_in.wait(), far()), 16: fars, 19: last, 20: lasts}
        schedule = (8, 9, 13, 14, 17, 18, fill.steps, fill.steps + 1)
        stream(ring, of_dh, dh_all, bt, sb, out, ot, sd, work, events, schedule, lambda k: pl.when(k < fill.steps)(lambda: fill.step(k)))
        links.sent(*GATHER, R2, R3, R4, L2, L3, L4, M5)

    pl.run_scoped(rest, V((2, n, T, F), BF), V((2, TILE, F), BF), V((2, n, T, TILE), BF), V((NQ, D), BF))


def middle(b, dhid, wg, wu, h, dy, wo, dy_all, n, cid):
    T, D = b.shape
    F, NQ = wg.shape[1], wo.shape[0]
    H = T // 2
    row, halves = V((T, D), BF), V((4, H, D), BF)
    scratch = [V((2, T, D), BF), V((T, D), F32), V((2, T, D), BF), row, halves, halves, row, V((2, H, D), BF), row, row, V((2, T, NQ), BF),
               DMA((2 * COPIES,)), DMA((2 * COPIES,)), DMA((2, 3)), DMA((2, 4)), DMA((2, 4)), DMA((3, 4)), DMA((9,)), DMA((2,)), DMA((2, 3))]
    wide, full, narrow = S((n, T, F), BF), S((n, T, D), BF), S((D, F), BF)
    outs = [full, wide, wide, wide, full, S((n, T, NQ), BF), S((F, D), BF), narrow, narrow, S((T, D), F32), S((T, D), BF)]
    got = call(functools.partial(_middle, n=n), [b, dhid, wg, wu, h, dy, wo, dy_all], outs, scratch, 14 * n * T * D * F, "middle", cid)
    return got[4:9], got[0], got[3]


def solution(mesh):
    n = mesh.shape["tp"]

    def step(x, dy, wq, wk, wv, wo, wg, wu, wd):
        x, dy = x[0], dy[0]
        blocks = lambda t: t.reshape(n, -1, t.shape[1])
        a, qkv, dy_all, dhid, heads, lse, cos, sin, h, b, wt = front(x, dy, wq, wk, wv, wo, wd, n, 0)
        (dh_all, d_heads, *by_mlp), b, du = middle(b, dhid, wg, wu, h, dy, wo, dy_all, n, 1)
        dqkv, by_down, by_gate, by_up = attend_bwd(qkv, flat(d_heads), heads, lse, cos, sin, by_mlp)
        dx, *by_qkvo, by_up = land(back(blocks(dqkv), x, wt, [wq, wk, wv], a, dh_all, blocks(heads), b, du, n, 2), by_up)
        return dx[None], *by_qkvo, by_gate, by_up, by_down

    states, by_columns, by_rows = P("dp", "tp", None), P(None, "tp"), P("tp", None)
    weights = (by_columns, by_columns, by_columns, by_rows, by_columns, by_columns, by_rows)
    own = tuple(P("dp", "tp") if spec == by_columns else P(("dp", "tp"), None) for spec in weights)
    return jax.shard_map(step, mesh=mesh, in_specs=(states, states, *weights), out_specs=(states, *own), check_vma=False)
```

```python
import functools

import jax
import jax.numpy as jnp
from jax import lax
from jax.experimental import pallas as pl
from jax.experimental.pallas import tpu as pltpu
from jax.sharding import PartitionSpec as P

BF, F32 = jnp.bfloat16, jnp.float32
HEAD = 128
THETA = 10000
NEG = -1e30
HIDDEN = 2 * NEG
LOG2E = 1.4426950408889634
SCALE = HEAD**-0.5
MOST = 67_000_000
BQ = BK = 512
TILE = 512
EARLY = 3
NN, NT, TN = ((((a,), (b,)), ((), ())) for a, b in ((1, 0), (1, 1), (0, 0)))
ANY = pl.BlockSpec(memory_space=pl.ANY)
S, V, DMA = jax.ShapeDtypeStruct, pltpu.VMEM, pltpu.SemaphoreType.DMA

RA, RB, RC, RD, RE, LA, LB, LC, LD, LE, MA, MB, MC, MD, ME, MF, MG = GATHER = range(17)
R1, R2, R3, R4, R5, L1, L2, L3, L4, L5, M0, M1, M2, M3, M4, M5, M6, M7, MH, MI = range(17, 37)
COPIES = 37
RUNS = 4
LO, HI = BOTH = range(2)


def dot(a, b, dims=NN, **kw):
    return lax.dot_general(a, b, dims, preferred_element_type=F32, **kw)


def norm_scale(wide):
    return lax.rsqrt(jnp.mean(wide * wide, -1, keepdims=True) + 1e-6)


def unnorm(wide, d):
    scale = norm_scale(wide)
    return d * scale - wide * (scale * scale * scale * jnp.mean(d * wide, -1, keepdims=True))


def turn(t, cos, sin):
    return t * cos + pltpu.roll(t, HEAD // 2, 1) * sin


def angles(places):
    half = HEAD // 2
    a = places.astype(F32)[:, None] * THETA ** (-jnp.arange(half, dtype=F32) / half)
    cos, sin = jnp.cos(a), jnp.sin(a)
    return jnp.concatenate([cos, cos], -1), jnp.concatenate([-sin, sin], -1)


class Ring:
    def __init__(self, n):
        self.me = lax.axis_index("tp")
        core, chips = lax.rem(self.me, 2), n // 2
        chip = [lax.rem(lax.div(self.me, 2) + k, chips) for k in range(chips)]
        self.next, self.opp, self.prev = [2 * c + core for c in chip[1:]]
        self.mate, self.nextm, self.oppm, self.prevm = [2 * c + 1 - core for c in chip]

    def barrier(self):
        b = pltpu.get_barrier_semaphore()
        near = (self.next, self.prev, self.mate)
        for d in near:
            pl.semaphore_signal(b, inc=1, device_id={"tp": d}, device_id_type=pl.DeviceIdType.MESH)
        pl.semaphore_wait(b, len(near))


class Links:
    def __init__(self, ss, rs, base=0):
        self.ss, self.rs, self.base, self.made = ss, rs, base, {}

    def put(self, k, src, dst, dev):
        self.made[k] = lambda: pltpu.make_async_remote_copy(src_ref=src, dst_ref=dst, send_sem=self.ss.at[self.base + k], recv_sem=self.rs.at[self.base + k],
                                                            device_id={"tp": dev}, device_id_type=pl.DeviceIdType.MESH)

    def start(self, *ks):
        for k in ks:
            self.made[k]().start()

    def got(self, *ks):
        for k in ks:
            self.made[k]().wait_recv()

    def sent(self, *ks):
        for k in ks:
            self.made[k]().wait_send()

    def passed_on(self, *ks):
        for k in ks:
            self.got(k)
            self.start(k + 2)


def flat(t):
    return t.reshape(-1, t.shape[-1])


def begin(copies):
    for c in copies:
        c.start()


def end(copies):
    for c in copies:
        c.wait()


def pick(u, values):
    out = values[0]
    for k, v in enumerate(values):
        out = jnp.where(u == k, v, out)
    return out


def steps(u, events):
    for k, f in events.items() if isinstance(events, dict) else enumerate(events):
        def run(f=f):
            f()
        if f is not None:
            pl.when(u == k)(run)


def loop(count, f, first=0):
    def body(k, _):
        f(k)
    lax.fori_loop(first, count, body, None)


def block_rows(i, size):
    return pl.ds(pl.multiple_of(i * size, size), size)


def chunked(size, width, f):
    loop(size // width, lambda j: f(block_rows(j, width)))


def gather_copies(links, ring, src, dst, T, fine=False):
    H, Q = T // 2, T // 4
    me, nx, pv, mt, opp = ring.me, ring.next, ring.prev, ring.mate, ring.opp
    for k, slot, a, rows, to in ((RA, me, 0, Q, nx), (RB, me, Q, Q, nx), (RC, pv, 0, Q, nx), (RD, pv, Q, Q, nx), (RE, me, H, H, nx),
                                 (LA, me, H, Q, pv), (LB, me, H + Q, Q, pv), (LC, nx, H, Q, pv), (LD, nx, H + Q, Q, pv), (LE, me, 0, H, pv),
                                 (MA, me, 0, T, mt), (MB, pv, 0, Q if fine else H, mt), (MC, nx, H, Q if fine else H, mt),
                                 (MH, pv, Q, Q, mt), (MI, nx, H + Q, Q, mt), (MD, opp, 0, H, mt), (ME, opp, H, H, mt), (MF, pv, H, H, mt), (MG, nx, 0, H, mt)):
        at = pl.ds(a, rows)
        links.put(k, src.at[at] if slot is me else dst.at[slot, at], dst.at[slot, at], to)


def whole(shard):
    return (shard, LO), (shard, HI)


def moves(u, units, far, near, sem, back=False):
    parts = len(units[0])
    size = near.shape[0] // parts
    out = []
    for k in range(parts):
        shard, place = (pick(u, [x[k][m] for x in units]) for m in BOTH)
        ends = far.at[shard, block_rows(place, size)], near.at[pl.ds(k * size, size)]
        out.append(pltpu.make_async_copy(*(ends[::-1] if back else ends), sem.at[k]))
    return out


def rows_of_unit(u, units, k, H):
    shard, half = (pick(u, [x[k][m] for x in units]) for m in BOTH)
    return pl.ds(pl.multiple_of((2 * shard + half) * H, H), H)


def stream(ring, links, src, tile, sin, dst, out, sout, work, events, schedule=range(8), beside=None):
    units = [whole(ring.me), whole(ring.mate), ((ring.prev, LO), (ring.next, HI)), ((ring.prevm, LO), (ring.nextm, HI)), whole(ring.opp),
             whole(ring.oppm), ((ring.prev, HI), (ring.next, LO)), ((ring.prevm, HI), (ring.nextm, LO))]
    fetch = lambda u, slot: moves(u, units, src, tile.at[slot], sin.at[slot])
    store = lambda u, slot: moves(u, units, dst, out.at[slot], sout.at[slot], True)
    latest = lambda k: sum(jnp.where(k < s, 0, 1) for s in schedule) - 1

    def fetch_for(k):
        u = latest(k)

        @pl.when(latest(k - 1) < u)
        def _():
            begin(fetch(u, lax.rem(u, 2)))

    fetch_for(0)

    def step(k):
        if beside is not None:
            beside(k)
        u = latest(k)

        @pl.when(latest(k - 1) < u)
        def _():
            slot = lax.rem(u, 2)
            end(fetch(u, slot))

            if dst is None:
                work(u, units, tile.at[slot])
            else:
                pl.when(u > 1)(lambda: end(store(u - 2, slot)))
                work(u, units, tile.at[slot], out.at[slot])
                begin(store(u, slot))

        steps(k, events)
        fetch_for(k + 1)

    loop(schedule[-1] + 1, step)
    if dst is not None:
        end(store(len(units) - 2, 0) + store(len(units) - 1, 1))
    links.sent(*GATHER)


class Fill:
    def __init__(self, jobs, tile, sin, sout):
        self.tile, self.sin, self.sout, self.jobs, at = tile, sin, sout, [], 0
        for srcs, fixed, out, right, ends, *tiles in jobs:
            per = srcs[0].shape[2] // TILE
            first, last = tiles or (0, per * len(srcs))
            self.jobs.append((at, last - first, first, per, srcs, fixed, out, right, ends))
            at += last - first
        self.steps = at

    def load(self, src, j, slot):
        return pltpu.make_async_copy(src.at[:, :, block_rows(j, TILE)], self.tile.at[slot], self.sin.at[slot])

    def fetch(self, k):
        for at, count, first, per, srcs, *_ in self.jobs:
            i = k - at + first
            for m, src in enumerate(srcs):
                mine = (k >= at) & (k < at + count) & (lax.div(i, per) == m)
                pl.when(mine)(lambda: begin([self.load(src, i - m * per, lax.rem(k, 2))]))

    def step(self, k):
        slot = lax.rem(k, 2)
        end([self.load(self.jobs[0][4][0], 0, slot)])
        self.fetch(k + 1)
        for at, count, first, per, srcs, fixed, out, right, ends in self.jobs:
            @pl.when((k >= at) & (k < at + count))
            def _():
                which, j = lax.div(k - at + first, per), lax.rem(k - at + first, per)
                store = lambda m, j, slot: [pltpu.make_async_copy(out.at[slot, :, a], b, self.sout.at[slot, i]) for i, (a, b) in enumerate(ends[m](j))]
                pl.when(k > at + 1)(lambda: end(store(0, j, slot)))
                t = self.tile[slot].reshape(-1, TILE)
                f = flat(fixed[which] if len(srcs) > 1 else fixed[...])
                r = dot(f, t, right) if right else dot(t, f, TN)
                for a in range(0, r.shape[0], TILE):
                    out[slot, :, (a if right else 0):(a if right else 0) + r.shape[1]] = r[a:a + TILE].astype(BF)
                for m in range(len(srcs)):
                    pl.when(which == m)(lambda: begin(store(m, j, slot)))
                pl.when(k == at + count - 1)(lambda: end(store(0, j, slot) + store(0, j, 1 - slot)))


def gather_events(links, near=None):
    def far():
        links.got(RC, RD)
        links.start(MD)
        links.got(LC, LD)
        links.start(ME)

    def last():
        links.got(RE)
        links.start(MF)
        links.got(LE)
        links.start(MG)

    got = lambda *ks: lambda: links.got(*ks)
    return [got(MA), near, got(MB, MC), far, got(MD, ME), last, got(MF, MG)]


def add_rows(links, acc, ms, fr, half):
    def add(at):
        at = pl.ds(half + at.start, at.size)
        acc[at, :] += fr[at, :].astype(F32)
    links.got(*ms)
    chunked(acc.shape[0] // 2, 16, add)


def finish(links, acc, fr, last, rs=(R3,), ls=(L3,)):
    H = acc.shape[0] // 2
    for ms, k, half in ((rs, 0, 0), (ls, 1, H)):
        def total(at):
            at = pl.ds(half + at.start, at.size)
            last(at, acc[at, :] + fr[k, at, :].astype(F32))
        links.got(*ms)
        chunked(H, 16, total)


class Scatter:
    def __init__(self, ring, links, product, stg, p, s, acc, tr, fr):
        self.ring, self.links, self.product, self.stg, self.p, self.s, self.acc, self.tr, self.fr = ring, links, product, stg, p, s, acc, tr, fr
        T = acc.shape[0]
        H = T // 2
        nx, pv, mt = ring.next, ring.prev, ring.mate
        self.every, self.lo, self.hi = every, lo, hi = pl.ds(0, T), pl.ds(0, H), pl.ds(H, H)
        at = lambda ref: [ref.at[k] for k in range(ref.shape[0])]
        even, odd, pa, pb, pc, pd, so, sn, sp, on, off, fp, fn = [*at(stg), *at(p), *at(s), *at(tr), *at(fr)]
        NB = acc.shape[1] // RUNS
        for j, k in enumerate((M0, M5, M6, M7)):
            links.put(k, even.at[:, pl.ds(j * NB, NB)], pa.at[:, pl.ds(j * NB, NB)], mt)
        for k, src, dst, to in ((M2, odd, pb, mt), (M3, even, pc, mt), (M4, odd, pd, mt),
                                (R1, so.at[lo], on, nx), (L1, so.at[hi], off, pv), (R2, sn.at[hi], fp.at[hi], nx), (L2, sp.at[lo], fn.at[lo], pv),
                                (R3, sn.at[lo], fp.at[lo], nx), (L3, sp.at[hi], fn.at[hi], pv)):
            links.put(k, src, dst, to)

    def send(self):
        links, ring, stg, p, s, acc = self.links, self.ring, self.stg, self.p, self.s, self.acc
        runs = (M0, M5, M6, M7)
        shards = (ring.oppm, ring.opp, ring.nextm, ring.prevm, ring.next, ring.prev, ring.mate, ring.me)
        got, sent, start = ((lambda f: lambda *ks: lambda: f(*ks))(f) for f in (links.got, links.sent, links.start))
        before = [None, None, None, sent(*runs), got(M2), got(M3), sent(M2)]
        after = [None, start(R1, L1), start(M2), start(M3), start(R2), start(L2), start(M4)]

        def step(i):
            steps(i, before)

            def then(c, v):
                j = lax.div(c.start, c.size)

                def to_mate(k, on=()):
                    def f():
                        stg[k, :, c] = v.astype(BF)
                        steps(j, on)
                    return f

                def to_chip(k, rows, wait=()):
                    def f():
                        steps(j, wait)
                        s[k, rows, c] = (v[rows.start:rows.start + rows.size] + p[k, rows, c].astype(F32)).astype(BF)
                    return f

                def keep():
                    acc[:, c] = v

                steps(i, [to_mate(0, [start(k) for k in runs]), to_chip(0, self.every, [got(k) for k in runs]), to_mate(1), to_mate(0), to_chip(1, self.hi),
                          to_chip(2, self.lo), to_mate(1), keep])

            self.product(pick(i, shards), self.every, then)
            steps(i, after)

        loop(len(shards), step)
        links.sent(M3, M4)

    def pass_on(self):
        H = self.lo.size

        def step(i):
            rows = block_rows(i, H)
            steps(i, [lambda: self.links.got(R1), lambda: self.links.got(L1)])

            def then(c, v):
                self.s[1 + i, rows, c] = (v + self.p[1 + i, rows, c].astype(F32) + self.tr[i, :, c].astype(F32)).astype(BF)
            self.product(pick(i, (self.ring.next, self.ring.prev)), rows, then)
            steps(i, [lambda: self.links.start(R3), lambda: self.links.start(L3)])

        loop(2, step)

    def finish(self, last):
        self.links.sent(R1, L1)
        for ms, fr, half in (([M4], self.p.at[3], self.hi), ([], self.p.at[3], self.lo), ([R2], self.fr.at[0], self.hi), ([L2], self.fr.at[1], self.lo)):
            add_rows(self.links, self.acc, ms, fr, half.start)
        finish(self.links, self.acc, self.fr, last)


def scatter_scratch(T, D):
    return [V((2, T, D), BF), V((4, T, D), BF), V((3, T, D), BF), V((T, D), F32), V((2, T // 2, D), BF), V((2, T, D), BF)]


def call(body, args, outs, scratch, flops, name, cid=None, aliases=()):
    return pl.pallas_call(
        body, in_specs=[ANY] * len(args), out_specs=[ANY] * len(outs), out_shape=outs, scratch_shapes=scratch, name=name, input_output_aliases=dict(aliases),
        compiler_params=pltpu.CompilerParams(collective_id=cid, has_side_effects=True, vmem_limit_bytes=MOST),
        cost_estimate=pl.CostEstimate(flops=flops, bytes_accessed=sum(t.size for t in (*args, *outs)), transcendentals=0),
    )(*args)


def rows_of(t):
    return jnp.concatenate([t[:, a:a + HEAD] for a in range(0, t.shape[1], HEAD)], axis=0)


def set_gap(gap):
    gap[...] = lax.broadcasted_iota(jnp.int32, gap.shape, 1) - lax.broadcasted_iota(jnp.int32, gap.shape, 0)


def key_blocks(iq, block):
    seen = lax.div(iq * BQ + 1, BK)
    loop(seen, lambda j: block(j, False))
    loop(lax.div((iq + 1) * BQ + BK - 1, BK), lambda j: block(j, True), seen)


def attend_block(iq, qkv, o_ref, ot_ref, lse_ref, qs, top, mix, gap):
    NQ = o_ref.shape[1]
    cols = qs.shape[0]
    mine = block_rows(iq, BQ)
    qs[...] = rows_of(qkv[mine, :NQ])
    top[...] = jnp.full_like(top, NEG)
    mix[...] = jnp.zeros_like(mix)
    ones = jnp.ones((8, BK), BF)
    strips = [slice(a, a + BQ) for a in range(0, cols, BQ)]

    def block(j, masked):
        here = block_rows(j, BK)
        keys = qkv[here, NQ:NQ + HEAD]
        values = jnp.concatenate([qkv[here, NQ + HEAD:].T, ones], axis=0)
        scores = [dot(keys, qs[at, :], NT) for at in strips]
        ps, keeps = [], []
        for at, s in zip(strips, scores):
            if masked:
                s = jnp.where(gap[...] >= j * BK - iq * BQ, s, HIDDEN)
            old = top[:, at]
            new = jnp.maximum(old, s.max(axis=0, keepdims=True))
            top[:, at] = new
            ps.append(jnp.exp2((s - new) * (SCALE * LOG2E)).astype(BF))
            keeps.append(jnp.exp2((old - new) * (SCALE * LOG2E)))
        for at, p, keep in zip(strips, ps, keeps):
            mix[:, at] = mix[:, at] * keep + dot(values, p)

    key_blocks(iq, block)
    total = mix[HEAD:HEAD + 1, :]
    out = mix[:HEAD, :] * (1 / total)
    for h in range(NQ // HEAD):
        part = out[:, h * BQ:(h + 1) * BQ]
        ot_ref[h * HEAD:(h + 1) * HEAD, mine] = part.astype(BF)
        o_ref[mine, h * HEAD:(h + 1) * HEAD] = part.T.astype(BF)
    lse_ref[iq] = top[...] * SCALE + jnp.log(total)


def _attend_bwd(qkv_ref, do_ref, o_ref, lse_ref, cos_ref, sin_ref, *refs):
    ins, (out_ref, *outs), (qkv, do, o, lse, cos, sin, out, qs, dos, dq, dk, dv, gap, *tiles, sem, sl) = refs[:3], refs[3:7], refs[7:]
    NQ = do.shape[1]
    tokens, cols = dk.shape[0], qs.shape[0]
    blocks = tokens // BQ
    ins, outs = ([*x[:-1], x[-1].at[pl.ds(0, EARLY * TILE)]] for x in (ins, outs))
    come, go = [[pltpu.make_async_copy(x, y, sl.at[k]) for k, (x, y) in enumerate(zip(*ends))] for ends in ((ins, tiles), (tiles, outs))]

    def loads(i):
        at = block_rows(i, BQ)
        pairs = [(x.at[at], y.at[at]) for x, y in ((qkv_ref, qkv), (do_ref, do), (o_ref, o), (cos_ref, cos), (sin_ref, sin))]
        return [pltpu.make_async_copy(x, y, sem.at[i, k]) for k, (x, y) in enumerate([*pairs, (lse_ref.at[i], lse.at[i])])]

    def store(i, columns, k):
        at = block_rows(i, BQ), columns
        return pltpu.make_async_copy(out.at[at], out_ref.at[at], sem.at[i, k])

    part, rest = pl.ds(0, NQ), pl.ds(NQ, 2 * HEAD)
    for i in range(blocks):
        begin(loads(i))
    begin(come)
    set_gap(gap)
    dk[...] = jnp.zeros_like(dk)
    dv[...] = jnp.zeros_like(dv)

    def landed(k):
        def f():
            come[k].wait()
            go[k].start()
        return f

    def queries(iq):
        end(loads(iq))
        steps(iq, [None, *[landed(k) for k in range(len(come))]])
        mine = block_rows(iq, BQ)
        qs[...] = rows_of(qkv[mine, :NQ])
        dos[...] = rows_of(do[mine, :])
        dq[...] = jnp.zeros_like(dq)
        delta = (dos[...].astype(F32) * rows_of(o[mine, :]).astype(F32)).T.sum(axis=0, keepdims=True)
        lses = lse[iq] * LOG2E

        def piece(j, masked, first, size):
            here = pl.ds(pl.multiple_of(j * BK + first, size), size)
            keys, values = qkv[here, NQ:NQ + HEAD], qkv[here, NQ + HEAD:]
            strips = [slice(a + (first if masked else 0), a + BQ) for a in range(0, cols, BQ)]
            scores = [dot(keys, qs[at, :], NT) for at in strips]
            dps = [dot(values, dos[at, :], NT) for at in strips]
            for at, s, dp in zip(strips, scores, dps):
                p = jnp.exp2(s * (SCALE * LOG2E) - lses[:, at])
                if masked:
                    p = jnp.where(gap[first:first + size, first:] >= j * BK - iq * BQ, p, 0.0)
                ds = (p * (dp - delta[:, at])).astype(BF)
                dv[here, :] += dot(p.astype(BF), dos[at, :])
                dk[here, :] += dot(ds, qs[at, :])
                dq[:, at] += dot(keys.T, ds)

        def block(j, masked):
            size = BK // 2 if masked else BK
            for first in range(0, BK, size):
                piece(j, masked, first, size)

        key_blocks(iq, block)
        back = (dq[...] * SCALE).T
        for h in range(NQ // HEAD):
            out[mine, h * HEAD:(h + 1) * HEAD] = turn(back[h * BQ:(h + 1) * BQ], cos[mine, :], -sin[mine, :]).astype(BF)
        store(iq, part, 0).start()

    loop(blocks, queries)

    def keys(at):
        out[at, NQ:NQ + HEAD] = turn(dk[at, :] * SCALE, cos[at, :], -sin[at, :]).astype(BF)
        out[at, NQ + HEAD:] = dv[at, :].astype(BF)
    chunked(tokens, BQ, keys)
    for i in range(blocks):
        store(i, rest, 1).start()
    end([*go, *(store(i, part, 0) for i in range(blocks)), *(store(i, rest, 1) for i in range(blocks))])


def attend_bwd(qkv, d_out, out, lse, cos, sin, others):
    tokens, NQ = out.shape
    cols = lse.shape[2]
    table, key = V(cos.shape, F32), V((tokens, HEAD), F32)
    scratch = [V(qkv.shape, BF), V(out.shape, BF), V(out.shape, BF), V(lse.shape, F32), table, table, V(qkv.shape, BF), V((cols, HEAD), BF), V((cols, HEAD), BF),
               V((HEAD, cols), F32), key, key, V((BK, BQ), jnp.int32), *(V(t.shape, BF) for t in others[:-1]), V((EARLY * TILE, others[-1].shape[1]), BF),
               DMA((tokens // BQ, 6)), DMA((len(others),))]
    return call(_attend_bwd, [qkv, d_out, out, lse, cos, sin, *others], [S(t.shape, BF) for t in (qkv, *others)], scratch, 5 * tokens * tokens * NQ, "attend_bwd")


def _front(x_ref, dy_ref, wq_ref, wk_ref, wv_ref, wo_ref, wd_ref, c_ref, s_ref, a_all, qkv_ref, dy_all, dhid, o_ref, lse_ref, cos_ref, sin_ref, h_ref, b_ref, wt_ref, ot_ref,
           tile, small, qkv, o, ot, lse, qs, top, mix, gap, wo, dt, stg, p, s, acc, tr, fr, ss, rs, sb, so, sl, *, n):
    T, D = x_ref.shape
    NQ, NK = wq_ref.shape[1], wk_ref.shape[1]
    turned, Q = NQ + NK, T // 4

    def links(an=None):
        ring = Ring(n)
        of_a, of_dy, of_o = (Links(ss, rs, k * COPIES) for k in range(3))
        if an is not None:
            gather_copies(of_a, ring, an, a_all, T)
        gather_copies(of_dy, ring, dy_ref, dy_all, T)
        return ring, of_a, of_dy, of_o

    pairs = ((x_ref, stg.at[0]), (dy_ref, stg.at[1]), (c_ref, small.at[0]), (s_ref, small.at[1]), (wo_ref, wo),
             (x_ref, stg.at[0]), (qkv, qkv_ref), (o, o_ref), (ot, ot_ref), (lse, lse_ref), (s.at[0], h_ref), (stg.at[1], b_ref))
    copies = [pltpu.make_async_copy(a, b, sl.at[k]) for k, (a, b) in enumerate(pairs)]
    x_in, dy_in, c_in, s_in, wo_in, x_again, *outs = copies
    x_in.start()

    def products(an, w, cos, sin, wt):
        tables = [pltpu.make_async_copy(a, b, so.at[0, k]) for k, (a, b) in enumerate(((cos, cos_ref), (sin, sin_ref)))]
        ring, of_a, of_dy, _ = links(an)
        keep, keep_dy = (pltpu.make_async_copy(a, b.at[ring.me], so.at[1, k]) for k, (a, b) in enumerate(((an, a_all), (stg.at[1], dy_all))))
        place = [pl.ds(0, NQ), pl.ds(NQ, NK), pl.ds(turned, NK)]
        loads = [dy_in, c_in, s_in, wo_in] + [pltpu.make_async_copy(r, w.at[:, c], sb.at[0, k]) for k, (r, c) in enumerate(zip((wq_ref, wk_ref, wv_ref), place))]
        begin(loads)
        ring.barrier()
        x_in.wait()
        for q, k in ((0, RA), (2, LA), (1, RB), (3, LB)):

            def norm(at):
                at = pl.ds(q * Q + at.start, at.size)
                wide = stg[0, at, :].astype(F32)
                an[at, :] = (wide * norm_scale(wide)).astype(BF)
            chunked(Q, 16, norm)
            of_a.start(k)
        of_a.start(MA)
        keep.start()
        end(loads)
        keep_dy.start()

        def table(at):
            row = pl.ds(HEAD + lax.div(at.start, HEAD), 1)
            c0, s0, c1, s1 = small[0, row, :], small[1, row, :], small[0, :HEAD, :], small[1, :HEAD, :]
            cos[at, :] = c0 * c1 - s0 * s1
            sin[at, :] = s0 * c1 + c0 * s1
        chunked(n * T, HEAD, table)
        begin(tables)
        end([keep, keep_dy])

        def work(u, units, x):
            r = dot(x[...], w[...]).astype(BF)
            for k in BOTH:
                rows = slice(k * T // 2, (k + 1) * T // 2)
                place = rows_of_unit(u, units, k, T // 2)
                c, s = cos[place, :], sin[place, :]
                for a in range(0, turned, HEAD):
                    qkv[place, a:a + HEAD] = turn(r[rows, a:a + HEAD].astype(F32), c, s).astype(BF)
                qkv[place, turned:] = r[rows, turned:]

        def turned_round(j):
            slot = lax.rem(j, 2)
            put = lambda j: pltpu.make_async_copy(wt.at[slot], wt_ref.at[:, block_rows(j, TILE)], so.at[1, slot])
            pl.when(j > 1)(lambda: put(j - 2).wait())
            wt[slot] = w[block_rows(j, TILE), :].T
            put(j).start()

        def near():
            of_a.passed_on(RA, LA)
            loop(D // TILE, turned_round)
            of_a.passed_on(RB, LB)
            of_a.start(RE, LE, MB, MC)
            of_dy.start(RA, LA, RB, LB, MA)

        stream(ring, of_a, a_all, tile, sb, None, None, None, work, gather_events(of_a, near))
        end([*tables, *[pltpu.make_async_copy(wt.at[k], wt_ref.at[:, pl.ds(0, TILE)], so.at[1, k]) for k in BOTH]])

    pl.run_scoped(products, V((T, D), BF), V((D, turned + NK), BF), *[V((n * T, HEAD), F32)] * 2, V((2, turned + NK, TILE), BF))
    outs[0].start()
    set_gap(gap)

    def rest(wd):
        ring, _, of_dy, of_o = links()
        wd_in = pltpu.make_async_copy(wd_ref, wd, so.at[0, 0])
        wd_in.start()
        blocks = n * T // BQ

        def attention(iq):
            attend_block(iq, qkv, o, ot, lse, qs, top, mix, gap)
            steps(iq, {blocks - 2: lambda: of_dy.passed_on(RA, LA)})

        loop(blocks, attention)
        begin(outs[1:4])
        of_dy.passed_on(RB, LB)
        of_dy.start(RE, LE, MB, MC)

        def product(shard, rows, then):
            at = pl.ds(pl.multiple_of(shard * T + rows.start, T // 2), rows.size)
            chunked(D, D // RUNS, lambda c: then(c, dot(o[at, :], wo[:, c])))

        scatter = Scatter(ring, of_o, product, stg, p, s, acc, tr, fr)
        scatter.send()
        x_again.start()
        wd_in.wait()

        def work(u, units, x, o):
            def run(c):
                o[:, c] = dot(x[...], wd[c, :], NT).astype(BF)
            chunked(wd.shape[0], TILE, run)

        stream(ring, of_dy, dy_all, tile, sb, dhid, dt, so, work, gather_events(of_dy))
        scatter.pass_on()
        x_again.wait()

        def last(at, total):
            h = (stg[0, at, :].astype(F32) + total).astype(BF)
            s[0, at, :] = h
            h = h.astype(F32)
            stg[1, at, :] = (h * norm_scale(h)).astype(BF)

        scatter.finish(last)
        begin(outs[4:])
        end(outs)
        of_o.sent(R2, L2, R3, L3)

    pl.run_scoped(rest, V(wd_ref.shape, BF))


def front(x, dy, wq, wk, wv, wo, wd, n, cid):
    T, D = x.shape
    NQ, F, tokens = wo.shape[0], wd.shape[0], n * T
    N, cols = NQ + 2 * HEAD, NQ // HEAD * BQ
    stat = (tokens // BQ, 1, cols)
    table, row = S((tokens, HEAD), F32), S((T, D), BF)
    small = angles(jnp.concatenate([jnp.arange(HEAD), jnp.arange(0, tokens, HEAD)]))
    outs = [S((n, T, D), BF), S((tokens, N), BF), S((n, T, D), BF), S((n, T, F), BF), S((tokens, NQ), BF), S(stat, F32), table, table, row, row, S((N, D), BF), S((NQ, tokens), BF)]
    scratch = [V((2, T, D), BF), V((2, *small[0].shape), F32), V((tokens, N), BF), V((tokens, NQ), BF), V((NQ, tokens), BF),
               V(stat, F32), V((cols, HEAD), BF), V((1, cols), F32), V((HEAD + 8, cols), F32), V((BK, BQ), jnp.int32), V((NQ, D), BF), V((2, T, F), BF),
               *scatter_scratch(T, D), DMA((3 * COPIES,)), DMA((3 * COPIES,)), DMA((2, 3)), DMA((2, 3)), DMA((15,))]
    return call(functools.partial(_front, n=n), [x, dy, wq, wk, wv, wo, wd, *small], outs, scratch, 2 * tokens * D * (N + F + NQ), "front", cid)


def _back(t_ref, x_ref, wt_ref, a_ref, dh_all, heads_ref, b_ref, du_ref, dx_ref, by_q, by_k, by_v, by_o, by_up,
          w, t, heads, du, out, ft, stg, p, s, acc, tr, fr, ss, rs, sl, sf, sg, *, n):
    ring, links = Ring(n), Links(ss, rs)
    T, D = x_ref.shape
    NQ, NK = by_q.shape[1], by_k.shape[1]
    columns = [pl.ds(0, NQ), pl.ds(NQ, NK), pl.ds(NQ + NK, NK)]
    pairs = ((t_ref, t), (wt_ref, w), (du_ref, du), (heads_ref, heads), (x_ref, stg.at[0]), (dh_all.at[ring.me], stg.at[1]),
             (s.at[0], dx_ref))
    *first, du_in, heads_in, x_in, dh_in, dx_out = [pltpu.make_async_copy(a, b, sl.at[k]) for k, (a, b) in enumerate(pairs)]
    begin(first)
    ring.barrier()
    end(first)
    begin([du_in, heads_in])
    late = lambda j: [(pl.ds(0, du.shape[2]), by_up.at[block_rows(j - EARLY, TILE)])]
    fill = Fill((([b_ref], du, out, None, [late], EARLY, D // TILE),
                 ([a_ref], t, out, None, [lambda j: [(c, r.at[block_rows(j, TILE)]) for c, r in zip(columns, (by_q, by_k, by_v))]]),
                 ([dh_all], heads, out, NN, [lambda j: [(pl.ds(0, TILE), by_o.at[:, block_rows(j, TILE)])]])), ft, sf, sg)
    fill.fetch(0)

    def product(shard, rows, then):
        chunked(D, D // RUNS, lambda c: then(c, dot(t[shard, rows, :], w[:, c])))

    scatter = Scatter(ring, links, product, stg, p, s, acc, tr, fr)
    scatter.send()
    begin([x_in, dh_in])
    end([du_in, heads_in])
    def beside(k):
        fill.step(k)
        steps(k, {1: scatter.pass_on})
    loop(fill.steps, beside)
    end([x_in, dh_in])

    def last(at, total):
        s[0, at, :] = (stg[1, at, :].astype(F32) + unnorm(stg[0, at, :].astype(F32), total)).astype(BF)

    scatter.finish(last)
    dx_out.start()
    dx_out.wait()
    links.sent(R2, L2, R3, L3)


def back(dqkv, x, wt, ws, a, dh_all, heads, b, du, n, cid):
    T, D = x.shape
    K, NQ, F = dqkv.shape[2], heads.shape[0], du.shape[2]
    scratch = [V((K, D), BF), V(dqkv.shape, BF), V(heads.shape, BF), V(du.shape, BF), V((2, TILE, F), BF), V((2, n, T, TILE), BF), *scatter_scratch(T, D),
               DMA((COPIES,)), DMA((COPIES,)), DMA((8,)), DMA((2,)), DMA((2, 3))]
    outs = [S((T, D), BF), *(S(w.shape, BF) for w in ws), S((NQ, D), BF), S((D - EARLY * TILE, F), BF)]
    return call(functools.partial(_back, n=n), [dqkv, x, wt, a, dh_all, heads, b, du], outs, scratch, 6 * n * T * D * K, "back", cid)


def _land(*refs):
    m = (len(refs) - 2) // 3
    ins, outs, tiles, sem = refs[:m], refs[m + 1:2 * m + 1], refs[2 * m + 1:-1], refs[-1]
    outs = [*outs[:-1], outs[-1].at[pl.ds(EARLY * TILE, ins[-1].shape[0])]]
    come = [pltpu.make_async_copy(a, b, sem.at[k]) for k, (a, b) in enumerate(zip(ins, tiles))]
    go = [pltpu.make_async_copy(a, b, sem.at[k]) for k, (a, b) in enumerate(zip(tiles, outs))]
    begin(come)
    for a, b in zip(come, go):
        a.wait()
        b.start()
    end(go)


def land(arrays, whole):
    shapes = [S(t.shape, BF) for t in (*arrays[:-1], whole)]
    return call(_land, [*arrays, whole], shapes, [*(V(t.shape, BF) for t in arrays), DMA((len(arrays),))], 0, "land", aliases={len(arrays): len(arrays) - 1})


def mlp_links(b_ref, bg, frm, stg, s3, s1, p1, p3, tr, fr, ss, rs, n):
    ring, links = Ring(n), Links(ss, rs)
    T = b_ref.shape[0]
    H, Q = T // 2, T // 4
    first = pl.ds(0, Q)
    frp, frn = fr.at[0], fr.at[1]
    nx, pv, mt = ring.next, ring.prev, ring.mate
    lo, hi = pl.ds(0, H), pl.ds(H, H)
    gather_copies(links, ring, b_ref, bg, T, True)
    at = lambda ref: [ref.at[k] for k in range(ref.shape[0])]
    pa, pb, pc, pd, sa, sb1, sc, sd1, even, odd, on, off = [*at(p1), *at(s1), *at(stg), *at(tr)]
    for k, src, dst, to in ((M5, odd, frm, mt), (M0, odd.at[hi], pa, mt), (M1, even, p3, mt), (M2, even.at[hi], pb, mt), (M3, odd.at[hi], pc, mt), (M4, even.at[hi], pd, mt),
                            (R1, s3.at[lo], on, nx), (L1, s3.at[hi], off, pv),
                            (L2, sa.at[first], frn.at[first], pv), (L5, sb1.at[first], frn.at[pl.ds(Q, Q)], pv),
                            (R2, sa.at[pl.ds(Q, Q)], frp.at[pl.ds(H, Q)], nx), (R5, sb1.at[pl.ds(Q, Q)], frp.at[pl.ds(H + Q, Q)], nx),
                            (R3, sc.at[first], frp.at[first], nx), (R4, sd1.at[first], frp.at[pl.ds(Q, Q)], nx),
                            (L3, sc.at[pl.ds(Q, Q)], frn.at[pl.ds(H, Q)], pv), (L4, sd1.at[pl.ds(Q, Q)], frn.at[pl.ds(H + Q, Q)], pv)):
        links.put(k, src, dst, to)
    return ring, links


def pair_sum(acc, p1, s1, tr, k, base=0, first=None):
    H = s1.shape[1]

    def add(at, *further):
        v = acc[pl.ds(base + at.start, at.size), :] + p1[k, at, :].astype(F32)
        s1[k, at, :] = sum([tr[t].astype(F32) for t in further], v).astype(BF)

    if first is None:
        chunked(H, 16, add)
    else:
        for side in BOTH:
            chunked(H // 2, 16, lambda at: add(pl.ds(side * (H // 2) + at.start, at.size), (side, pl.ds(first + at.start, at.size))))


def _units(b_ref, dhid_ref, wg_ref, wu_ref, bg, hid, dgo, duo, own, frm, bt, acc, stg, s3, s1, p1, p3, tr, fr, ss, rs, sw, sb, sd, so, sl, n, wg, wu, dht, st):
    ring, links = mlp_links(b_ref, bg, frm, stg, s3, s1, p1, p3, tr, fr, ss, rs, n)
    T, D = b_ref.shape
    F = wg_ref.shape[1]
    H, NC, NB = T // 2, F // 3, D // 4
    me, nx, pv, mt = ring.me, ring.next, ring.prev, ring.mate
    Q0, Q1, Q2, Q3 = range(4)
    quarters = lambda *shards: tuple((shard, q) for shard in shards for q in range(4))
    pvm, nxm = ring.prevm, ring.nextm
    units = [quarters(me), ((pv, Q0), (nx, Q2), (pvm, Q0), (nxm, Q2)), ((pv, Q1), (nx, Q3), (pvm, Q1), (nxm, Q3)), quarters(ring.opp), quarters(ring.oppm),
             ((nx, Q0), (pv, Q2), (nxm, Q0), (pvm, Q2)), ((nx, Q1), (pv, Q3), (nxm, Q1), (pvm, Q3)), quarters(mt)]
    count = len(units)

    def fetch(u, slot):
        return moves(u, units, bg, bt.at[slot], sb.at[slot]) + moves(u, units, dhid_ref, dht.at[slot], sd.at[slot])

    def store(u):
        return [c for m, ref in enumerate((hid, dgo, duo)) for c in moves(u, units, ref, st.at[m], so.at[m], True)]

    def weights(j):
        s = block_rows(j, NC)
        return [pltpu.make_async_copy(a.at[:, s], b.at[:, s], sw.at[k, j]) for k, (a, b) in enumerate(((wg_ref, wg), (wu_ref, wu)))]

    pairs = ((b_ref, bt.at[0]), (dhid_ref.at[me], dht.at[0]), (bt.at[0], bg.at[me]), (acc, own))
    *first, keep, own_out = [pltpu.make_async_copy(a, b, sl.at[k]) for k, (a, b) in enumerate(pairs)]
    begin(first)
    for j in range(F // NC):
        begin(weights(j))
    ring.barrier()
    links.start(RA, LA, RB, LB, MA)
    end(first)
    keep.start()

    pair = functools.partial(pair_sum, acc, p1, s1, tr)

    def late0():
        links.passed_on(RA, LA)
        links.start(MB, MC)

    def post0():
        keep.wait()
        own_out.start()
        links.got(MB, MC)
        begin(fetch(1, 1))

    def mid1():
        own_out.wait()
        links.passed_on(RB)
        links.start(RE)
        links.passed_on(LB)
        links.start(LE, MH, MI)

    def late1():
        links.got(MH, MI)
        begin(fetch(2, 0))

    def mid2():
        links.got(M0)
        pair(0)
        links.start(L2, R2)

    def post2():
        links.start(M2)
        far()
        begin(fetch(3, 1))

    def mid3():
        links.got(M2)
        pair(1)
        links.start(L5, R5)

    def late3():
        links.got(MD, ME)
        begin(fetch(4, 0))
        links.sent(M2)

    def late4():
        links.got(MF, MG)
        begin(fetch(5, 1))

    def mid5():
        links.got(M1)

        def add(at):
            s3[at, :] = (acc[at, :] + p3[at, :].astype(F32)).astype(BF)
        chunked(T, 16, add)
        links.start(R1, L1)
        links.sent(M0)

    def late6():
        links.got(MA)
        begin(fetch(7, 1))

    def pairs_left():
        links.got(M3, R1, L1)
        pair(2, 0, 0)
        links.start(R3, L3)
        links.got(M4)
        pair(3, H, H // 2)
        links.start(R4, L4)

    def post7():
        links.start(M5)
        end(store(7))

    _, _, _, far, _, last, _ = gather_events(links)
    starting = lambda *ks: lambda: links.start(*ks)
    mids = [None, mid1, mid2, mid3, last, mid5, lambda: links.sent(M1), lambda: links.sent(M3)]
    lates = [late0, late1, None, late3, late4, lambda: begin(fetch(6, 0)), late6]
    posts = [post0, starting(M0), post2, None, starting(M1), starting(M3), starting(M4), post7]

    def forth_unit(u, slot):
        @pl.when(u > 0)
        def _():
            end(fetch(u, slot))
            end(store(u - 1))

        def forth(j):
            @pl.when(u == 0)
            def _():
                end(weights(j))
            s = block_rows(j, NC)
            x = bt[slot]
            gate, up = dot(x, wg[:, s]), dot(x, wu[:, s])
            d = dht[slot, :, s].astype(F32)
            sig = jax.nn.sigmoid(gate)
            act = gate * sig
            for m, v in enumerate((act * up, d * up * (sig + act * (1 - sig)), d * act)):
                st[m, :, s] = v.astype(BF)
            pl.when((u == count - 1) & (j == 0))(pairs_left)

        loop(F // NC, forth)
        begin(store(u))

    def unit(u):
        slot = lax.rem(u, 2)
        forth_unit(u, slot)
        steps(u, mids)
        among = lambda *us: functools.reduce(jnp.logical_or, [u == k for k in us])
        side = jnp.where(among(2, 4, 6), 0, 1)

        def back(c):
            v = dot(st[1], wg[c, :], NT) + dot(st[2], wu[c, :], NT)

            @pl.when(among(0, 3))
            def _():
                acc[:, c] = v

            @pl.when(among(4, 7))
            def _():
                stg[side, :, c] = v.astype(BF)

            @pl.when(among(1, 2, 5, 6))
            def _():
                acc[pl.ds(pl.multiple_of(jnp.where(u == 6, H, 0), H), H), c] = v[:H]
                stg[side, H:, c] = v[H:].astype(BF)

        half = D // NB // 2
        loop(half, lambda j: back(block_rows(j, NB)))
        steps(u, lates)
        loop(D // NB, lambda j: back(block_rows(j, NB)), half)
        steps(u, posts)

    loop(count, unit)


def _middle(b_ref, dhid_ref, wg_ref, wu_ref, h_ref, dy_ref, wo_ref, dy_all, bg, hid, dgo, duo, dh_all, out, by_down, by_gate, by_up, own, frm,
            bt, acc, stg, s3, s1, p1, p3, tr, fr, ot, ss, rs, sw, sb, sd, so, sl, sf, sg, *, n):
    T, D = b_ref.shape
    F, NQ = wg_ref.shape[1], wo_ref.shape[0]
    shared = (bt, acc, stg, s3, s1, p1, p3, tr, fr, ss, rs)
    pl.run_scoped(functools.partial(_units, b_ref, dhid_ref, wg_ref, wu_ref, bg, hid, dgo, duo, own, frm, *shared, sw, sb, sd, so, sl, n),
                  V((D, F), BF), V((D, F), BF), V((2, T, F), BF), V((3, T, F), BF))

    def rest(fixed, left, tile, wo):
        ring, links = mlp_links(b_ref, bg, frm, *shared[2:], n)
        of_dh = Links(ss, rs, COPIES)
        gather_copies(of_dh, ring, stg.at[0], dh_all, T)
        pairs = ((hid, fixed.at[1]), (dgo, fixed.at[0]), (duo, fixed.at[1]), (wo_ref, wo), (own, acc), (frm, bt.at[0]), (h_ref, bt.at[1]), (dy_ref, s3),
                 (stg.at[0], dh_all.at[ring.me]))
        hid_in, dg_in, du_in, wo_in, own_in, frm_in, *rows_in, keep = [pltpu.make_async_copy(a, b, sl.at[k]) for k, (a, b) in enumerate(pairs)]
        side = lambda ref: lambda j: [(pl.ds(0, F), ref.at[block_rows(j, TILE)])]
        fill = Fill((([dy_all], fixed.at[1], left, TN, [lambda j: [(pl.ds(a, TILE), by_down.at[pl.ds(a, TILE), block_rows(j, TILE)]) for a in range(0, F, TILE)]]),
                     ([bg, bg], fixed, left, None, [side(by_gate), side(by_up)], 0, D // TILE + EARLY)), tile, sf, sg)
        own_in.start()
        hid_in.start()
        fill.fetch(0)
        links.sent(R1, L1)
        begin(rows_in)
        own_in.wait()
        add_rows(links, acc, (R2, R5), fr.at[0], T // 2)
        add_rows(links, acc, (L2, L5), fr.at[1], 0)
        hid_in.wait()

        def mates_part():
            links.got(M5)
            frm_in.start()

        def scattered():
            end([frm_in, *rows_in])
            links.sent(M4)

            def add(at):
                acc[at, :] += bt[0, at, :].astype(F32)
            chunked(T, 16, add)

            def last(at, total):
                stg[0, at, :] = (s3[at, :].astype(F32) + unnorm(bt[1, at, :].astype(F32), total)).astype(BF)

            finish(links, acc, fr, last, (R3, R4), (L3, L4))
            of_dh.start(RA, LA, RB, LB, MA)
            keep.start()

        def near():
            of_dh.passed_on(RB, LB)
            of_dh.start(RE, LE, MB, MC)

        def work(u, units, x, o):
            o[...] = dot(x[...], wo[...], NT).astype(BF)

        mate, _, mates, far, fars, last, lasts = gather_events(of_dh)
        events = {0: mates_part, 1: scattered, 3: lambda: begin([dg_in, wo_in]), 5: lambda: (mate(), end([keep, wo_in, dg_in]), of_dh.passed_on(RA, LA)),
                  7: du_in.start, 8: near, 10: mates, 14: far, 15: lambda: (fars(), du_in.wait()), fill.steps - 1: last, fill.steps: lasts}
        schedule = (6, 7, 11, 12, 16, 17, fill.steps, fill.steps + 1)
        stream(ring, of_dh, dh_all, bt, sb, out, ot, sd, work, events, schedule, lambda k: pl.when(k < fill.steps)(lambda: fill.step(k)))
        links.sent(*GATHER, MH, MI, R2, R3, R4, R5, L2, L3, L4, L5, M5)

    pl.run_scoped(rest, V((2, n, T, F), BF), V((2, TILE, F), BF), V((2, n, T, TILE), BF), V((NQ, D), BF))


def middle(b, dhid, wg, wu, h, dy, wo, dy_all, n, cid):
    T, D = b.shape
    F, NQ = wg.shape[1], wo.shape[0]
    H = T // 2
    row, halves = V((T, D), BF), V((4, H, D), BF)
    scratch = [V((2, T, D), BF), V((T, D), F32), V((2, T, D), BF), row, halves, halves, row, V((2, H, D), BF), V((2, T, D), BF), V((2, T, NQ), BF),
               DMA((2 * COPIES,)), DMA((2 * COPIES,)), DMA((2, 3)), DMA((2, 4)), DMA((2, 4)), DMA((3, 4)), DMA((9,)), DMA((2,)), DMA((2, 3))]
    wide, full, narrow = S((n, T, F), BF), S((n, T, D), BF), S((D, F), BF)
    outs = [full, wide, wide, wide, full, S((n, T, NQ), BF), S((F, D), BF), narrow, narrow, S((T, D), F32), S((T, D), BF)]
    got = call(functools.partial(_middle, n=n), [b, dhid, wg, wu, h, dy, wo, dy_all], outs, scratch, 14 * n * T * D * F, "middle", cid)
    return got[4:9], got[0], got[3]


def solution(mesh):
    n = mesh.shape["tp"]

    def step(x, dy, wq, wk, wv, wo, wg, wu, wd):
        x, dy = x[0], dy[0]
        blocks = lambda t: t.reshape(n, -1, t.shape[1])
        a, qkv, dy_all, dhid, heads, lse, cos, sin, h, b, wt, heads_t = front(x, dy, wq, wk, wv, wo, wd, n, 0)
        (dh_all, d_heads, *by_mlp), b, du = middle(b, dhid, wg, wu, h, dy, wo, dy_all, n, 1)
        dqkv, by_down, by_gate, by_up = attend_bwd(qkv, flat(d_heads), heads, lse, cos, sin, by_mlp)
        dx, *by_qkvo, by_up = land(back(blocks(dqkv), x, wt, [wq, wk, wv], a, dh_all, heads_t, b, du, n, 2), by_up)
        return dx[None], *by_qkvo, by_gate, by_up, by_down

    states, by_columns, by_rows = P("dp", "tp", None), P(None, "tp"), P("tp", None)
    weights = (by_columns, by_columns, by_columns, by_rows, by_columns, by_columns, by_rows)
    own = tuple(P("dp", "tp") if spec == by_columns else P(("dp", "tp"), None) for spec in weights)
    return jax.shard_map(step, mesh=mesh, in_specs=(states, states, *weights), out_specs=(states, *own), check_vma=False)
```

```python
import functools

import jax
import jax.numpy as jnp
from jax import lax
from jax.experimental import pallas as pl
from jax.experimental.pallas import tpu as pltpu
from jax.sharding import PartitionSpec as P

BF, F32 = jnp.bfloat16, jnp.float32
HEAD = 128
THETA = 10000
NEG = -1e30
HIDDEN = 2 * NEG
LOG2E = 1.4426950408889634
SCALE = HEAD**-0.5
MOST = 67_000_000
BQ = BK = 512
TILE = 512
EARLY = 3
NN, NT, TN = ((((a,), (b,)), ((), ())) for a, b in ((1, 0), (1, 1), (0, 0)))
ANY = pl.BlockSpec(memory_space=pl.ANY)
S, V, DMA = jax.ShapeDtypeStruct, pltpu.VMEM, pltpu.SemaphoreType.DMA

RA, RB, RC, RD, RE, LA, LB, LC, LD, LE, MA, MB, MC, MD, ME, MF, MG = GATHER = range(17)
R1, R2, R3, R4, R5, L1, L2, L3, L4, L5, M0, M1, M2, M3, M4, M5, M6, M7, MH, MI = range(17, 37)
COPIES = 37
RUNS = 4
LO, HI = BOTH = range(2)


def dot(a, b, dims=NN, **kw):
    return lax.dot_general(a, b, dims, preferred_element_type=F32, **kw)


def norm_scale(wide):
    return lax.rsqrt(jnp.mean(wide * wide, -1, keepdims=True) + 1e-6)


def unnorm(wide, d):
    scale = norm_scale(wide)
    return d * scale - wide * (scale * scale * scale * jnp.mean(d * wide, -1, keepdims=True))


def turn(t, cos, sin):
    return t * cos + pltpu.roll(t, HEAD // 2, 1) * sin


def angles(places):
    half = HEAD // 2
    a = places.astype(F32)[:, None] * THETA ** (-jnp.arange(half, dtype=F32) / half)
    cos, sin = jnp.cos(a), jnp.sin(a)
    return jnp.concatenate([cos, cos], -1), jnp.concatenate([-sin, sin], -1)


class Ring:
    def __init__(self, n):
        self.me = lax.axis_index("tp")
        core, chips = lax.rem(self.me, 2), n // 2
        chip = [lax.rem(lax.div(self.me, 2) + k, chips) for k in range(chips)]
        self.next, self.opp, self.prev = [2 * c + core for c in chip[1:]]
        self.mate, self.nextm, self.oppm, self.prevm = [2 * c + 1 - core for c in chip]

    def barrier(self):
        b = pltpu.get_barrier_semaphore()
        near = (self.next, self.prev, self.mate)
        for d in near:
            pl.semaphore_signal(b, inc=1, device_id={"tp": d}, device_id_type=pl.DeviceIdType.MESH)
        pl.semaphore_wait(b, len(near))


class Links:
    def __init__(self, ss, rs, base=0):
        self.ss, self.rs, self.base, self.made = ss, rs, base, {}

    def put(self, k, src, dst, dev):
        self.made[k] = lambda: pltpu.make_async_remote_copy(src_ref=src, dst_ref=dst, send_sem=self.ss.at[self.base + k], recv_sem=self.rs.at[self.base + k],
                                                            device_id={"tp": dev}, device_id_type=pl.DeviceIdType.MESH)

    def start(self, *ks):
        for k in ks:
            self.made[k]().start()

    def got(self, *ks):
        for k in ks:
            self.made[k]().wait_recv()

    def sent(self, *ks):
        for k in ks:
            self.made[k]().wait_send()

    def passed_on(self, *ks):
        for k in ks:
            self.got(k)
            self.start(k + 2)


def flat(t):
    return t.reshape(-1, t.shape[-1])


def begin(copies):
    for c in copies:
        c.start()


def end(copies):
    for c in copies:
        c.wait()


def pick(u, values):
    out = values[0]
    for k, v in enumerate(values):
        out = jnp.where(u == k, v, out)
    return out


def steps(u, events):
    for k, f in events.items() if isinstance(events, dict) else enumerate(events):
        def run(f=f):
            f()
        if f is not None:
            pl.when(u == k)(run)


def loop(count, f, first=0):
    def body(k, _):
        f(k)
    lax.fori_loop(first, count, body, None)


def block_rows(i, size):
    return pl.ds(pl.multiple_of(i * size, size), size)


def upto(size):
    return pl.ds(0, size)


def chunked(size, width, f):
    loop(size // width, lambda j: f(block_rows(j, width)))


def gather_copies(links, ring, src, dst, T, fine=False):
    H, Q = T // 2, T // 4
    me, nx, pv, mt, opp = ring.me, ring.next, ring.prev, ring.mate, ring.opp
    for k, slot, a, rows, to in ((RA, me, 0, Q, nx), (RB, me, Q, Q, nx), (RC, pv, 0, Q, nx), (RD, pv, Q, Q, nx), (RE, me, H, H, nx),
                                 (LA, me, H, Q, pv), (LB, me, H + Q, Q, pv), (LC, nx, H, Q, pv), (LD, nx, H + Q, Q, pv), (LE, me, 0, H, pv),
                                 (MA, me, 0, T, mt), (MB, pv, 0, Q if fine else H, mt), (MC, nx, H, Q if fine else H, mt),
                                 (MH, pv, Q, Q, mt), (MI, nx, H + Q, Q, mt), (MD, opp, 0, H, mt), (ME, opp, H, H, mt), (MF, pv, H, H, mt), (MG, nx, 0, H, mt)):
        at = pl.ds(a, rows)
        links.put(k, src.at[at] if slot is me else dst.at[slot, at], dst.at[slot, at], to)


def whole(shard):
    return (shard, LO), (shard, HI)


def moves(u, units, far, near, sem, back=False):
    parts = len(units[0])
    size = near.shape[0] // parts
    out = []
    for k in range(parts):
        shard, place = (pick(u, [x[k][m] for x in units]) for m in BOTH)
        ends = far.at[shard, block_rows(place, size)], near.at[pl.ds(k * size, size)]
        out.append(pltpu.make_async_copy(*(ends[::-1] if back else ends), sem.at[k]))
    return out


def rows_of_unit(u, units, k, H):
    shard, half = (pick(u, [x[k][m] for x in units]) for m in BOTH)
    return pl.ds(pl.multiple_of((2 * shard + half) * H, H), H)


def stream(ring, links, src, tile, sin, dst, out, sout, work, events, schedule=range(8), beside=None):
    units = [whole(ring.me), whole(ring.mate), ((ring.prev, LO), (ring.next, HI)), ((ring.prevm, LO), (ring.nextm, HI)), whole(ring.opp),
             whole(ring.oppm), ((ring.prev, HI), (ring.next, LO)), ((ring.prevm, HI), (ring.nextm, LO))]
    fetch = lambda u, slot: moves(u, units, src, tile.at[slot], sin.at[slot])
    store = lambda u, slot: moves(u, units, dst, out.at[slot], sout.at[slot], True)
    latest = lambda k: sum(jnp.where(k < s, 0, 1) for s in schedule) - 1

    def fetch_for(k):
        u = latest(k)

        @pl.when(latest(k - 1) < u)
        def _():
            begin(fetch(u, lax.rem(u, 2)))

    fetch_for(0)

    def step(k):
        if beside is not None:
            beside(k)
        u = latest(k)

        @pl.when(latest(k - 1) < u)
        def _():
            slot = lax.rem(u, 2)
            end(fetch(u, slot))

            if dst is None:
                work(u, units, tile.at[slot])
            else:
                pl.when(u > 1)(lambda: end(store(u - 2, slot)))
                work(u, units, tile.at[slot], out.at[slot])
                begin(store(u, slot))

        steps(k, events)
        fetch_for(k + 1)

    loop(schedule[-1] + 1, step)
    if dst is not None:
        end(store(len(units) - 2, 0) + store(len(units) - 1, 1))
    links.sent(*GATHER)


class Fill:
    def __init__(self, jobs, tile, sin, sout):
        self.tile, self.sin, self.sout, self.jobs, at = tile, sin, sout, [], 0
        for srcs, fixed, out, right, ends, *tiles in jobs:
            per = srcs[0].shape[2] // TILE
            first, last = tiles or (0, per * len(srcs))
            self.jobs.append((at, last - first, first, per, srcs, fixed, out, right, ends))
            at += last - first
        self.steps = at

    def load(self, src, j, slot):
        return pltpu.make_async_copy(src.at[:, :, block_rows(j, TILE)], self.tile.at[slot], self.sin.at[slot])

    def fetch(self, k):
        for at, count, first, per, srcs, *_ in self.jobs:
            i = k - at + first
            for m, src in enumerate(srcs):
                mine = (k >= at) & (k < at + count) & (lax.div(i, per) == m)
                pl.when(mine)(lambda: begin([self.load(src, i - m * per, lax.rem(k, 2))]))

    def step(self, k):
        slot = lax.rem(k, 2)
        end([self.load(self.jobs[0][4][0], 0, slot)])
        self.fetch(k + 1)
        for at, count, first, per, srcs, fixed, out, right, ends in self.jobs:
            @pl.when((k >= at) & (k < at + count))
            def _():
                which, j = lax.div(k - at + first, per), lax.rem(k - at + first, per)
                store = lambda m, j, slot: [pltpu.make_async_copy(out.at[slot, :, a], b, self.sout.at[slot, i]) for i, (a, b) in enumerate(ends[m](j))]
                pl.when(k > at + 1)(lambda: end(store(0, j, slot)))
                t = self.tile[slot].reshape(-1, TILE)
                f = flat(fixed[which] if len(srcs) > 1 else fixed[...])
                r = dot(f, t, right) if right else dot(t, f, TN)
                for a in range(0, r.shape[0], TILE):
                    out[slot, :, (a if right else 0):(a if right else 0) + r.shape[1]] = r[a:a + TILE].astype(BF)
                for m in range(len(srcs)):
                    pl.when(which == m)(lambda: begin(store(m, j, slot)))
                pl.when(k == at + count - 1)(lambda: end(store(0, j, slot) + store(0, j, 1 - slot)))


def gather_events(links, near=None):
    def far():
        links.got(RC, RD)
        links.start(MD)
        links.got(LC, LD)
        links.start(ME)

    def last():
        links.got(RE)
        links.start(MF)
        links.got(LE)
        links.start(MG)

    got = lambda *ks: lambda: links.got(*ks)
    return [got(MA), near, got(MB, MC), far, got(MD, ME), last, got(MF, MG)]


def add_rows(links, acc, ms, fr, half):
    def add(at):
        at = pl.ds(half + at.start, at.size)
        acc[at, :] += fr[at, :].astype(F32)
    links.got(*ms)
    chunked(acc.shape[0] // 2, 16, add)


def finish(links, acc, fr, last, rs=(R3,), ls=(L3,), out=None):
    H = acc.shape[0] // 2
    halves = [pl.ds(k * H, H) for k in BOTH]
    for ms, k in ((rs, LO), (ls, HI)):
        def total(at):
            at = pl.ds(k * H + at.start, at.size)
            last(at, acc[at, :] + fr[k, at, :].astype(F32))
        links.got(*ms)
        chunked(H, 16, total)
        if out is not None:
            begin(out(k, halves[k]))
    if out is not None:
        end([c for k in BOTH for c in out(k, halves[k])])


class Scatter:
    def __init__(self, ring, links, product, stg, p, s, acc, tr, fr):
        self.ring, self.links, self.product, self.stg, self.p, self.s, self.acc, self.tr, self.fr = ring, links, product, stg, p, s, acc, tr, fr
        T = acc.shape[0]
        H = T // 2
        nx, pv, mt = ring.next, ring.prev, ring.mate
        self.every, self.lo, self.hi = every, lo, hi = upto(T), upto(H), pl.ds(H, H)
        at = lambda ref: [ref.at[k] for k in range(ref.shape[0])]
        even, odd, pa, pb, pc, pd, so, sn, sp, on, off, fp, fn = [*at(stg), *at(p), *at(s), *at(tr), *at(fr)]
        NB = acc.shape[1] // RUNS
        for j, k in enumerate((M0, M5, M6, M7)):
            links.put(k, even.at[:, pl.ds(j * NB, NB)], pa.at[:, pl.ds(j * NB, NB)], mt)
        for k, src, dst, to in ((M2, odd, pb, mt), (M3, even, pc, mt), (M4, odd, pd, mt),
                                (R1, so.at[lo], on, nx), (L1, so.at[hi], off, pv), (R2, sn.at[hi], fp.at[hi], nx), (L2, sp.at[lo], fn.at[lo], pv),
                                (R3, sn.at[lo], fp.at[lo], nx), (L3, sp.at[hi], fn.at[hi], pv)):
            links.put(k, src, dst, to)

    def send(self):
        links, ring, stg, p, s, acc = self.links, self.ring, self.stg, self.p, self.s, self.acc
        runs = (M0, M5, M6, M7)
        shards = (ring.oppm, ring.opp, ring.nextm, ring.prevm, ring.next, ring.prev, ring.mate, ring.me)
        got, sent, start = ((lambda f: lambda *ks: lambda: f(*ks))(f) for f in (links.got, links.sent, links.start))
        before = [None, None, None, sent(*runs), got(M2), got(M3), sent(M2)]
        after = [None, start(R1, L1), start(M2), start(M3), start(R2), start(L2), start(M4)]

        def step(i):
            steps(i, before)

            def then(c, v):
                j = lax.div(c.start, c.size)

                def to_mate(k, on=()):
                    def f():
                        stg[k, :, c] = v.astype(BF)
                        steps(j, on)
                    return f

                def to_chip(k, rows, wait=()):
                    def f():
                        steps(j, wait)
                        s[k, rows, c] = (v[rows.start:rows.start + rows.size] + p[k, rows, c].astype(F32)).astype(BF)
                    return f

                def keep():
                    acc[:, c] = v

                steps(i, [to_mate(0, [start(k) for k in runs]), to_chip(0, self.every, [got(k) for k in runs]), to_mate(1), to_mate(0), to_chip(1, self.hi),
                          to_chip(2, self.lo), to_mate(1), keep])

            self.product(pick(i, shards), self.every, then)
            steps(i, after)

        loop(len(shards), step)
        links.sent(M3, M4)

    def pass_on(self):
        H = self.lo.size

        def step(i):
            rows = block_rows(i, H)
            steps(i, [lambda: self.links.got(R1), lambda: self.links.got(L1)])

            def then(c, v):
                self.s[1 + i, rows, c] = (v + self.p[1 + i, rows, c].astype(F32) + self.tr[i, :, c].astype(F32)).astype(BF)
            self.product(pick(i, (self.ring.next, self.ring.prev)), rows, then)
            steps(i, [lambda: self.links.start(R3), lambda: self.links.start(L3)])

        loop(2, step)

    def finish(self, last, out):
        self.links.sent(R1, L1)
        p = self.p.at[3]
        for ms, fr, half in (([M4], p, self.hi), ([], p, self.lo), ([R2], self.fr.at[LO], self.hi), ([L2], self.fr.at[HI], self.lo)):
            add_rows(self.links, self.acc, ms, fr, half.start)
        finish(self.links, self.acc, self.fr, last, out=out)


def scatter_scratch(T, D):
    return [V((2, T, D), BF), V((4, T, D), BF), V((3, T, D), BF), V((T, D), F32), V((2, T // 2, D), BF), V((2, T, D), BF)]


def call(body, args, outs, scratch, flops, name, cid=None, aliases=()):
    return pl.pallas_call(
        body, in_specs=[ANY] * len(args), out_specs=[ANY] * len(outs), out_shape=outs, scratch_shapes=scratch, name=name, input_output_aliases=dict(aliases),
        compiler_params=pltpu.CompilerParams(collective_id=cid, has_side_effects=True, vmem_limit_bytes=MOST),
        cost_estimate=pl.CostEstimate(flops=flops, bytes_accessed=sum(t.size for t in (*args, *outs)), transcendentals=0),
    )(*args)


def rows_of(t):
    return jnp.concatenate([t[:, a:a + HEAD] for a in range(0, t.shape[1], HEAD)], axis=0)


def set_gap(gap):
    gap[...] = lax.broadcasted_iota(jnp.int32, gap.shape, 1) - lax.broadcasted_iota(jnp.int32, gap.shape, 0)


def key_blocks(iq, block):
    seen = lax.div(iq * BQ + 1, BK)
    loop(seen, lambda j: block(j, False))
    loop(lax.div((iq + 1) * BQ + BK - 1, BK), lambda j: block(j, True), seen)


def attend_block(iq, qkv, o_ref, ot_ref, lse_ref, qs, top, mix, gap):
    NQ = o_ref.shape[1]
    cols = qs.shape[0]
    mine = block_rows(iq, BQ)
    qs[...] = rows_of(qkv[mine, :NQ])
    top[...] = jnp.full_like(top, NEG)
    mix[...] = jnp.zeros_like(mix)
    ones = jnp.ones((8, BK), BF)
    strips = [slice(a, a + BQ) for a in range(0, cols, BQ)]

    def block(j, masked):
        here = block_rows(j, BK)
        keys = qkv[here, NQ:NQ + HEAD]
        values = jnp.concatenate([qkv[here, NQ + HEAD:].T, ones], axis=0)
        scores = [dot(keys, qs[at, :], NT) for at in strips]
        ps, keeps = [], []
        for at, s in zip(strips, scores):
            if masked:
                s = jnp.where(gap[...] >= j * BK - iq * BQ, s, HIDDEN)
            old = top[:, at]
            new = jnp.maximum(old, s.max(axis=0, keepdims=True))
            top[:, at] = new
            ps.append(jnp.exp2((s - new) * (SCALE * LOG2E)).astype(BF))
            keeps.append(jnp.exp2((old - new) * (SCALE * LOG2E)))
        for at, p, keep in zip(strips, ps, keeps):
            mix[:, at] = mix[:, at] * keep + dot(values, p)

    key_blocks(iq, block)
    total = mix[HEAD:HEAD + 1, :]
    out = mix[:HEAD, :] * (1 / total)
    for h in range(NQ // HEAD):
        part = out[:, h * BQ:(h + 1) * BQ]
        ot_ref[h * HEAD:(h + 1) * HEAD, mine] = part.astype(BF)
        o_ref[mine, h * HEAD:(h + 1) * HEAD] = part.T.astype(BF)
    lse_ref[iq] = top[...] * SCALE + jnp.log(total)


def _attend_bwd(qkv_ref, do_ref, o_ref, lse_ref, cos_ref, sin_ref, *refs):
    ins, (out_ref, *outs), (qkv, do, o, lse, cos, sin, out, qs, dos, dq, dk, dv, gap, *tiles, sem, sl) = refs[:3], refs[3:7], refs[7:]
    NQ = do.shape[1]
    tokens, cols = dk.shape[0], qs.shape[0]
    blocks = tokens // BQ
    ins, outs = ([*x[:-1], x[-1].at[upto(EARLY * TILE)]] for x in (ins, outs))
    come, go = [[pltpu.make_async_copy(x, y, sl.at[k]) for k, (x, y) in enumerate(zip(*ends))] for ends in ((ins, tiles), (tiles, outs))]

    def loads(i):
        at = block_rows(i, BQ)
        pairs = [(x.at[at], y.at[at]) for x, y in ((qkv_ref, qkv), (do_ref, do), (o_ref, o), (cos_ref, cos), (sin_ref, sin))]
        return [pltpu.make_async_copy(x, y, sem.at[i, k]) for k, (x, y) in enumerate([*pairs, (lse_ref.at[i], lse.at[i])])]

    def store(i, columns, k):
        at = block_rows(i, BQ), columns
        return pltpu.make_async_copy(out.at[at], out_ref.at[at], sem.at[i, k])

    part, rest = upto(NQ), pl.ds(NQ, 2 * HEAD)
    for i in range(blocks):
        begin(loads(i))
    begin(come)
    set_gap(gap)
    dk[...] = jnp.zeros_like(dk)
    dv[...] = jnp.zeros_like(dv)

    def landed(*ks):
        def f():
            for k in ks:
                come[k].wait()
                go[k].start()
        return f

    def queries(iq):
        end(loads(iq))
        steps(iq, {blocks - 2: landed(0), blocks - 1: landed(*range(1, len(come)))})
        mine = block_rows(iq, BQ)
        qs[...] = rows_of(qkv[mine, :NQ])
        dos[...] = rows_of(do[mine, :])
        dq[...] = jnp.zeros_like(dq)
        delta = (dos[...].astype(F32) * rows_of(o[mine, :]).astype(F32)).T.sum(axis=0, keepdims=True)
        lses = lse[iq] * LOG2E

        def piece(j, masked, first, size):
            here = pl.ds(pl.multiple_of(j * BK + first, size), size)
            keys, values = qkv[here, NQ:NQ + HEAD], qkv[here, NQ + HEAD:]
            strips = [slice(a + (first if masked else 0), a + BQ) for a in range(0, cols, BQ)]
            scores = [dot(keys, qs[at, :], NT) for at in strips]
            dps = [dot(values, dos[at, :], NT) for at in strips]
            for at, s, dp in zip(strips, scores, dps):
                p = jnp.exp2(s * (SCALE * LOG2E) - lses[:, at])
                if masked:
                    p = jnp.where(gap[first:first + size, first:] >= j * BK - iq * BQ, p, 0.0)
                ds = (p * (dp - delta[:, at])).astype(BF)
                dv[here, :] += dot(p.astype(BF), dos[at, :])
                dk[here, :] += dot(ds, qs[at, :])
                dq[:, at] += dot(keys.T, ds)

        def block(j, masked):
            size = BK // 2 if masked else BK
            for first in range(0, BK, size):
                piece(j, masked, first, size)

        key_blocks(iq, block)
        back = (dq[...] * SCALE).T
        for h in range(NQ // HEAD):
            out[mine, h * HEAD:(h + 1) * HEAD] = turn(back[h * BQ:(h + 1) * BQ], cos[mine, :], -sin[mine, :]).astype(BF)
        store(iq, part, 0).start()

    loop(blocks, queries)

    def keys(at):
        out[at, NQ:NQ + HEAD] = turn(dk[at, :] * SCALE, cos[at, :], -sin[at, :]).astype(BF)
        out[at, NQ + HEAD:] = dv[at, :].astype(BF)
    chunked(tokens, BQ, keys)
    for i in range(blocks):
        store(i, rest, 1).start()
    end([*go, *(store(i, part, 0) for i in range(blocks)), *(store(i, rest, 1) for i in range(blocks))])


def attend_bwd(qkv, d_out, out, lse, cos, sin, others):
    tokens, NQ = out.shape
    cols = lse.shape[2]
    table, key = V(cos.shape, F32), V((tokens, HEAD), F32)
    scratch = [V(qkv.shape, BF), V(out.shape, BF), V(out.shape, BF), V(lse.shape, F32), table, table, V(qkv.shape, BF), V((cols, HEAD), BF), V((cols, HEAD), BF),
               V((HEAD, cols), F32), key, key, V((BK, BQ), jnp.int32), *(V(t.shape, BF) for t in others[:-1]), V((EARLY * TILE, others[-1].shape[1]), BF),
               DMA((tokens // BQ, 6)), DMA((len(others),))]
    return call(_attend_bwd, [qkv, d_out, out, lse, cos, sin, *others], [S(t.shape, BF) for t in (qkv, *others)], scratch, 5 * tokens * tokens * NQ, "attend_bwd")


def _front(x_ref, dy_ref, wq_ref, wk_ref, wv_ref, wo_ref, wd_ref, c_ref, s_ref, a_all, qkv_ref, dy_all, dhid, o_ref, lse_ref, cos_ref, sin_ref, h_ref, b_ref, wt_ref, ot_ref,
           tile, small, qkv, o, ot, lse, qs, top, mix, gap, wo, dt, stg, p, s, acc, tr, fr, ss, rs, sb, so, sl, *, n):
    T, D = x_ref.shape
    NQ, NK = wq_ref.shape[1], wk_ref.shape[1]
    turned, Q = NQ + NK, T // 4

    def links(an=None):
        ring = Ring(n)
        of_a, of_dy, of_o = (Links(ss, rs, k * COPIES) for k in range(3))
        if an is not None:
            gather_copies(of_a, ring, an, a_all, T)
        gather_copies(of_dy, ring, dy_ref, dy_all, T)
        return ring, of_a, of_dy, of_o

    pairs = ((x_ref, stg.at[0]), (dy_ref, stg.at[1]), (c_ref, small.at[0]), (s_ref, small.at[1]), (wo_ref, wo),
             (x_ref, stg.at[0]), (qkv, qkv_ref), (o, o_ref), (ot, ot_ref), (lse, lse_ref))
    copies = [pltpu.make_async_copy(a, b, sl.at[k]) for k, (a, b) in enumerate(pairs)]
    x_in, dy_in, c_in, s_in, wo_in, x_again, *outs = copies
    x_in.start()

    def products(an, w, cos, sin, wt):
        tables = [pltpu.make_async_copy(a, b, so.at[0, k]) for k, (a, b) in enumerate(((cos, cos_ref), (sin, sin_ref)))]
        ring, of_a, of_dy, _ = links(an)
        keep, keep_dy = (pltpu.make_async_copy(a, b.at[ring.me], so.at[1, k]) for k, (a, b) in enumerate(((an, a_all), (stg.at[1], dy_all))))
        place = [upto(NQ), pl.ds(NQ, NK), pl.ds(turned, NK)]
        loads = [dy_in, c_in, s_in, wo_in] + [pltpu.make_async_copy(r, w.at[:, c], sb.at[0, k]) for k, (r, c) in enumerate(zip((wq_ref, wk_ref, wv_ref), place))]
        begin(loads)
        ring.barrier()
        x_in.wait()
        for q, k in ((0, RA), (2, LA), (1, RB), (3, LB)):

            def norm(at):
                at = pl.ds(q * Q + at.start, at.size)
                wide = stg[0, at, :].astype(F32)
                an[at, :] = (wide * norm_scale(wide)).astype(BF)
            chunked(Q, 16, norm)
            of_a.start(k)
        of_a.start(MA)
        keep.start()
        end(loads)
        keep_dy.start()

        def table(at):
            row = pl.ds(HEAD + lax.div(at.start, HEAD), 1)
            c0, s0, c1, s1 = small[0, row, :], small[1, row, :], small[0, :HEAD, :], small[1, :HEAD, :]
            cos[at, :] = c0 * c1 - s0 * s1
            sin[at, :] = s0 * c1 + c0 * s1
        chunked(n * T, HEAD, table)
        begin(tables)
        end([keep, keep_dy])

        def work(u, units, x):
            r = dot(x[...], w[...]).astype(BF)
            for k in BOTH:
                rows = slice(k * T // 2, (k + 1) * T // 2)
                place = rows_of_unit(u, units, k, T // 2)
                c, s = cos[place, :], sin[place, :]
                for a in range(0, turned, HEAD):
                    qkv[place, a:a + HEAD] = turn(r[rows, a:a + HEAD].astype(F32), c, s).astype(BF)
                qkv[place, turned:] = r[rows, turned:]

        def turned_round(j):
            slot = lax.rem(j, 2)
            put = lambda j: pltpu.make_async_copy(wt.at[slot], wt_ref.at[:, block_rows(j, TILE)], so.at[1, slot])
            pl.when(j > 1)(lambda: put(j - 2).wait())
            wt[slot] = w[block_rows(j, TILE), :].T
            put(j).start()

        def near():
            of_a.passed_on(RA, LA)
            loop(D // TILE, turned_round)
            of_a.passed_on(RB, LB)
            of_a.start(RE, LE, MB, MC)
            of_dy.start(RA, LA, RB, LB, MA)

        stream(ring, of_a, a_all, tile, sb, None, None, None, work, gather_events(of_a, near))
        end([*tables, *[pltpu.make_async_copy(wt.at[k], wt_ref.at[:, upto(TILE)], so.at[1, k]) for k in BOTH]])

    pl.run_scoped(products, V((T, D), BF), V((D, turned + NK), BF), *[V((n * T, HEAD), F32)] * 2, V((2, turned + NK, TILE), BF))
    outs[0].start()
    set_gap(gap)

    def rest(wd):
        ring, _, of_dy, of_o = links()
        wd_in = pltpu.make_async_copy(wd_ref, wd, so.at[0, 0])
        wd_in.start()
        blocks = n * T // BQ

        def attention(iq):
            attend_block(iq, qkv, o, ot, lse, qs, top, mix, gap)
            steps(iq, {blocks - 2: lambda: of_dy.passed_on(RA, LA)})

        loop(blocks, attention)
        begin(outs[1:])
        of_dy.passed_on(RB, LB)
        of_dy.start(RE, LE, MB, MC)

        def product(shard, rows, then):
            at = pl.ds(pl.multiple_of(shard * T + rows.start, T // 2), rows.size)
            chunked(D, D // RUNS, lambda c: then(c, dot(o[at, :], wo[:, c])))

        scatter = Scatter(ring, of_o, product, stg, p, s, acc, tr, fr)
        scatter.send()
        x_again.start()
        wd_in.wait()

        def work(u, units, x, o):
            def run(c):
                o[:, c] = dot(x[...], wd[c, :], NT).astype(BF)
            chunked(wd.shape[0], TILE, run)

        stream(ring, of_dy, dy_all, tile, sb, dhid, dt, so, work, gather_events(of_dy))
        scatter.pass_on()
        x_again.wait()

        def last(at, total):
            h = (stg[0, at, :].astype(F32) + total).astype(BF)
            s[0, at, :] = h
            h = h.astype(F32)
            stg[1, at, :] = (h * norm_scale(h)).astype(BF)

        scatter.finish(last, lambda k, at: [pltpu.make_async_copy(a.at[at], b.at[at], so.at[k, m]) for m, (a, b) in enumerate(((s.at[0], h_ref), (stg.at[1], b_ref)))])
        end(outs)
        of_o.sent(R2, L2, R3, L3)

    pl.run_scoped(rest, V(wd_ref.shape, BF))


def front(x, dy, wq, wk, wv, wo, wd, n, cid):
    T, D = x.shape
    NQ, F, tokens = wo.shape[0], wd.shape[0], n * T
    N, cols = NQ + 2 * HEAD, NQ // HEAD * BQ
    stat = (tokens // BQ, 1, cols)
    table, row = S((tokens, HEAD), F32), S((T, D), BF)
    small = angles(jnp.concatenate([jnp.arange(HEAD), jnp.arange(0, tokens, HEAD)]))
    outs = [S((n, T, D), BF), S((tokens, N), BF), S((n, T, D), BF), S((n, T, F), BF), S((tokens, NQ), BF), S(stat, F32), table, table, row, row, S((N, D), BF), S((NQ, tokens), BF)]
    scratch = [V((2, T, D), BF), V((2, *small[0].shape), F32), V((tokens, N), BF), V((tokens, NQ), BF), V((NQ, tokens), BF),
               V(stat, F32), V((cols, HEAD), BF), V((1, cols), F32), V((HEAD + 8, cols), F32), V((BK, BQ), jnp.int32), V((NQ, D), BF), V((2, T, F), BF),
               *scatter_scratch(T, D), DMA((3 * COPIES,)), DMA((3 * COPIES,)), DMA((2, 3)), DMA((2, 3)), DMA((15,))]
    return call(functools.partial(_front, n=n), [x, dy, wq, wk, wv, wo, wd, *small], outs, scratch, 2 * tokens * D * (N + F + NQ), "front", cid)


def _back(t_ref, x_ref, wt_ref, a_ref, dh_all, heads_ref, b_ref, du_ref, dx_ref, by_q, by_k, by_v, by_o, by_up,
          w, t, heads, du, out, ft, stg, p, s, acc, tr, fr, ss, rs, sl, sf, sg, *, n):
    ring, links = Ring(n), Links(ss, rs)
    T, D = x_ref.shape
    NQ, NK = by_q.shape[1], by_k.shape[1]
    columns = [upto(NQ), pl.ds(NQ, NK), pl.ds(NQ + NK, NK)]
    pairs = ((t_ref, t), (wt_ref, w), (du_ref, du), (heads_ref, heads), (x_ref, stg.at[0]), (dh_all.at[ring.me], stg.at[1]))
    *first, du_in, heads_in, x_in, dh_in = [pltpu.make_async_copy(a, b, sl.at[k]) for k, (a, b) in enumerate(pairs)]
    begin(first)
    ring.barrier()
    end(first)
    begin([du_in, heads_in])
    late = lambda j: [(upto(du.shape[2]), by_up.at[block_rows(j - EARLY, TILE)])]
    fill = Fill((([b_ref], du, out, None, [late], EARLY, D // TILE),
                 ([a_ref], t, out, None, [lambda j: [(c, r.at[block_rows(j, TILE)]) for c, r in zip(columns, (by_q, by_k, by_v))]]),
                 ([dh_all], heads, out, NN, [lambda j: [(upto(TILE), by_o.at[:, block_rows(j, TILE)])]])), ft, sf, sg)
    fill.fetch(0)

    def product(shard, rows, then):
        chunked(D, D // RUNS, lambda c: then(c, dot(t[shard, rows, :], w[:, c])))

    scatter = Scatter(ring, links, product, stg, p, s, acc, tr, fr)
    scatter.send()
    begin([x_in, dh_in])
    end([du_in, heads_in])
    def beside(k):
        fill.step(k)
        steps(k, {1: scatter.pass_on})
    loop(fill.steps, beside)
    end([x_in, dh_in])

    def last(at, total):
        s[0, at, :] = (stg[1, at, :].astype(F32) + unnorm(stg[0, at, :].astype(F32), total)).astype(BF)

    scatter.finish(last, lambda k, at: [pltpu.make_async_copy(s.at[0, at], dx_ref.at[at], sg.at[k, 0])])
    links.sent(R2, L2, R3, L3)


def back(dqkv, x, wt, ws, a, dh_all, heads, b, du, n, cid):
    T, D = x.shape
    K, NQ, F = dqkv.shape[2], heads.shape[0], du.shape[2]
    scratch = [V((K, D), BF), V(dqkv.shape, BF), V(heads.shape, BF), V(du.shape, BF), V((2, TILE, F), BF), V((2, n, T, TILE), BF), *scatter_scratch(T, D),
               DMA((COPIES,)), DMA((COPIES,)), DMA((8,)), DMA((2,)), DMA((2, 3))]
    outs = [S((T, D), BF), *(S(w.shape, BF) for w in ws), S((NQ, D), BF), S((D - EARLY * TILE, F), BF)]
    return call(functools.partial(_back, n=n), [dqkv, x, wt, a, dh_all, heads, b, du], outs, scratch, 6 * n * T * D * K, "back", cid)


def _land(*refs):
    m = (len(refs) - 2) // 3
    ins, outs, tiles, sem = refs[:m], refs[m + 1:2 * m + 1], refs[2 * m + 1:-1], refs[-1]
    outs = [*outs[:-1], outs[-1].at[pl.ds(EARLY * TILE, ins[-1].shape[0])]]
    come = [pltpu.make_async_copy(a, b, sem.at[k]) for k, (a, b) in enumerate(zip(ins, tiles))]
    go = [pltpu.make_async_copy(a, b, sem.at[k]) for k, (a, b) in enumerate(zip(tiles, outs))]
    begin(come)
    for a, b in zip(come, go):
        a.wait()
        b.start()
    end(go)


def land(arrays, whole):
    shapes = [S(t.shape, BF) for t in (*arrays[:-1], whole)]
    return call(_land, [*arrays, whole], shapes, [*(V(t.shape, BF) for t in arrays), DMA((len(arrays),))], 0, "land", aliases={len(arrays): len(arrays) - 1})


def mlp_links(b_ref, bg, frm, stg, s3, s1, p1, p3, tr, fr, ss, rs, n):
    ring, links = Ring(n), Links(ss, rs)
    T = b_ref.shape[0]
    H, Q = T // 2, T // 4
    first = upto(Q)
    frp, frn = fr.at[0], fr.at[1]
    nx, pv, mt = ring.next, ring.prev, ring.mate
    lo, hi = upto(H), pl.ds(H, H)
    gather_copies(links, ring, b_ref, bg, T, True)
    at = lambda ref: [ref.at[k] for k in range(ref.shape[0])]
    pa, pb, pc, pd, sa, sb1, sc, sd1, even, odd, on, off = [*at(p1), *at(s1), *at(stg), *at(tr)]
    for k, src, dst, to in ((M5, odd, frm, mt), (M0, odd.at[hi], pa, mt), (M1, even, p3, mt), (M2, even.at[hi], pb, mt), (M3, odd.at[hi], pc, mt), (M4, even.at[hi], pd, mt),
                            (R1, s3.at[lo], on, nx), (L1, s3.at[hi], off, pv),
                            (L2, sa.at[first], frn.at[first], pv), (L5, sb1.at[first], frn.at[pl.ds(Q, Q)], pv),
                            (R2, sa.at[pl.ds(Q, Q)], frp.at[pl.ds(H, Q)], nx), (R5, sb1.at[pl.ds(Q, Q)], frp.at[pl.ds(H + Q, Q)], nx),
                            (R3, sc.at[first], frp.at[first], nx), (R4, sd1.at[first], frp.at[pl.ds(Q, Q)], nx),
                            (L3, sc.at[pl.ds(Q, Q)], frn.at[pl.ds(H, Q)], pv), (L4, sd1.at[pl.ds(Q, Q)], frn.at[pl.ds(H + Q, Q)], pv)):
        links.put(k, src, dst, to)
    return ring, links


def pair_sum(acc, p1, s1, tr, k, base=0, first=None):
    H = s1.shape[1]

    def add(at, *further):
        v = acc[pl.ds(base + at.start, at.size), :] + p1[k, at, :].astype(F32)
        s1[k, at, :] = sum([tr[t].astype(F32) for t in further], v).astype(BF)

    if first is None:
        chunked(H, 16, add)
    else:
        for side in BOTH:
            chunked(H // 2, 16, lambda at: add(pl.ds(side * (H // 2) + at.start, at.size), (side, pl.ds(first + at.start, at.size))))


def _units(b_ref, dhid_ref, wg_ref, wu_ref, bg, hid, dgo, duo, own, frm, bt, acc, stg, s3, s1, p1, p3, tr, fr, ss, rs, sw, sb, sd, so, sl, n, wg, wu, dht, st):
    ring, links = mlp_links(b_ref, bg, frm, stg, s3, s1, p1, p3, tr, fr, ss, rs, n)
    T, D = b_ref.shape
    F = wg_ref.shape[1]
    H, NC, NB = T // 2, F // 3, D // 4
    me, nx, pv, mt = ring.me, ring.next, ring.prev, ring.mate
    Q0, Q1, Q2, Q3 = range(4)
    quarters = lambda *shards: tuple((shard, q) for shard in shards for q in range(4))
    pvm, nxm = ring.prevm, ring.nextm
    units = [quarters(me), ((pv, Q0), (nx, Q2), (pvm, Q0), (nxm, Q2)), ((pv, Q1), (nx, Q3), (pvm, Q1), (nxm, Q3)), quarters(ring.opp), quarters(ring.oppm),
             ((nx, Q0), (pv, Q2), (nxm, Q0), (pvm, Q2)), ((nx, Q1), (pv, Q3), (nxm, Q1), (pvm, Q3)), quarters(mt)]
    count = len(units)

    def fetch(u, slot):
        return moves(u, units, bg, bt.at[slot], sb.at[slot]) + moves(u, units, dhid_ref, dht.at[slot], sd.at[slot])

    def store(u):
        return [c for m, ref in enumerate((hid, dgo, duo)) for c in moves(u, units, ref, st.at[m], so.at[m], True)]

    def weights(j):
        s = block_rows(j, NC)
        return [pltpu.make_async_copy(a.at[:, s], b.at[:, s], sw.at[k, j]) for k, (a, b) in enumerate(((wg_ref, wg), (wu_ref, wu)))]

    pairs = ((b_ref, bt.at[0]), (dhid_ref.at[me], dht.at[0]), (bt.at[0], bg.at[me]), (acc, own))
    *first, keep, own_out = [pltpu.make_async_copy(a, b, sl.at[k]) for k, (a, b) in enumerate(pairs)]
    begin(first)
    for j in range(F // NC):
        begin(weights(j))
    ring.barrier()
    links.start(RA, LA, RB, LB, MA)
    end(first)
    keep.start()

    pair = functools.partial(pair_sum, acc, p1, s1, tr)

    def late0():
        links.passed_on(RA, LA)
        links.start(MB, MC)

    def post0():
        keep.wait()
        own_out.start()
        links.got(MB, MC)
        begin(fetch(1, 1))

    def mid1():
        own_out.wait()
        links.passed_on(RB)
        links.start(RE)
        links.passed_on(LB)
        links.start(LE, MH, MI)

    def late1():
        links.got(MH, MI)
        begin(fetch(2, 0))

    def mid2():
        links.got(M0)
        pair(0)
        links.start(L2, R2)

    def post2():
        links.start(M2)
        far()
        begin(fetch(3, 1))

    def mid3():
        links.got(M2)
        pair(1)
        links.start(L5, R5)

    def late3():
        links.got(MD, ME)
        begin(fetch(4, 0))
        links.sent(M2)

    def late4():
        links.got(MF, MG)
        begin(fetch(5, 1))

    def mid5():
        links.got(M1)

        def add(at):
            s3[at, :] = (acc[at, :] + p3[at, :].astype(F32)).astype(BF)
        chunked(T, 16, add)
        links.start(R1, L1)
        links.sent(M0)

    def late6():
        links.got(MA)
        begin(fetch(7, 1))

    def pairs_left():
        links.got(M3, R1, L1)
        pair(2, 0, 0)
        links.start(R3, L3)
        links.got(M4)
        pair(3, H, H // 2)
        links.start(R4, L4)

    def post7():
        links.start(M5)
        end(store(7))

    _, _, _, far, _, last, _ = gather_events(links)
    starting = lambda *ks: lambda: links.start(*ks)
    mids = [None, mid1, mid2, mid3, last, mid5, lambda: links.sent(M1), lambda: links.sent(M3)]
    lates = [late0, late1, None, late3, late4, lambda: begin(fetch(6, 0)), late6]
    posts = [post0, starting(M0), post2, None, starting(M1), starting(M3), starting(M4), post7]

    def forth_unit(u, slot):
        @pl.when(u > 0)
        def _():
            end(fetch(u, slot))
            end(store(u - 1))

        def forth(j):
            @pl.when(u == 0)
            def _():
                end(weights(j))
            s = block_rows(j, NC)
            x = bt[slot]
            gate, up = dot(x, wg[:, s]), dot(x, wu[:, s])
            d = dht[slot, :, s].astype(F32)
            sig = jax.nn.sigmoid(gate)
            act = gate * sig
            for m, v in enumerate((act * up, d * up * (sig + act * (1 - sig)), d * act)):
                st[m, :, s] = v.astype(BF)
            pl.when((u == count - 1) & (j == 0))(pairs_left)

        loop(F // NC, forth)
        begin(store(u))

    def unit(u):
        slot = lax.rem(u, 2)
        forth_unit(u, slot)
        steps(u, mids)
        among = lambda *us: functools.reduce(jnp.logical_or, [u == k for k in us])
        side = jnp.where(among(2, 4, 6), 0, 1)

        def back(c):
            v = dot(st[1], wg[c, :], NT) + dot(st[2], wu[c, :], NT)

            @pl.when(among(0, 3))
            def _():
                acc[:, c] = v

            @pl.when(among(4, 7))
            def _():
                stg[side, :, c] = v.astype(BF)

            @pl.when(among(1, 2, 5, 6))
            def _():
                acc[pl.ds(pl.multiple_of(jnp.where(u == 6, H, 0), H), H), c] = v[:H]
                stg[side, H:, c] = v[H:].astype(BF)

        half = D // NB // 2
        loop(half, lambda j: back(block_rows(j, NB)))
        steps(u, lates)
        loop(D // NB, lambda j: back(block_rows(j, NB)), half)
        steps(u, posts)

    loop(count, unit)


def _middle(b_ref, dhid_ref, wg_ref, wu_ref, h_ref, dy_ref, wo_ref, dy_all, bg, hid, dgo, duo, dh_all, out, by_down, by_gate, by_up, own, frm,
            bt, acc, stg, s3, s1, p1, p3, tr, fr, ot, ss, rs, sw, sb, sd, so, sl, sf, sg, *, n):
    T, D = b_ref.shape
    F, NQ = wg_ref.shape[1], wo_ref.shape[0]
    shared = (bt, acc, stg, s3, s1, p1, p3, tr, fr, ss, rs)
    pl.run_scoped(functools.partial(_units, b_ref, dhid_ref, wg_ref, wu_ref, bg, hid, dgo, duo, own, frm, *shared, sw, sb, sd, so, sl, n),
                  V((D, F), BF), V((D, F), BF), V((2, T, F), BF), V((3, T, F), BF))

    def rest(fixed, left, tile, wo):
        ring, links = mlp_links(b_ref, bg, frm, *shared[2:], n)
        of_dh = Links(ss, rs, COPIES)
        gather_copies(of_dh, ring, stg.at[0], dh_all, T)
        pairs = ((hid, fixed.at[1]), (dgo, fixed.at[0]), (duo, fixed.at[1]), (wo_ref, wo), (own, acc), (frm, bt.at[0]), (h_ref, bt.at[1]), (dy_ref, s3),
                 (stg.at[0], dh_all.at[ring.me]))
        hid_in, dg_in, du_in, wo_in, own_in, frm_in, *rows_in, keep = [pltpu.make_async_copy(a, b, sl.at[k]) for k, (a, b) in enumerate(pairs)]
        side = lambda ref: lambda j: [(upto(F), ref.at[block_rows(j, TILE)])]
        fill = Fill((([dy_all], fixed.at[1], left, TN, [lambda j: [(pl.ds(a, TILE), by_down.at[pl.ds(a, TILE), block_rows(j, TILE)]) for a in range(0, F, TILE)]]),
                     ([bg, bg], fixed, left, None, [side(by_gate), side(by_up)], 0, D // TILE + EARLY)), tile, sf, sg)
        own_in.start()
        hid_in.start()
        fill.fetch(0)
        links.sent(R1, L1)
        begin(rows_in)
        own_in.wait()
        add_rows(links, acc, (R2, R5), fr.at[0], T // 2)
        add_rows(links, acc, (L2, L5), fr.at[1], 0)
        hid_in.wait()

        def mates_part():
            links.got(M5)
            frm_in.start()

        def scattered():
            end([frm_in, *rows_in])
            links.sent(M4)

            def add(at):
                acc[at, :] += bt[0, at, :].astype(F32)
            chunked(T, 16, add)

            def last(at, total):
                stg[0, at, :] = (s3[at, :].astype(F32) + unnorm(bt[1, at, :].astype(F32), total)).astype(BF)

            finish(links, acc, fr, last, (R3, R4), (L3, L4))
            of_dh.start(RA, LA, RB, LB, MA)
            keep.start()

        def near():
            of_dh.passed_on(RB, LB)
            of_dh.start(RE, LE, MB, MC)

        def work(u, units, x, o):
            o[...] = dot(x[...], wo[...], NT).astype(BF)

        mate, _, mates, far, fars, last, lasts = gather_events(of_dh)
        events = {0: mates_part, 1: scattered, 3: lambda: begin([dg_in, wo_in]), 5: lambda: (mate(), end([keep, wo_in, dg_in]), of_dh.passed_on(RA, LA)),
                  7: du_in.start, 8: near, 10: mates, 13: far, 14: fars, 15: du_in.wait, fill.steps - 2: last, fill.steps - 1: lasts}
        schedule = (6, 7, 11, 12, 15, 16, fill.steps - 1, fill.steps)
        stream(ring, of_dh, dh_all, bt, sb, out, ot, sd, work, events, schedule, lambda k: pl.when(k < fill.steps)(lambda: fill.step(k)))
        links.sent(*GATHER, MH, MI, R2, R3, R4, R5, L2, L3, L4, L5, M5)

    pl.run_scoped(rest, V((2, n, T, F), BF), V((2, TILE, F), BF), V((2, n, T, TILE), BF), V((NQ, D), BF))


def middle(b, dhid, wg, wu, h, dy, wo, dy_all, n, cid):
    T, D = b.shape
    F, NQ = wg.shape[1], wo.shape[0]
    H = T // 2
    row, halves = V((T, D), BF), V((4, H, D), BF)
    scratch = [V((2, T, D), BF), V((T, D), F32), V((2, T, D), BF), row, halves, halves, row, V((2, H, D), BF), V((2, T, D), BF), V((2, T, NQ), BF),
               DMA((2 * COPIES,)), DMA((2 * COPIES,)), DMA((2, 3)), DMA((2, 4)), DMA((2, 4)), DMA((3, 4)), DMA((9,)), DMA((2,)), DMA((2, 3))]
    wide, full, narrow = S((n, T, F), BF), S((n, T, D), BF), S((D, F), BF)
    outs = [full, wide, wide, wide, full, S((n, T, NQ), BF), S((F, D), BF), narrow, narrow, S((T, D), F32), S((T, D), BF)]
    got = call(functools.partial(_middle, n=n), [b, dhid, wg, wu, h, dy, wo, dy_all], outs, scratch, 14 * n * T * D * F, "middle", cid)
    return got[4:9], got[0], got[3]


def solution(mesh):
    n = mesh.shape["tp"]

    def step(x, dy, wq, wk, wv, wo, wg, wu, wd):
        x, dy = x[0], dy[0]
        blocks = lambda t: t.reshape(n, -1, t.shape[1])
        a, qkv, dy_all, dhid, heads, lse, cos, sin, h, b, wt, heads_t = front(x, dy, wq, wk, wv, wo, wd, n, 0)
        (dh_all, d_heads, *by_mlp), b, du = middle(b, dhid, wg, wu, h, dy, wo, dy_all, n, 1)
        dqkv, by_down, by_gate, by_up = attend_bwd(qkv, flat(d_heads), heads, lse, cos, sin, by_mlp)
        dx, *by_qkvo, by_up = land(back(blocks(dqkv), x, wt, [wq, wk, wv], a, dh_all, heads_t, b, du, n, 2), by_up)
        return dx[None], *by_qkvo, by_gate, by_up, by_down

    states, by_columns, by_rows = P("dp", "tp", None), P(None, "tp"), P("tp", None)
    weights = (by_columns, by_columns, by_columns, by_rows, by_columns, by_columns, by_rows)
    own = tuple(P("dp", "tp") if spec == by_columns else P(("dp", "tp"), None) for spec in weights)
    return jax.shard_map(step, mesh=mesh, in_specs=(states, states, *weights), out_specs=(states, *own), check_vma=False)
```

```python
import functools

import jax
import jax.numpy as jnp
from jax import lax
from jax.experimental import pallas as pl
from jax.experimental.pallas import tpu as pltpu
from jax.sharding import PartitionSpec as P

BF, F32 = jnp.bfloat16, jnp.float32
HEAD = 128
THETA = 10000
NEG = -1e30
HIDDEN = 2 * NEG
LOG2E = 1.4426950408889634
SCALE = HEAD**-0.5
MOST = 67_000_000
BQ = BK = 512
TILE = 512
EARLY = 3
NN, NT, TN = ((((a,), (b,)), ((), ())) for a, b in ((1, 0), (1, 1), (0, 0)))
ANY = pl.BlockSpec(memory_space=pl.ANY)
S, V, DMA = jax.ShapeDtypeStruct, pltpu.VMEM, pltpu.SemaphoreType.DMA

RA, RB, RC, RD, RE, LA, LB, LC, LD, LE, MA, MB, MC, MD, ME, MF, MG = GATHER = range(17)
R1, R2, R3, R4, R5, L1, L2, L3, L4, L5, M0, M1, M2, M3, M4, M5, MH, MI = range(17, 35)
COPIES = 35
RUNS = 2
LO, HI = BOTH = range(2)


def dot(a, b, dims=NN, **kw):
    return lax.dot_general(a, b, dims, preferred_element_type=F32, **kw)


def norm_scale(wide):
    return lax.rsqrt(jnp.mean(wide * wide, -1, keepdims=True) + 1e-6)


def unnorm(wide, d):
    scale = norm_scale(wide)
    return d * scale - wide * (scale * scale * scale * jnp.mean(d * wide, -1, keepdims=True))


def turn(t, cos, sin):
    return t * cos + pltpu.roll(t, HEAD // 2, 1) * sin


def angles(places):
    half = HEAD // 2
    a = places.astype(F32)[:, None] * THETA ** (-jnp.arange(half, dtype=F32) / half)
    cos, sin = jnp.cos(a), jnp.sin(a)
    return jnp.concatenate([cos, cos], -1), jnp.concatenate([-sin, sin], -1)


class Ring:
    def __init__(self, n):
        self.me = lax.axis_index("tp")
        core, chips = lax.rem(self.me, 2), n // 2
        chip = [lax.rem(lax.div(self.me, 2) + k, chips) for k in range(chips)]
        self.next, self.opp, self.prev = [2 * c + core for c in chip[1:]]
        self.mate, self.nextm, self.oppm, self.prevm = [2 * c + 1 - core for c in chip]

    def barrier(self):
        b = pltpu.get_barrier_semaphore()
        near = (self.next, self.prev, self.mate)
        for d in near:
            pl.semaphore_signal(b, inc=1, device_id={"tp": d}, device_id_type=pl.DeviceIdType.MESH)
        pl.semaphore_wait(b, len(near))


class Links:
    def __init__(self, ss, rs, base=0):
        self.ss, self.rs, self.base, self.made = ss, rs, base, {}

    def put(self, k, src, dst, dev):
        self.made[k] = lambda: pltpu.make_async_remote_copy(src_ref=src, dst_ref=dst, send_sem=self.ss.at[self.base + k], recv_sem=self.rs.at[self.base + k],
                                                            device_id={"tp": dev}, device_id_type=pl.DeviceIdType.MESH)

    def start(self, *ks):
        for k in ks:
            self.made[k]().start()

    def got(self, *ks):
        for k in ks:
            self.made[k]().wait_recv()

    def sent(self, *ks):
        for k in ks:
            self.made[k]().wait_send()

    def passed_on(self, *ks):
        for k in ks:
            self.got(k)
            self.start(k + 2)


def flat(t):
    return t.reshape(-1, t.shape[-1])


def begin(copies):
    for c in copies:
        c.start()


def end(copies):
    for c in copies:
        c.wait()


def pick(u, values):
    out = values[0]
    for k, v in enumerate(values):
        out = jnp.where(u == k, v, out)
    return out


def steps(u, events):
    for k, f in events.items() if isinstance(events, dict) else enumerate(events):
        def run(f=f):
            f()
        if f is not None:
            pl.when(u == k)(run)


def loop(count, f, first=0):
    def body(k, _):
        f(k)
    lax.fori_loop(first, count, body, None)


def block_rows(i, size):
    return pl.ds(pl.multiple_of(i * size, size), size)


def upto(size):
    return pl.ds(0, size)


def chunked(size, width, f):
    loop(size // width, lambda j: f(block_rows(j, width)))


def gather_copies(links, ring, src, dst, T, fine=False):
    H, Q = T // 2, T // 4
    me, nx, pv, mt, opp = ring.me, ring.next, ring.prev, ring.mate, ring.opp
    for k, slot, a, rows, to in ((RA, me, 0, Q, nx), (RB, me, Q, Q, nx), (RC, pv, 0, Q, nx), (RD, pv, Q, Q, nx), (RE, me, H, H, nx),
                                 (LA, me, H, Q, pv), (LB, me, H + Q, Q, pv), (LC, nx, H, Q, pv), (LD, nx, H + Q, Q, pv), (LE, me, 0, H, pv),
                                 (MA, me, 0, T, mt), (MB, pv, 0, Q if fine else H, mt), (MC, nx, H, Q if fine else H, mt),
                                 (MH, pv, Q, Q, mt), (MI, nx, H + Q, Q, mt), (MD, opp, 0, H, mt), (ME, opp, H, H, mt), (MF, pv, H, H, mt), (MG, nx, 0, H, mt)):
        at = pl.ds(a, rows)
        links.put(k, src.at[at] if slot is me else dst.at[slot, at], dst.at[slot, at], to)


def whole(shard):
    return (shard, LO), (shard, HI)


def moves(u, units, far, near, sem, back=False):
    parts = len(units[0])
    size = near.shape[0] // parts
    out = []
    for k in range(parts):
        shard, place = (pick(u, [x[k][m] for x in units]) for m in BOTH)
        ends = far.at[shard, block_rows(place, size)], near.at[pl.ds(k * size, size)]
        out.append(pltpu.make_async_copy(*(ends[::-1] if back else ends), sem.at[k]))
    return out


def rows_of_unit(u, units, k, H):
    shard, half = (pick(u, [x[k][m] for x in units]) for m in BOTH)
    return pl.ds(pl.multiple_of((2 * shard + half) * H, H), H)


def stream(ring, links, src, tile, sin, dst, out, sout, work, events, schedule=range(8), beside=None):
    units = [whole(ring.me), whole(ring.mate), ((ring.prev, LO), (ring.next, HI)), ((ring.prevm, LO), (ring.nextm, HI)), whole(ring.opp),
             whole(ring.oppm), ((ring.prev, HI), (ring.next, LO)), ((ring.prevm, HI), (ring.nextm, LO))]
    fetch = lambda u, slot: moves(u, units, src, tile.at[slot], sin.at[slot])
    store = lambda u, slot: moves(u, units, dst, out.at[slot], sout.at[slot], True)
    latest = lambda k: sum(jnp.where(k < s, 0, 1) for s in schedule) - 1

    def fetch_for(k):
        u = latest(k)

        @pl.when(latest(k - 1) < u)
        def _():
            begin(fetch(u, lax.rem(u, 2)))

    fetch_for(0)

    def step(k):
        if beside is not None:
            beside(k)
        u = latest(k)

        @pl.when(latest(k - 1) < u)
        def _():
            slot = lax.rem(u, 2)
            end(fetch(u, slot))

            if dst is None:
                work(u, units, tile.at[slot])
            else:
                pl.when(u > 1)(lambda: end(store(u - 2, slot)))
                work(u, units, tile.at[slot], out.at[slot])
                begin(store(u, slot))

        steps(k, events)
        fetch_for(k + 1)

    loop(schedule[-1] + 1, step)
    if dst is not None:
        end(store(len(units) - 2, 0) + store(len(units) - 1, 1))
    links.sent(*GATHER)


class Fill:
    def __init__(self, jobs, tile, sin, sout):
        self.tile, self.sin, self.sout, self.jobs, at = tile, sin, sout, [], 0
        for srcs, fixed, out, right, ends, *tiles in jobs:
            per = srcs[0].shape[2] // TILE
            first, last = tiles or (0, per * len(srcs))
            self.jobs.append((at, last - first, first, per, srcs, fixed, out, right, ends))
            at += last - first
        self.steps = at

    def load(self, src, j, slot):
        return pltpu.make_async_copy(src.at[:, :, block_rows(j, TILE)], self.tile.at[slot], self.sin.at[slot])

    def fetch(self, k):
        for at, count, first, per, srcs, *_ in self.jobs:
            i = k - at + first
            for m, src in enumerate(srcs):
                mine = (k >= at) & (k < at + count) & (lax.div(i, per) == m)
                pl.when(mine)(lambda: begin([self.load(src, i - m * per, lax.rem(k, 2))]))

    def step(self, k):
        slot = lax.rem(k, 2)
        end([self.load(self.jobs[0][4][0], 0, slot)])
        self.fetch(k + 1)
        before = None
        for at, count, first, per, srcs, fixed, out, right, ends in self.jobs:
            def store(m, j, slot, out=out, ends=ends):
                return [pltpu.make_async_copy(out.at[slot, :, a], b, self.sout.at[slot, i]) for i, (a, b) in enumerate(ends[m](j))]

            @pl.when((k >= at) & (k < at + count))
            def _():
                which, j = lax.div(k - at + first, per), lax.rem(k - at + first, per)
                pl.when(k > at + 1)(lambda: end(store(0, j, slot)))
                if before is not None:
                    pl.when(k <= at + 1)(lambda: end(before(0, EARLY, slot)))
                t = self.tile[slot].reshape(-1, TILE)
                f = flat(fixed[which] if len(srcs) > 1 else fixed[...])
                r = dot(f, t, right) if right else dot(t, f, TN)
                for a in range(0, r.shape[0], TILE):
                    out[slot, :, (a if right else 0):(a if right else 0) + r.shape[1]] = r[a:a + TILE].astype(BF)
                for m in range(len(srcs)):
                    pl.when(which == m)(lambda: begin(store(m, j, slot)))
            before = store
        self.finish = lambda: end([c for slot in BOTH for c in before(0, EARLY, slot)])


def gather_events(links, near=None):
    def far():
        links.got(RC, RD)
        links.start(MD)
        links.got(LC, LD)
        links.start(ME)

    def last():
        links.got(RE)
        links.start(MF)
        links.got(LE)
        links.start(MG)

    got = lambda *ks: lambda: links.got(*ks)
    return [got(MA), near, got(MB, MC), far, got(MD, ME), last, got(MF, MG)]


def add_rows(links, acc, ms, fr, half):
    def add(at):
        at = pl.ds(half + at.start, at.size)
        acc[at, :] += fr[at, :].astype(F32)
    links.got(*ms)
    chunked(acc.shape[0] // 2, 16, add)


def finish(links, acc, fr, last, out=None):
    Q = acc.shape[0] // 4
    quarters = [(k, pl.ds(k * Q, Q)) for k in (0, 2, 1, 3)]
    for m, (k, rows) in zip((R3, L3, R4, L4), quarters):
        def total(at):
            at = pl.ds(k * Q + at.start, at.size)
            last(at, acc[at, :] + fr[k // 2, at, :].astype(F32))
        links.got(m)
        chunked(Q, 16, total)
        if out is not None:
            begin(out(k, rows))
    if out is not None:
        end([c for k, rows in quarters for c in out(k, rows)])


class Scatter:
    def __init__(self, ring, links, product, stg, p, s, acc, tr, fr):
        self.ring, self.links, self.product, self.stg, self.p, self.s, self.acc, self.tr, self.fr = ring, links, product, stg, p, s, acc, tr, fr
        T = acc.shape[0]
        H = T // 2
        nx, pv, mt = ring.next, ring.prev, ring.mate
        self.every, self.lo, self.hi = every, lo, hi = upto(T), upto(H), pl.ds(H, H)
        quarters = [pl.ds(a, H // 2) for a in range(0, T, H // 2)]
        at = lambda ref: [ref.at[k] for k in range(ref.shape[0])]
        even, odd, pa, pb, pc, pd, so, sn, sp, on, off, fp, fn = [*at(stg), *at(p), *at(s), *at(tr), *at(fr)]
        NB = acc.shape[1] // RUNS
        for j, k in enumerate((M0, M5)):
            links.put(k, even.at[:, pl.ds(j * NB, NB)], pa.at[:, pl.ds(j * NB, NB)], mt)
        for k, src, dst, to in ((M2, odd, pb, mt), (M3, even, pc, mt), (M4, odd, pd, mt),
                                (R1, so.at[lo], on, nx), (L1, so.at[hi], off, pv), (R2, sn.at[hi], fp.at[hi], nx), (L2, sp.at[lo], fn.at[lo], pv),
                                *((k, sn.at[at], fp.at[at], nx) for k, at in zip((R3, R4), quarters)), *((k, sp.at[at], fn.at[at], pv) for k, at in zip((L3, L4), quarters[2:]))):
            links.put(k, src, dst, to)

    def send(self):
        links, ring, stg, p, s, acc = self.links, self.ring, self.stg, self.p, self.s, self.acc
        runs = (M0, M5)
        shards = (ring.oppm, ring.opp, ring.nextm, ring.prevm, ring.next, ring.prev, ring.mate, ring.me)
        got, sent, start = ((lambda f: lambda *ks: lambda: f(*ks))(f) for f in (links.got, links.sent, links.start))
        before = [None, None, None, sent(*runs), got(M2), got(M3), sent(M2)]
        after = [None, start(R1, L1), start(M2), start(M3), start(R2), start(L2), start(M4)]

        def step(i):
            steps(i, before)

            def then(c, v):
                j = lax.div(c.start, c.size)

                def to_mate(k, on=()):
                    def f():
                        stg[k, :, c] = v.astype(BF)
                        steps(j, on)
                    return f

                def to_chip(k, rows, wait=()):
                    def f():
                        steps(j, wait)
                        s[k, rows, c] = (v[rows.start:rows.start + rows.size] + p[k, rows, c].astype(F32)).astype(BF)
                    return f

                def keep():
                    acc[:, c] = v

                steps(i, [to_mate(0, [start(k) for k in runs]), to_chip(0, self.every, [got(k) for k in runs]), to_mate(1), to_mate(0), to_chip(1, self.hi),
                          to_chip(2, self.lo), to_mate(1), keep])

            self.product(pick(i, shards), self.every, then)
            steps(i, after)

        loop(len(shards), step)

    def pass_on(self):
        H = self.lo.size

        def step(i):
            rows = block_rows(i, H)
            steps(i, [lambda: self.links.got(R1), lambda: self.links.got(L1)])

            def then(c, v):
                self.s[1 + i, rows, c] = (v + self.p[1 + i, rows, c].astype(F32) + self.tr[i, :, c].astype(F32)).astype(BF)
            self.product(pick(i, (self.ring.next, self.ring.prev)), rows, then)
            steps(i, [lambda: self.links.start(R3, R4), lambda: self.links.start(L3, L4)])

        loop(2, step)

    def finish(self, last, out):
        self.links.sent(R1, L1)
        p = self.p.at[3]
        for ms, fr, half in (([M4], p, self.hi), ([], p, self.lo), ([R2], self.fr.at[LO], self.hi), ([L2], self.fr.at[HI], self.lo)):
            add_rows(self.links, self.acc, ms, fr, half.start)
        finish(self.links, self.acc, self.fr, last, out)


def scatter_scratch(T, D):
    return [V((2, T, D), BF), V((4, T, D), BF), V((3, T, D), BF), V((T, D), F32), V((2, T // 2, D), BF), V((2, T, D), BF)]


def call(body, args, outs, scratch, flops, name, cid=None, aliases=()):
    return pl.pallas_call(
        body, in_specs=[ANY] * len(args), out_specs=[ANY] * len(outs), out_shape=outs, scratch_shapes=scratch, name=name, input_output_aliases=dict(aliases),
        compiler_params=pltpu.CompilerParams(collective_id=cid, has_side_effects=True, vmem_limit_bytes=MOST),
        cost_estimate=pl.CostEstimate(flops=flops, bytes_accessed=sum(t.size for t in (*args, *outs)), transcendentals=0),
    )(*args)


def rows_of(t):
    return jnp.concatenate([t[:, a:a + HEAD] for a in range(0, t.shape[1], HEAD)], axis=0)


def set_gap(gap):
    gap[...] = lax.broadcasted_iota(jnp.int32, gap.shape, 1) - lax.broadcasted_iota(jnp.int32, gap.shape, 0)


def key_blocks(iq, block):
    seen = lax.div(iq * BQ + 1, BK)
    loop(seen, lambda j: block(j, False))
    loop(lax.div((iq + 1) * BQ + BK - 1, BK), lambda j: block(j, True), seen)


def attend_block(iq, qkv, o_ref, ot_ref, lse_ref, qs, top, mix, gap):
    NQ = o_ref.shape[1]
    cols = qs.shape[0]
    mine = block_rows(iq, BQ)
    qs[...] = rows_of(qkv[mine, :NQ])
    top[...] = jnp.full_like(top, NEG)
    mix[...] = jnp.zeros_like(mix)
    ones = jnp.ones((8, BK), BF)
    strips = [slice(a, a + BQ) for a in range(0, cols, BQ)]

    def block(j, masked):
        here = block_rows(j, BK)
        keys = qkv[here, NQ:NQ + HEAD]
        values = jnp.concatenate([qkv[here, NQ + HEAD:].T, ones], axis=0)
        scores = [dot(keys, qs[at, :], NT) for at in strips]
        ps, keeps = [], []
        for at, s in zip(strips, scores):
            if masked:
                s = jnp.where(gap[...] >= j * BK - iq * BQ, s, HIDDEN)
            old = top[:, at]
            new = jnp.maximum(old, s.max(axis=0, keepdims=True))
            top[:, at] = new
            ps.append(jnp.exp2((s - new) * (SCALE * LOG2E)).astype(BF))
            keeps.append(jnp.exp2((old - new) * (SCALE * LOG2E)))
        for at, p, keep in zip(strips, ps, keeps):
            mix[:, at] = mix[:, at] * keep + dot(values, p)

    key_blocks(iq, block)
    total = mix[HEAD:HEAD + 1, :]
    out = mix[:HEAD, :] * (1 / total)
    for h in range(NQ // HEAD):
        part = out[:, h * BQ:(h + 1) * BQ]
        ot_ref[h * HEAD:(h + 1) * HEAD, mine] = part.astype(BF)
        o_ref[mine, h * HEAD:(h + 1) * HEAD] = part.T.astype(BF)
    lse_ref[iq] = top[...] * SCALE + jnp.log(total)


def _attend_bwd(qkv_ref, do_ref, o_ref, lse_ref, cos_ref, sin_ref, *refs):
    ins, (out_ref, *outs), (qkv, do, o, lse, cos, sin, out, qs, dos, dq, dk, dv, gap, *tiles, sem, sl) = refs[:3], refs[3:7], refs[7:]
    NQ = do.shape[1]
    tokens, cols = dk.shape[0], qs.shape[0]
    blocks = tokens // BQ
    ins, outs = ([*x[:-1], x[-1].at[upto(EARLY * TILE)]] for x in (ins, outs))
    come, go = [[pltpu.make_async_copy(x, y, sl.at[k]) for k, (x, y) in enumerate(zip(*ends))] for ends in ((ins, tiles), (tiles, outs))]

    def loads(i):
        at = block_rows(i, BQ)
        pairs = [(x.at[at], y.at[at]) for x, y in ((qkv_ref, qkv), (do_ref, do), (o_ref, o), (cos_ref, cos), (sin_ref, sin))]
        return [pltpu.make_async_copy(x, y, sem.at[i, k]) for k, (x, y) in enumerate([*pairs, (lse_ref.at[i], lse.at[i])])]

    def store(i, columns, k):
        at = block_rows(i, BQ), columns
        return pltpu.make_async_copy(out.at[at], out_ref.at[at], sem.at[i, k])

    part, rest = upto(NQ), pl.ds(NQ, 2 * HEAD)
    for i in range(blocks):
        begin(loads(i))
    begin(come)
    set_gap(gap)
    dk[...] = jnp.zeros_like(dk)
    dv[...] = jnp.zeros_like(dv)

    def landed(*ks):
        def f():
            for k in ks:
                come[k].wait()
                go[k].start()
        return f

    def queries(iq):
        end(loads(iq))
        steps(iq, {blocks - 2: landed(0), blocks - 1: landed(*range(1, len(come)))})
        mine = block_rows(iq, BQ)
        qs[...] = rows_of(qkv[mine, :NQ])
        dos[...] = rows_of(do[mine, :])
        dq[...] = jnp.zeros_like(dq)
        delta = (dos[...].astype(F32) * rows_of(o[mine, :]).astype(F32)).T.sum(axis=0, keepdims=True)
        lses = lse[iq] * LOG2E

        def piece(j, masked, first, size):
            here = pl.ds(pl.multiple_of(j * BK + first, size), size)
            keys, values = qkv[here, NQ:NQ + HEAD], qkv[here, NQ + HEAD:]
            strips = [slice(a + (first if masked else 0), a + BQ) for a in range(0, cols, BQ)]
            scores = [dot(keys, qs[at, :], NT) for at in strips]
            dps = [dot(values, dos[at, :], NT) for at in strips]
            for at, s, dp in zip(strips, scores, dps):
                p = jnp.exp2(s * (SCALE * LOG2E) - lses[:, at])
                if masked:
                    p = jnp.where(gap[first:first + size, first:] >= j * BK - iq * BQ, p, 0.0)
                ds = (p * (dp - delta[:, at])).astype(BF)
                dv[here, :] += dot(p.astype(BF), dos[at, :])
                dk[here, :] += dot(ds, qs[at, :])
                dq[:, at] += dot(keys.T, ds)

        def block(j, masked):
            size = BK // 2 if masked else BK
            for first in range(0, BK, size):
                piece(j, masked, first, size)

        key_blocks(iq, block)
        back = (dq[...] * SCALE).T
        for h in range(NQ // HEAD):
            out[mine, h * HEAD:(h + 1) * HEAD] = turn(back[h * BQ:(h + 1) * BQ], cos[mine, :], -sin[mine, :]).astype(BF)
        store(iq, part, 0).start()

    loop(blocks, queries)

    def keys(at):
        out[at, NQ:NQ + HEAD] = turn(dk[at, :] * SCALE, cos[at, :], -sin[at, :]).astype(BF)
        out[at, NQ + HEAD:] = dv[at, :].astype(BF)
    chunked(tokens, BQ, keys)
    for i in range(blocks):
        store(i, rest, 1).start()
    end([*go, *(store(i, part, 0) for i in range(blocks)), *(store(i, rest, 1) for i in range(blocks))])


def attend_bwd(qkv, d_out, out, lse, cos, sin, others):
    tokens, NQ = out.shape
    cols = lse.shape[2]
    table, key = V(cos.shape, F32), V((tokens, HEAD), F32)
    scratch = [V(qkv.shape, BF), V(out.shape, BF), V(out.shape, BF), V(lse.shape, F32), table, table, V(qkv.shape, BF), V((cols, HEAD), BF), V((cols, HEAD), BF),
               V((HEAD, cols), F32), key, key, V((BK, BQ), jnp.int32), *(V(t.shape, BF) for t in others[:-1]), V((EARLY * TILE, others[-1].shape[1]), BF),
               DMA((tokens // BQ, 6)), DMA((len(others),))]
    return call(_attend_bwd, [qkv, d_out, out, lse, cos, sin, *others], [S(t.shape, BF) for t in (qkv, *others)], scratch, 5 * tokens * tokens * NQ, "attend_bwd")


def _front(x_ref, dy_ref, wq_ref, wk_ref, wv_ref, wo_ref, wd_ref, c_ref, s_ref, a_all, qkv_ref, dy_all, dhid, o_ref, lse_ref, cos_ref, sin_ref, h_ref, b_ref, wt_ref, ot_ref,
           tile, small, qkv, o, ot, lse, qs, top, mix, gap, wo, dt, stg, p, s, acc, tr, fr, ss, rs, sb, so, sl, *, n):
    T, D = x_ref.shape
    NQ, NK = wq_ref.shape[1], wk_ref.shape[1]
    turned, Q = NQ + NK, T // 4

    def links(an=None):
        ring = Ring(n)
        of_a, of_dy, of_o = (Links(ss, rs, k * COPIES) for k in range(3))
        if an is not None:
            gather_copies(of_a, ring, an, a_all, T)
        gather_copies(of_dy, ring, dy_ref, dy_all, T)
        return ring, of_a, of_dy, of_o

    pairs = ((x_ref, stg.at[0]), (dy_ref, stg.at[1]), (c_ref, small.at[0]), (s_ref, small.at[1]), (wo_ref, wo),
             (x_ref, stg.at[0]), (qkv, qkv_ref), (o, o_ref), (ot, ot_ref), (lse, lse_ref))
    copies = [pltpu.make_async_copy(a, b, sl.at[k]) for k, (a, b) in enumerate(pairs)]
    x_in, dy_in, c_in, s_in, wo_in, x_again, *outs = copies
    x_in.start()

    def products(an, w, cos, sin, wt):
        tables = [pltpu.make_async_copy(a, b, so.at[0, k]) for k, (a, b) in enumerate(((cos, cos_ref), (sin, sin_ref)))]
        ring, of_a, of_dy, _ = links(an)
        keep, keep_dy = (pltpu.make_async_copy(a, b.at[ring.me], so.at[1, k]) for k, (a, b) in enumerate(((an, a_all), (stg.at[1], dy_all))))
        place = [upto(NQ), pl.ds(NQ, NK), pl.ds(turned, NK)]
        loads = [dy_in, c_in, s_in, wo_in] + [pltpu.make_async_copy(r, w.at[:, c], sb.at[0, k]) for k, (r, c) in enumerate(zip((wq_ref, wk_ref, wv_ref), place))]
        begin(loads)
        ring.barrier()
        x_in.wait()
        for q, k in ((0, RA), (2, LA), (1, RB), (3, LB)):

            def norm(at):
                at = pl.ds(q * Q + at.start, at.size)
                wide = stg[0, at, :].astype(F32)
                an[at, :] = (wide * norm_scale(wide)).astype(BF)
            chunked(Q, 16, norm)
            of_a.start(k)
        of_a.start(MA)
        keep.start()
        end(loads)
        keep_dy.start()

        def table(at):
            row = pl.ds(HEAD + lax.div(at.start, HEAD), 1)
            c0, s0, c1, s1 = small[0, row, :], small[1, row, :], small[0, :HEAD, :], small[1, :HEAD, :]
            cos[at, :] = c0 * c1 - s0 * s1
            sin[at, :] = s0 * c1 + c0 * s1
        chunked(n * T, HEAD, table)
        begin(tables)
        end([keep, keep_dy])

        def work(u, units, x):
            r = dot(x[...], w[...]).astype(BF)
            for k in BOTH:
                rows = slice(k * T // 2, (k + 1) * T // 2)
                place = rows_of_unit(u, units, k, T // 2)
                c, s = cos[place, :], sin[place, :]
                for a in range(0, turned, HEAD):
                    qkv[place, a:a + HEAD] = turn(r[rows, a:a + HEAD].astype(F32), c, s).astype(BF)
                qkv[place, turned:] = r[rows, turned:]

        def turned_round(j):
            slot = lax.rem(j, 2)
            put = lambda j: pltpu.make_async_copy(wt.at[slot], wt_ref.at[:, block_rows(j, TILE)], so.at[1, slot])
            pl.when(j > 1)(lambda: put(j - 2).wait())
            wt[slot] = w[block_rows(j, TILE), :].T
            put(j).start()

        def near():
            of_a.passed_on(RA, LA)
            loop(D // TILE, turned_round)
            of_a.passed_on(RB, LB)
            of_a.start(RE, LE, MB, MC)
            of_dy.start(RA, LA, RB, LB, MA)

        stream(ring, of_a, a_all, tile, sb, None, None, None, work, gather_events(of_a, near))
        end([*tables, *[pltpu.make_async_copy(wt.at[k], wt_ref.at[:, upto(TILE)], so.at[1, k]) for k in BOTH]])

    pl.run_scoped(products, V((T, D), BF), V((D, turned + NK), BF), *[V((n * T, HEAD), F32)] * 2, V((2, turned + NK, TILE), BF))
    outs[0].start()
    set_gap(gap)

    def rest(wd):
        ring, _, of_dy, of_o = links()
        wd_in = pltpu.make_async_copy(wd_ref, wd, so.at[0, 0])
        wd_in.start()
        blocks = n * T // BQ

        def attention(iq):
            attend_block(iq, qkv, o, ot, lse, qs, top, mix, gap)
            steps(iq, {blocks - 2: lambda: of_dy.passed_on(RA, LA)})

        loop(blocks, attention)
        begin(outs[1:])
        of_dy.passed_on(RB, LB)
        of_dy.start(RE, LE, MB, MC)

        def product(shard, rows, then):
            at = pl.ds(pl.multiple_of(shard * T + rows.start, T // 2), rows.size)
            chunked(D, D // RUNS, lambda c: then(c, dot(o[at, :], wo[:, c])))

        scatter = Scatter(ring, of_o, product, stg, p, s, acc, tr, fr)
        scatter.send()
        wd_in.wait()

        def work(u, units, x, o):
            def run(c):
                o[:, c] = dot(x[...], wd[c, :], NT).astype(BF)
            chunked(wd.shape[0], TILE, run)

        stream(ring, of_dy, dy_all, tile, sb, dhid, dt, so, work, gather_events(of_dy))
        of_o.sent(M3, M4)
        x_again.start()
        scatter.pass_on()
        end([x_again, *outs])

        def last(at, total):
            h = (stg[0, at, :].astype(F32) + total).astype(BF)
            s[0, at, :] = h
            h = h.astype(F32)
            stg[1, at, :] = (h * norm_scale(h)).astype(BF)

        scatter.finish(last, lambda k, at: [pltpu.make_async_copy(a.at[at], b.at[at], sl.at[2 * k + m]) for m, (a, b) in enumerate(((s.at[0], h_ref), (stg.at[1], b_ref)))])
        of_o.sent(R2, L2, R3, L3, R4, L4)

    pl.run_scoped(rest, V(wd_ref.shape, BF))


def front(x, dy, wq, wk, wv, wo, wd, n, cid):
    T, D = x.shape
    NQ, F, tokens = wo.shape[0], wd.shape[0], n * T
    N, cols = NQ + 2 * HEAD, NQ // HEAD * BQ
    stat = (tokens // BQ, 1, cols)
    table, row = S((tokens, HEAD), F32), S((T, D), BF)
    small = angles(jnp.concatenate([jnp.arange(HEAD), jnp.arange(0, tokens, HEAD)]))
    outs = [S((n, T, D), BF), S((tokens, N), BF), S((n, T, D), BF), S((n, T, F), BF), S((tokens, NQ), BF), S(stat, F32), table, table, row, row, S((N, D), BF), S((NQ, tokens), BF)]
    scratch = [V((2, T, D), BF), V((2, *small[0].shape), F32), V((tokens, N), BF), V((tokens, NQ), BF), V((NQ, tokens), BF),
               V(stat, F32), V((cols, HEAD), BF), V((1, cols), F32), V((HEAD + 8, cols), F32), V((BK, BQ), jnp.int32), V((NQ, D), BF), V((2, T, F), BF),
               *scatter_scratch(T, D), DMA((3 * COPIES,)), DMA((3 * COPIES,)), DMA((2, 3)), DMA((2, 3)), DMA((15,))]
    return call(functools.partial(_front, n=n), [x, dy, wq, wk, wv, wo, wd, *small], outs, scratch, 2 * tokens * D * (N + F + NQ), "front", cid)


def _back(t_ref, x_ref, wt_ref, a_ref, dh_all, heads_ref, b_ref, du_ref, dx_ref, by_q, by_k, by_v, by_o, by_up,
          w, t, heads, du, out, ft, stg, p, s, acc, tr, fr, ss, rs, sl, sf, sg, *, n):
    ring, links = Ring(n), Links(ss, rs)
    T, D = x_ref.shape
    NQ, NK = by_q.shape[1], by_k.shape[1]
    columns = [upto(NQ), pl.ds(NQ, NK), pl.ds(NQ + NK, NK)]
    pairs = ((t_ref, t), (wt_ref, w), (du_ref, du), (heads_ref, heads), (x_ref, stg.at[0]), (dh_all.at[ring.me], stg.at[1]))
    *first, du_in, heads_in, x_in, dh_in = [pltpu.make_async_copy(a, b, sl.at[k]) for k, (a, b) in enumerate(pairs)]
    begin(first)
    ring.barrier()
    end(first)
    begin([du_in, heads_in])
    late = lambda j: [(upto(du.shape[2]), by_up.at[block_rows(j - EARLY, TILE)])]
    fill = Fill((([b_ref], du, out, None, [late], EARLY, D // TILE),
                 ([a_ref], t, out, None, [lambda j: [(c, r.at[block_rows(j, TILE)]) for c, r in zip(columns, (by_q, by_k, by_v))]]),
                 ([dh_all], heads, out, NN, [lambda j: [(upto(TILE), by_o.at[:, block_rows(j, TILE)])]])), ft, sf, sg)
    fill.fetch(0)

    def product(shard, rows, then):
        chunked(D, D // RUNS, lambda c: then(c, dot(t[shard, rows, :], w[:, c])))

    scatter = Scatter(ring, links, product, stg, p, s, acc, tr, fr)
    scatter.send()
    end([du_in, heads_in])

    def rows_in():
        links.sent(M3, M4)
        begin([x_in, dh_in])
    def beside(k):
        fill.step(k)
        steps(k, [None, scatter.pass_on, rows_in])
    loop(fill.steps, beside)
    fill.finish()
    end([x_in, dh_in])

    def last(at, total):
        s[0, at, :] = (stg[1, at, :].astype(F32) + unnorm(stg[0, at, :].astype(F32), total)).astype(BF)

    scatter.finish(last, lambda k, at: [pltpu.make_async_copy(s.at[0, at], dx_ref.at[at], sl.at[k])])
    links.sent(R2, L2, R3, L3, R4, L4)


def back(dqkv, x, wt, ws, a, dh_all, heads, b, du, n, cid):
    T, D = x.shape
    K, NQ, F = dqkv.shape[2], heads.shape[0], du.shape[2]
    scratch = [V((K, D), BF), V(dqkv.shape, BF), V(heads.shape, BF), V(du.shape, BF), V((2, TILE, F), BF), V((2, n, T, TILE), BF), *scatter_scratch(T, D),
               DMA((COPIES,)), DMA((COPIES,)), DMA((8,)), DMA((2,)), DMA((2, 3))]
    outs = [S((T, D), BF), *(S(w.shape, BF) for w in ws), S((NQ, D), BF), S((D - EARLY * TILE, F), BF)]
    return call(functools.partial(_back, n=n), [dqkv, x, wt, a, dh_all, heads, b, du], outs, scratch, 6 * n * T * D * K, "back", cid)


def _land(*refs):
    m = (len(refs) - 2) // 3
    ins, outs, tiles, sem = refs[:m], refs[m + 1:2 * m + 1], refs[2 * m + 1:-1], refs[-1]
    outs = [*outs[:-1], outs[-1].at[pl.ds(EARLY * TILE, ins[-1].shape[0])]]
    come = [pltpu.make_async_copy(a, b, sem.at[k]) for k, (a, b) in enumerate(zip(ins, tiles))]
    go = [pltpu.make_async_copy(a, b, sem.at[k]) for k, (a, b) in enumerate(zip(tiles, outs))]
    begin(come)
    for a, b in zip(come, go):
        a.wait()
        b.start()
    end(go)


def land(arrays, whole):
    shapes = [S(t.shape, BF) for t in (*arrays[:-1], whole)]
    return call(_land, [*arrays, whole], shapes, [*(V(t.shape, BF) for t in arrays), DMA((len(arrays),))], 0, "land", aliases={len(arrays): len(arrays) - 1})


def mlp_links(b_ref, bg, frm, stg, s3, s1, p1, p3, tr, fr, ss, rs, n):
    ring, links = Ring(n), Links(ss, rs)
    T = b_ref.shape[0]
    H, Q = T // 2, T // 4
    first = upto(Q)
    frp, frn = fr.at[0], fr.at[1]
    nx, pv, mt = ring.next, ring.prev, ring.mate
    lo, hi = upto(H), pl.ds(H, H)
    gather_copies(links, ring, b_ref, bg, T, True)
    at = lambda ref: [ref.at[k] for k in range(ref.shape[0])]
    pa, pb, pc, pd, sa, sb1, sc, sd1, even, odd, on, off = [*at(p1), *at(s1), *at(stg), *at(tr)]
    for k, src, dst, to in ((M5, odd, frm, mt), (M0, odd.at[hi], pa, mt), (M1, even, p3, mt), (M2, even.at[hi], pb, mt), (M3, odd.at[hi], pc, mt), (M4, even.at[hi], pd, mt),
                            (R1, s3.at[lo], on, nx), (L1, s3.at[hi], off, pv),
                            (L2, sa.at[first], frn.at[first], pv), (L5, sb1.at[first], frn.at[pl.ds(Q, Q)], pv),
                            (R2, sa.at[pl.ds(Q, Q)], frp.at[pl.ds(H, Q)], nx), (R5, sb1.at[pl.ds(Q, Q)], frp.at[pl.ds(H + Q, Q)], nx),
                            (R3, sc.at[first], frp.at[first], nx), (R4, sd1.at[first], frp.at[pl.ds(Q, Q)], nx),
                            (L3, sc.at[pl.ds(Q, Q)], frn.at[pl.ds(H, Q)], pv), (L4, sd1.at[pl.ds(Q, Q)], frn.at[pl.ds(H + Q, Q)], pv)):
        links.put(k, src, dst, to)
    return ring, links


def pair_sum(acc, p1, s1, tr, k, base=0, first=None):
    H = s1.shape[1]

    def add(at, *further):
        v = acc[pl.ds(base + at.start, at.size), :] + p1[k, at, :].astype(F32)
        s1[k, at, :] = sum([tr[t].astype(F32) for t in further], v).astype(BF)

    if first is None:
        chunked(H, 16, add)
    else:
        for side in BOTH:
            chunked(H // 2, 16, lambda at: add(pl.ds(side * (H // 2) + at.start, at.size), (side, pl.ds(first + at.start, at.size))))


def _units(b_ref, dhid_ref, wg_ref, wu_ref, bg, hid, dgo, duo, own, frm, bt, acc, stg, s3, s1, p1, p3, tr, fr, ss, rs, sw, sb, sd, so, sl, n, wg, wu, dht, st):
    ring, links = mlp_links(b_ref, bg, frm, stg, s3, s1, p1, p3, tr, fr, ss, rs, n)
    T, D = b_ref.shape
    F = wg_ref.shape[1]
    H, NC, NB = T // 2, F // 3, D // 2
    me, nx, pv, mt = ring.me, ring.next, ring.prev, ring.mate
    Q0, Q1, Q2, Q3 = range(4)
    quarters = lambda *shards: tuple((shard, q) for shard in shards for q in range(4))
    pvm, nxm = ring.prevm, ring.nextm
    units = [quarters(me), ((pv, Q0), (nx, Q2), (pvm, Q0), (nxm, Q2)), ((pv, Q1), (nx, Q3), (pvm, Q1), (nxm, Q3)), quarters(ring.opp), quarters(ring.oppm),
             ((nx, Q0), (pv, Q2), (nxm, Q0), (pvm, Q2)), ((nx, Q1), (pv, Q3), (nxm, Q1), (pvm, Q3)), quarters(mt)]
    count = len(units)

    def fetch(u, slot):
        return moves(u, units, bg, bt.at[slot], sb.at[slot]) + moves(u, units, dhid_ref, dht.at[slot], sd.at[slot])

    def store(u):
        return [c for m, ref in enumerate((hid, dgo, duo)) for c in moves(u, units, ref, st.at[m], so.at[m], True)]

    def weights(j):
        s = block_rows(j, NC)
        return [pltpu.make_async_copy(a.at[:, s], b.at[:, s], sw.at[k, j]) for k, (a, b) in enumerate(((wg_ref, wg), (wu_ref, wu)))]

    pairs = ((b_ref, bt.at[0]), (dhid_ref.at[me], dht.at[0]), (bt.at[0], bg.at[me]), (acc, own))
    *first, keep, own_out = [pltpu.make_async_copy(a, b, sl.at[k]) for k, (a, b) in enumerate(pairs)]
    begin(first)
    for j in range(F // NC):
        begin(weights(j))
    ring.barrier()
    links.start(RA, LA, RB, LB, MA)
    end(first)
    keep.start()

    pair = functools.partial(pair_sum, acc, p1, s1, tr)

    def late0():
        links.passed_on(RA, LA)
        links.start(MB, MC)

    def post0():
        keep.wait()
        own_out.start()
        links.got(MB, MC)
        begin(fetch(1, 1))

    def mid1():
        own_out.wait()
        links.passed_on(RB)
        links.start(RE)
        links.passed_on(LB)
        links.start(LE, MH, MI)

    def late1():
        links.got(MH, MI)
        begin(fetch(2, 0))

    def mid2():
        links.got(M0)
        pair(0)
        links.start(L2, R2)

    def post2():
        links.start(M2)
        far()
        begin(fetch(3, 1))

    def mid3():
        links.got(M2)
        pair(1)
        links.start(L5, R5)

    def late3():
        links.got(MD, ME)
        begin(fetch(4, 0))
        links.sent(M2)

    def late4():
        links.got(MF, MG)
        begin(fetch(5, 1))

    def mid5():
        links.got(M1)

        def add(at):
            s3[at, :] = (acc[at, :] + p3[at, :].astype(F32)).astype(BF)
        chunked(T, 16, add)
        links.start(R1, L1)
        links.sent(M0)

    def late6():
        links.got(MA)
        begin(fetch(7, 1))

    def pairs_left():
        links.got(M3, R1, L1)
        pair(2, 0, 0)
        links.start(R3, L3)
        links.got(M4)
        pair(3, H, H // 2)
        links.start(R4, L4)

    def post7():
        links.start(M5)
        end(store(7))

    _, _, _, far, _, last, _ = gather_events(links)
    starting = lambda *ks: lambda: links.start(*ks)
    mids = [None, mid1, mid2, mid3, last, mid5, lambda: links.sent(M1), lambda: links.sent(M3)]
    lates = [late0, late1, None, late3, late4, lambda: begin(fetch(6, 0)), late6]
    posts = [post0, starting(M0), post2, None, starting(M1), starting(M3), starting(M4), post7]

    def forth_unit(u, slot):
        @pl.when(u > 0)
        def _():
            end(fetch(u, slot))
            end(store(u - 1))

        def forth(j):
            @pl.when(u == 0)
            def _():
                end(weights(j))
            s = block_rows(j, NC)
            x = bt[slot]
            gate, up = dot(x, wg[:, s]), dot(x, wu[:, s])
            d = dht[slot, :, s].astype(F32)
            sig = jax.nn.sigmoid(gate)
            act = gate * sig
            for m, v in enumerate((act * up, d * up * (sig + act * (1 - sig)), d * act)):
                st[m, :, s] = v.astype(BF)
            pl.when((u == count - 1) & (j == 0))(pairs_left)

        loop(F // NC, forth)
        begin(store(u))

    def unit(u):
        slot = lax.rem(u, 2)
        forth_unit(u, slot)
        steps(u, mids)
        among = lambda *us: functools.reduce(jnp.logical_or, [u == k for k in us])
        side = jnp.where(among(2, 4, 6), 0, 1)

        def back(c):
            v = dot(st[1], wg[c, :], NT) + dot(st[2], wu[c, :], NT)

            @pl.when(among(0, 3))
            def _():
                acc[:, c] = v

            @pl.when(among(4, 7))
            def _():
                stg[side, :, c] = v.astype(BF)

            @pl.when(among(1, 2, 5, 6))
            def _():
                acc[pl.ds(pl.multiple_of(jnp.where(u == 6, H, 0), H), H), c] = v[:H]
                stg[side, H:, c] = v[H:].astype(BF)

        half = D // NB // 2
        loop(half, lambda j: back(block_rows(j, NB)))
        steps(u, lates)
        loop(D // NB, lambda j: back(block_rows(j, NB)), half)
        steps(u, posts)

    loop(count, unit)


def _middle(b_ref, dhid_ref, wg_ref, wu_ref, h_ref, dy_ref, wo_ref, dy_all, bg, hid, dgo, duo, dh_all, out, by_down, by_gate, by_up, own, frm,
            bt, acc, stg, s3, s1, p1, p3, tr, fr, ot, ss, rs, sw, sb, sd, so, sl, sf, sg, *, n):
    T, D = b_ref.shape
    F, NQ = wg_ref.shape[1], wo_ref.shape[0]
    shared = (bt, acc, stg, s3, s1, p1, p3, tr, fr, ss, rs)
    pl.run_scoped(functools.partial(_units, b_ref, dhid_ref, wg_ref, wu_ref, bg, hid, dgo, duo, own, frm, *shared, sw, sb, sd, so, sl, n),
                  V((D, F), BF), V((D, F), BF), V((2, T, F), BF), V((3, T, F), BF))

    def rest(fixed, left, tile, wo):
        ring, links = mlp_links(b_ref, bg, frm, *shared[2:], n)
        of_dh = Links(ss, rs, COPIES)
        gather_copies(of_dh, ring, stg.at[0], dh_all, T)
        pairs = ((hid, fixed.at[1]), (dgo, fixed.at[0]), (duo, fixed.at[1]), (wo_ref, wo), (own, acc), (frm, bt.at[0]), (h_ref, bt.at[1]), (dy_ref, s3),
                 (stg.at[0], dh_all.at[ring.me]))
        hid_in, dg_in, du_in, wo_in, own_in, frm_in, *rows_in, keep = [pltpu.make_async_copy(a, b, sl.at[k]) for k, (a, b) in enumerate(pairs)]
        side = lambda ref: lambda j: [(upto(F), ref.at[block_rows(j, TILE)])]
        fill = Fill((([dy_all], fixed.at[1], left, TN, [lambda j: [(pl.ds(a, TILE), by_down.at[pl.ds(a, TILE), block_rows(j, TILE)]) for a in range(0, F, TILE)]]),
                     ([bg, bg], fixed, left, None, [side(by_gate), side(by_up)], 0, D // TILE + EARLY)), tile, sf, sg)
        hid_in.start()
        fill.fetch(0)
        own_in.start()
        links.sent(R1, L1)
        begin(rows_in)
        hid_in.wait()

        def mates_part():
            links.got(M5)
            frm_in.start()
            own_in.wait()
            add_rows(links, acc, (R2, R5), fr.at[0], T // 2)
            add_rows(links, acc, (L2, L5), fr.at[1], 0)

        def scattered():
            end([frm_in, *rows_in])
            links.sent(M4)

            def add(at):
                acc[at, :] += bt[0, at, :].astype(F32)
            chunked(T, 16, add)

            def last(at, total):
                stg[0, at, :] = (s3[at, :].astype(F32) + unnorm(bt[1, at, :].astype(F32), total)).astype(BF)

            finish(links, acc, fr, last)
            of_dh.start(RA, LA, RB, LB, MA)
            keep.start()

        def near():
            of_dh.passed_on(RB, LB)
            of_dh.start(RE, LE, MB, MC)

        def work(u, units, x, o):
            o[...] = dot(x[...], wo[...], NT).astype(BF)

        mate, _, mates, far, fars, last, lasts = gather_events(of_dh)
        events = {0: mates_part, 1: scattered, 3: lambda: begin([dg_in, wo_in]), 5: lambda: (mate(), end([keep, wo_in, dg_in]), of_dh.passed_on(RA, LA)),
                  7: du_in.start, 8: near, 10: mates, 13: far, 14: fars, 15: du_in.wait, fill.steps - 2: last, fill.steps - 1: lasts}
        schedule = (6, 7, 11, 12, 15, 16, fill.steps - 1, fill.steps)
        stream(ring, of_dh, dh_all, bt, sb, out, ot, sd, work, events, schedule, lambda k: pl.when(k < fill.steps)(lambda: fill.step(k)))
        fill.finish()
        links.sent(*GATHER, MH, MI, R2, R3, R4, R5, L2, L3, L4, L5, M5)

    pl.run_scoped(rest, V((2, n, T, F), BF), V((2, TILE, F), BF), V((2, n, T, TILE), BF), V((NQ, D), BF))


def middle(b, dhid, wg, wu, h, dy, wo, dy_all, n, cid):
    T, D = b.shape
    F, NQ = wg.shape[1], wo.shape[0]
    H = T // 2
    row, halves = V((T, D), BF), V((4, H, D), BF)
    scratch = [V((2, T, D), BF), V((T, D), F32), V((2, T, D), BF), row, halves, halves, row, V((2, H, D), BF), V((2, T, D), BF), V((2, T, NQ), BF),
               DMA((2 * COPIES,)), DMA((2 * COPIES,)), DMA((2, 3)), DMA((2, 4)), DMA((2, 4)), DMA((3, 4)), DMA((9,)), DMA((2,)), DMA((2, 3))]
    wide, full, narrow = S((n, T, F), BF), S((n, T, D), BF), S((D, F), BF)
    outs = [full, wide, wide, wide, full, S((n, T, NQ), BF), S((F, D), BF), narrow, narrow, S((T, D), F32), S((T, D), BF)]
    got = call(functools.partial(_middle, n=n), [b, dhid, wg, wu, h, dy, wo, dy_all], outs, scratch, 14 * n * T * D * F, "middle", cid)
    return got[4:9], got[0], got[3]


def solution(mesh):
    n = mesh.shape["tp"]

    def step(x, dy, wq, wk, wv, wo, wg, wu, wd):
        x, dy = x[0], dy[0]
        blocks = lambda t: t.reshape(n, -1, t.shape[1])
        a, qkv, dy_all, dhid, heads, lse, cos, sin, h, b, wt, heads_t = front(x, dy, wq, wk, wv, wo, wd, n, 0)
        (dh_all, d_heads, *by_mlp), b, du = middle(b, dhid, wg, wu, h, dy, wo, dy_all, n, 1)
        dqkv, by_down, by_gate, by_up = attend_bwd(qkv, flat(d_heads), heads, lse, cos, sin, by_mlp)
        dx, *by_qkvo, by_up = land(back(blocks(dqkv), x, wt, [wq, wk, wv], a, dh_all, heads_t, b, du, n, 2), by_up)
        return dx[None], *by_qkvo, by_gate, by_up, by_down

    states, by_columns, by_rows = P("dp", "tp", None), P(None, "tp"), P("tp", None)
    weights = (by_columns, by_columns, by_columns, by_rows, by_columns, by_columns, by_rows)
    own = tuple(P("dp", "tp") if spec == by_columns else P(("dp", "tp"), None) for spec in weights)
    return jax.shard_map(step, mesh=mesh, in_specs=(states, states, *weights), out_specs=(states, *own), check_vma=False)
```

```python
import functools

import jax
import jax.numpy as jnp
from jax import lax
from jax.experimental import pallas as pl
from jax.experimental.pallas import tpu as pltpu
from jax.sharding import PartitionSpec as P

BF, F32 = jnp.bfloat16, jnp.float32
HEAD = 128
THETA = 10000
NEG = -1e30
HIDDEN = 2 * NEG
LOG2E = 1.4426950408889634
SCALE = HEAD**-0.5
MOST = 67_000_000
BQ = BK = 512
TILE = 512
EARLY = 3
NN, NT, TN = ((((a,), (b,)), ((), ())) for a, b in ((1, 0), (1, 1), (0, 0)))
ANY = pl.BlockSpec(memory_space=pl.ANY)
S, V, DMA = jax.ShapeDtypeStruct, pltpu.VMEM, pltpu.SemaphoreType.DMA

RA, RB, RC, RD, RE, LA, LB, LC, LD, LE, MA, MB, MC, MD, ME, MF, MG = GATHER = range(17)
R1, R2, R3, R4, R5, L1, L2, L3, L4, L5, M0, M1, M2, M3, M4, M5, MH, MI = range(17, 35)
COPIES = 35
RUNS = 2
LO, HI = BOTH = range(2)


def dot(a, b, dims=NN, **kw):
    return lax.dot_general(a, b, dims, preferred_element_type=F32, **kw)


def norm_scale(wide):
    return lax.rsqrt(jnp.mean(wide * wide, -1, keepdims=True) + 1e-6)


def unnorm(wide, d):
    scale = norm_scale(wide)
    return d * scale - wide * (scale * scale * scale * jnp.mean(d * wide, -1, keepdims=True))


def turn(t, cos, sin):
    return t * cos + pltpu.roll(t, HEAD // 2, 1) * sin


def angles(places):
    half = HEAD // 2
    a = places.astype(F32)[:, None] * THETA ** (-jnp.arange(half, dtype=F32) / half)
    cos, sin = jnp.cos(a), jnp.sin(a)
    return jnp.concatenate([cos, cos], -1), jnp.concatenate([-sin, sin], -1)


class Ring:
    def __init__(self, n):
        self.me = lax.axis_index("tp")
        core, chips = lax.rem(self.me, 2), n // 2
        chip = [lax.rem(lax.div(self.me, 2) + k, chips) for k in range(chips)]
        self.next, self.opp, self.prev = [2 * c + core for c in chip[1:]]
        self.mate, self.nextm, self.oppm, self.prevm = [2 * c + 1 - core for c in chip]

    def barrier(self):
        b = pltpu.get_barrier_semaphore()
        near = (self.next, self.prev, self.mate)
        for d in near:
            pl.semaphore_signal(b, inc=1, device_id={"tp": d}, device_id_type=pl.DeviceIdType.MESH)
        pl.semaphore_wait(b, len(near))


class Links:
    def __init__(self, ss, rs, base=0):
        self.ss, self.rs, self.base, self.made = ss, rs, base, {}

    def put(self, k, src, dst, dev):
        self.made[k] = lambda: pltpu.make_async_remote_copy(src_ref=src, dst_ref=dst, send_sem=self.ss.at[self.base + k], recv_sem=self.rs.at[self.base + k],
                                                            device_id={"tp": dev}, device_id_type=pl.DeviceIdType.MESH)

    def start(self, *ks):
        for k in ks:
            self.made[k]().start()

    def got(self, *ks):
        for k in ks:
            self.made[k]().wait_recv()

    def sent(self, *ks):
        for k in ks:
            self.made[k]().wait_send()

    def passed_on(self, *ks):
        for k in ks:
            self.got(k)
            self.start(k + 2)


def flat(t):
    return t.reshape(-1, t.shape[-1])


def begin(copies):
    for c in copies:
        c.start()


def end(copies):
    for c in copies:
        c.wait()


def pick(u, values):
    out = values[0]
    for k, v in enumerate(values):
        out = jnp.where(u == k, v, out)
    return out


def steps(u, events):
    for k, f in events.items() if isinstance(events, dict) else enumerate(events):
        def run(f=f):
            f()
        if f is not None:
            pl.when(u == k)(run)


def loop(count, f, first=0):
    def body(k, _):
        f(k)
    lax.fori_loop(first, count, body, None)


def block_rows(i, size):
    return pl.ds(pl.multiple_of(i * size, size), size)


def upto(size):
    return pl.ds(0, size)


def chunked(size, width, f):
    loop(size // width, lambda j: f(block_rows(j, width)))


def gather_copies(links, ring, src, dst, T, fine=False):
    H, Q = T // 2, T // 4
    me, nx, pv, mt, opp = ring.me, ring.next, ring.prev, ring.mate, ring.opp
    for k, slot, a, rows, to in ((RA, me, 0, Q, nx), (RB, me, Q, Q, nx), (RC, pv, 0, Q, nx), (RD, pv, Q, Q, nx), (RE, me, H, H, nx),
                                 (LA, me, H, Q, pv), (LB, me, H + Q, Q, pv), (LC, nx, H, Q, pv), (LD, nx, H + Q, Q, pv), (LE, me, 0, H, pv),
                                 (MA, me, 0, T, mt), (MB, pv, 0, Q if fine else H, mt), (MC, nx, H, Q if fine else H, mt),
                                 (MH, pv, Q, Q, mt), (MI, nx, H + Q, Q, mt), (MD, opp, 0, H, mt), (ME, opp, H, H, mt), (MF, pv, H, H, mt), (MG, nx, 0, H, mt)):
        at = pl.ds(a, rows)
        links.put(k, src.at[at] if slot is me else dst.at[slot, at], dst.at[slot, at], to)


def whole(shard):
    return (shard, LO), (shard, HI)


def moves(u, units, far, near, sem, back=False):
    parts = len(units[0])
    size = near.shape[0] // parts
    out = []
    for k in range(parts):
        shard, place = (pick(u, [x[k][m] for x in units]) for m in BOTH)
        ends = far.at[shard, block_rows(place, size)], near.at[pl.ds(k * size, size)]
        out.append(pltpu.make_async_copy(*(ends[::-1] if back else ends), sem.at[k]))
    return out


def rows_of_unit(u, units, k, H):
    shard, half = (pick(u, [x[k][m] for x in units]) for m in BOTH)
    return pl.ds(pl.multiple_of((2 * shard + half) * H, H), H)


def stream(ring, links, src, tile, sin, dst, out, sout, work, events, schedule=range(8), beside=None):
    units = [whole(ring.me), whole(ring.mate), ((ring.prev, LO), (ring.next, HI)), ((ring.prevm, LO), (ring.nextm, HI)), whole(ring.opp),
             whole(ring.oppm), ((ring.prev, HI), (ring.next, LO)), ((ring.prevm, HI), (ring.nextm, LO))]
    fetch = lambda u, slot: moves(u, units, src, tile.at[slot], sin.at[slot])
    store = lambda u, slot: moves(u, units, dst, out.at[slot], sout.at[slot], True)
    latest = lambda k: sum(jnp.where(k < s, 0, 1) for s in schedule) - 1

    def fetch_for(k):
        u = latest(k)

        @pl.when(latest(k - 1) < u)
        def _():
            begin(fetch(u, lax.rem(u, 2)))

    fetch_for(0)

    def step(k):
        if beside is not None:
            beside(k)
        u = latest(k)

        @pl.when(latest(k - 1) < u)
        def _():
            slot = lax.rem(u, 2)
            end(fetch(u, slot))

            if dst is None:
                work(u, units, tile.at[slot])
            else:
                pl.when(u > 1)(lambda: end(store(u - 2, slot)))
                work(u, units, tile.at[slot], out.at[slot])
                begin(store(u, slot))

        steps(k, events)
        fetch_for(k + 1)

    loop(schedule[-1] + 1, step)
    if dst is not None:
        end(store(len(units) - 2, 0) + store(len(units) - 1, 1))
    links.sent(*GATHER)


class Fill:
    def __init__(self, jobs, tile, sin, sout):
        self.tile, self.sin, self.sout, self.jobs, at = tile, sin, sout, [], 0
        for srcs, fixed, out, right, ends, *tiles in jobs:
            per = srcs[0].shape[2] // TILE
            first, last = tiles or (0, per * len(srcs))
            self.jobs.append((at, last - first, first, per, srcs, fixed, out, right, ends))
            at += last - first
        self.steps = at

    def load(self, src, j, slot):
        return pltpu.make_async_copy(src.at[:, :, block_rows(j, TILE)], self.tile.at[slot], self.sin.at[slot])

    def fetch(self, k):
        for at, count, first, per, srcs, *_ in self.jobs:
            i = k - at + first
            for m, src in enumerate(srcs):
                mine = (k >= at) & (k < at + count) & (lax.div(i, per) == m)
                pl.when(mine)(lambda: begin([self.load(src, i - m * per, lax.rem(k, 2))]))

    def step(self, k):
        slot = lax.rem(k, 2)
        end([self.load(self.jobs[0][4][0], 0, slot)])
        self.fetch(k + 1)
        before = None
        for at, count, first, per, srcs, fixed, out, right, ends in self.jobs:
            def store(m, j, slot, out=out, ends=ends):
                return [pltpu.make_async_copy(out.at[slot, :, a], b, self.sout.at[slot, i]) for i, (a, b) in enumerate(ends[m](j))]

            @pl.when((k >= at) & (k < at + count))
            def _():
                which, j = lax.div(k - at + first, per), lax.rem(k - at + first, per)
                pl.when(k > at + 1)(lambda: end(store(0, j, slot)))
                if before is not None:
                    pl.when(k <= at + 1)(lambda: end(before(0, EARLY, slot)))
                t = self.tile[slot].reshape(-1, TILE)
                f = flat(fixed[which] if len(srcs) > 1 else fixed[...])
                r = dot(f, t, right) if right else dot(t, f, TN)
                for a in range(0, r.shape[0], TILE):
                    out[slot, :, (a if right else 0):(a if right else 0) + r.shape[1]] = r[a:a + TILE].astype(BF)
                for m in range(len(srcs)):
                    pl.when(which == m)(lambda: begin(store(m, j, slot)))
            before = store
        self.finish = lambda: end([c for slot in BOTH for c in before(0, EARLY, slot)])


def gather_events(links, near=None):
    def far():
        links.got(RC, RD)
        links.start(MD)
        links.got(LC, LD)
        links.start(ME)

    def last():
        links.got(RE)
        links.start(MF)
        links.got(LE)
        links.start(MG)

    got = lambda *ks: lambda: links.got(*ks)
    return [got(MA), near, got(MB, MC), far, got(MD, ME), last, got(MF, MG)]


def add_rows(links, acc, ms, fr, half):
    def add(at):
        at = pl.ds(half + at.start, at.size)
        acc[at, :] += fr[at, :].astype(F32)
    links.got(*ms)
    chunked(acc.shape[0] // 2, 16, add)


def finish(links, acc, fr, last, out=None):
    Q = acc.shape[0] // 4
    quarters = [(k, pl.ds(k * Q, Q)) for k in (0, 2, 1, 3)]
    for m, (k, rows) in zip((R3, L3, R4, L4), quarters):
        def total(at):
            at = pl.ds(k * Q + at.start, at.size)
            last(at, acc[at, :] + fr[k // 2, at, :].astype(F32))
        links.got(m)
        chunked(Q, 16, total)
        if out is not None:
            begin(out(k, rows))
    if out is not None:
        end([c for k, rows in quarters for c in out(k, rows)])


class Scatter:
    def __init__(self, ring, links, product, stg, p, s, acc, tr, fr):
        self.ring, self.links, self.product, self.stg, self.p, self.s, self.acc, self.tr, self.fr = ring, links, product, stg, p, s, acc, tr, fr
        T = acc.shape[0]
        H = T // 2
        nx, pv, mt = ring.next, ring.prev, ring.mate
        self.every, self.lo, self.hi = every, lo, hi = upto(T), upto(H), pl.ds(H, H)
        quarters = [pl.ds(a, H // 2) for a in range(0, T, H // 2)]
        at = lambda ref: [ref.at[k] for k in range(ref.shape[0])]
        even, odd, pa, pb, pc, pd, so, sn, sp, on, off, fp, fn = [*at(stg), *at(p), *at(s), *at(tr), *at(fr)]
        NB = acc.shape[1] // RUNS
        for j, k in enumerate((M0, M5)):
            links.put(k, even.at[:, pl.ds(j * NB, NB)], pa.at[:, pl.ds(j * NB, NB)], mt)
        for k, src, dst, to in ((M2, odd, pb, mt), (M3, even, pc, mt), (M4, odd, pd, mt),
                                (R1, so.at[lo], on, nx), (L1, so.at[hi], off, pv), (R2, sn.at[hi], fp.at[hi], nx), (L2, sp.at[lo], fn.at[lo], pv),
                                *((k, sn.at[at], fp.at[at], nx) for k, at in zip((R3, R4), quarters)), *((k, sp.at[at], fn.at[at], pv) for k, at in zip((L3, L4), quarters[2:]))):
            links.put(k, src, dst, to)

    def send(self):
        links, ring, stg, p, s, acc = self.links, self.ring, self.stg, self.p, self.s, self.acc
        runs = (M0, M5)
        shards = (ring.oppm, ring.opp, ring.nextm, ring.prevm, ring.next, ring.prev, ring.mate, ring.me)
        got, sent, start = ((lambda f: lambda *ks: lambda: f(*ks))(f) for f in (links.got, links.sent, links.start))
        before = [None, None, None, sent(*runs), got(M2), got(M3), sent(M2)]
        after = [None, start(R1, L1), start(M2), start(M3), start(R2), start(L2), start(M4)]

        def step(i):
            steps(i, before)

            def then(c, v):
                j = lax.div(c.start, c.size)

                def to_mate(k, on=()):
                    def f():
                        stg[k, :, c] = v.astype(BF)
                        steps(j, on)
                    return f

                def to_chip(k, rows, wait=()):
                    def f():
                        steps(j, wait)
                        s[k, rows, c] = (v[rows.start:rows.start + rows.size] + p[k, rows, c].astype(F32)).astype(BF)
                    return f

                def keep():
                    acc[:, c] = v

                steps(i, [to_mate(0, [start(k) for k in runs]), to_chip(0, self.every, [got(k) for k in runs]), to_mate(1), to_mate(0), to_chip(1, self.hi),
                          to_chip(2, self.lo), to_mate(1), keep])

            self.product(pick(i, shards), self.every, then)
            steps(i, after)

        loop(len(shards), step)

    def pass_on(self):
        H = self.lo.size

        def step(i):
            rows = block_rows(i, H)
            steps(i, [lambda: self.links.got(R1), lambda: self.links.got(L1)])

            def then(c, v):
                self.s[1 + i, rows, c] = (v + self.p[1 + i, rows, c].astype(F32) + self.tr[i, :, c].astype(F32)).astype(BF)
            self.product(pick(i, (self.ring.next, self.ring.prev)), rows, then)
            steps(i, [lambda: self.links.start(R3, R4), lambda: self.links.start(L3, L4)])

        loop(2, step)

    def finish(self, last, out):
        self.links.sent(R1, L1)
        p = self.p.at[3]
        for ms, fr, half in (([M4], p, self.hi), ([], p, self.lo), ([R2], self.fr.at[LO], self.hi), ([L2], self.fr.at[HI], self.lo)):
            add_rows(self.links, self.acc, ms, fr, half.start)
        finish(self.links, self.acc, self.fr, last, out)


def scatter_scratch(T, D):
    return [V((2, T, D), BF), V((4, T, D), BF), V((3, T, D), BF), V((T, D), F32), V((2, T // 2, D), BF), V((2, T, D), BF)]


def call(body, args, outs, scratch, flops, name, cid=None, aliases=()):
    return pl.pallas_call(
        body, in_specs=[ANY] * len(args), out_specs=[ANY] * len(outs), out_shape=outs, scratch_shapes=scratch, name=name, input_output_aliases=dict(aliases),
        compiler_params=pltpu.CompilerParams(collective_id=cid, has_side_effects=True, vmem_limit_bytes=MOST),
        cost_estimate=pl.CostEstimate(flops=flops, bytes_accessed=sum(t.size for t in (*args, *outs)), transcendentals=0),
    )(*args)


def rows_of(t):
    return jnp.concatenate([t[:, a:a + HEAD] for a in range(0, t.shape[1], HEAD)], axis=0)


def set_gap(gap):
    gap[...] = lax.broadcasted_iota(jnp.int32, gap.shape, 1) - lax.broadcasted_iota(jnp.int32, gap.shape, 0)


def key_blocks(iq, block):
    per = BQ // BK
    loop(iq * per, lambda j: block(j, False))
    loop((iq + 1) * per, lambda j: block(j, True), iq * per)


def attend_block(iq, qkv, o_ref, ot_ref, lse_ref, qs, top, mix, gap):
    NQ = o_ref.shape[1]
    cols = qs.shape[0]
    mine = block_rows(iq, BQ)
    qs[...] = rows_of(qkv[mine, :NQ])
    top[...] = jnp.full_like(top, NEG)
    mix[...] = jnp.zeros_like(mix)
    ones = jnp.ones((8, BK), BF)
    strips = [slice(a, a + BQ) for a in range(0, cols, BQ)]

    def block(j):
        here = block_rows(j, BK)
        keys = qkv[here, NQ:NQ + HEAD]
        values = jnp.concatenate([qkv[here, NQ + HEAD:].T, ones], axis=0)
        scores = [dot(keys, qs[at, :], NT) for at in strips]
        ps, keeps = [], []
        for at, s in zip(strips, scores):
            s = jnp.where(gap[...] >= j * BK - iq * BQ, s, HIDDEN)
            old = top[:, at]
            new = jnp.maximum(old, s.max(axis=0, keepdims=True))
            top[:, at] = new
            ps.append(jnp.exp2((s - new) * (SCALE * LOG2E)).astype(BF))
            keeps.append(jnp.exp2((old - new) * (SCALE * LOG2E)))
        for at, p, keep in zip(strips, ps, keeps):
            mix[:, at] = mix[:, at] * keep + dot(values, p)

    loop((iq + 1) * (BQ // BK), block)
    total = mix[HEAD:HEAD + 1, :]
    out = mix[:HEAD, :] * (1 / total)
    for h in range(NQ // HEAD):
        part = out[:, h * BQ:(h + 1) * BQ]
        ot_ref[h * HEAD:(h + 1) * HEAD, mine] = part.astype(BF)
        o_ref[mine, h * HEAD:(h + 1) * HEAD] = part.T.astype(BF)
    lse_ref[iq] = top[...] * SCALE + jnp.log(total)


def _attend_bwd(qkv_ref, do_ref, o_ref, lse_ref, cos_ref, sin_ref, *refs):
    ins, (out_ref, *outs), (qkv, do, o, lse, cos, sin, out, qs, dos, dq, dk, dv, gap, *tiles, sem, sl) = refs[:3], refs[3:7], refs[7:]
    NQ = do.shape[1]
    tokens, cols = dk.shape[0], qs.shape[0]
    blocks = tokens // BQ
    ins, outs = ([*x[:-1], x[-1].at[upto(EARLY * TILE)]] for x in (ins, outs))
    come, go = [[pltpu.make_async_copy(x, y, sl.at[k]) for k, (x, y) in enumerate(zip(*ends))] for ends in ((ins, tiles), (tiles, outs))]

    def loads(i):
        at = block_rows(i, BQ)
        pairs = [(x.at[at], y.at[at]) for x, y in ((qkv_ref, qkv), (do_ref, do), (o_ref, o), (cos_ref, cos), (sin_ref, sin))]
        return [pltpu.make_async_copy(x, y, sem.at[i, k]) for k, (x, y) in enumerate([*pairs, (lse_ref.at[i], lse.at[i])])]

    def store(i, columns, k):
        at = block_rows(i, BQ), columns
        return pltpu.make_async_copy(out.at[at], out_ref.at[at], sem.at[i, k])

    part, rest = upto(NQ), pl.ds(NQ, 2 * HEAD)
    for i in range(blocks):
        begin(loads(i))
    begin(come)
    set_gap(gap)
    dk[...] = jnp.zeros_like(dk)
    dv[...] = jnp.zeros_like(dv)

    def landed(*ks):
        def f():
            for k in ks:
                come[k].wait()
                go[k].start()
        return f

    def queries(iq):
        end(loads(iq))
        steps(iq, {blocks - 2: landed(0), blocks - 1: landed(*range(1, len(come)))})
        mine = block_rows(iq, BQ)
        qs[...] = rows_of(qkv[mine, :NQ])
        dos[...] = rows_of(do[mine, :])
        dq[...] = jnp.zeros_like(dq)
        delta = (dos[...].astype(F32) * rows_of(o[mine, :]).astype(F32)).T.sum(axis=0, keepdims=True)
        lses = lse[iq] * LOG2E

        def piece(j, masked, first, size):
            here = pl.ds(pl.multiple_of(j * BK + first, size), size)
            keys, values = qkv[here, NQ:NQ + HEAD], qkv[here, NQ + HEAD:]
            strips = [slice(a + (first if masked else 0), a + BQ) for a in range(0, cols, BQ)]
            scores = [dot(keys, qs[at, :], NT) for at in strips]
            dps = [dot(values, dos[at, :], NT) for at in strips]
            for at, s, dp in zip(strips, scores, dps):
                p = jnp.exp2(s * (SCALE * LOG2E) - lses[:, at])
                if masked:
                    p = jnp.where(gap[first:first + size, first:] >= j * BK - iq * BQ, p, 0.0)
                ds = (p * (dp - delta[:, at])).astype(BF)
                dv[here, :] += dot(p.astype(BF), dos[at, :])
                dk[here, :] += dot(ds, qs[at, :])
                dq[:, at] += dot(keys.T, ds)

        def block(j, masked):
            size = BK // 2 if masked else BK
            for first in range(0, BK, size):
                piece(j, masked, first, size)

        key_blocks(iq, block)
        back = (dq[...] * SCALE).T
        for h in range(NQ // HEAD):
            out[mine, h * HEAD:(h + 1) * HEAD] = turn(back[h * BQ:(h + 1) * BQ], cos[mine, :], -sin[mine, :]).astype(BF)
        store(iq, part, 0).start()

    loop(blocks, queries)

    def keys(at):
        out[at, NQ:NQ + HEAD] = turn(dk[at, :] * SCALE, cos[at, :], -sin[at, :]).astype(BF)
        out[at, NQ + HEAD:] = dv[at, :].astype(BF)
    chunked(tokens, BQ, keys)
    for i in range(blocks):
        store(i, rest, 1).start()
    end([*go, *(store(i, part, 0) for i in range(blocks)), *(store(i, rest, 1) for i in range(blocks))])


def attend_bwd(qkv, d_out, out, lse, cos, sin, others):
    tokens, NQ = out.shape
    cols = lse.shape[2]
    table, key = V(cos.shape, F32), V((tokens, HEAD), F32)
    scratch = [V(qkv.shape, BF), V(out.shape, BF), V(out.shape, BF), V(lse.shape, F32), table, table, V(qkv.shape, BF), V((cols, HEAD), BF), V((cols, HEAD), BF),
               V((HEAD, cols), F32), key, key, V((BK, BQ), jnp.int32), *(V(t.shape, BF) for t in others[:-1]), V((EARLY * TILE, others[-1].shape[1]), BF),
               DMA((tokens // BQ, 6)), DMA((len(others),))]
    return call(_attend_bwd, [qkv, d_out, out, lse, cos, sin, *others], [S(t.shape, BF) for t in (qkv, *others)], scratch, 5 * tokens * tokens * NQ, "attend_bwd")


def _front(x_ref, dy_ref, wq_ref, wk_ref, wv_ref, wo_ref, wd_ref, c_ref, s_ref, a_all, qkv_ref, dy_all, dhid, o_ref, lse_ref, cos_ref, sin_ref, h_ref, b_ref, wt_ref, ot_ref,
           tile, small, qkv, o, ot, lse, qs, top, mix, gap, wo, dt, stg, p, s, acc, tr, fr, ss, rs, sb, so, sl, *, n):
    T, D = x_ref.shape
    NQ, NK = wq_ref.shape[1], wk_ref.shape[1]
    turned, Q = NQ + NK, T // 4

    def links(an=None):
        ring = Ring(n)
        of_a, of_dy, of_o = (Links(ss, rs, k * COPIES) for k in range(3))
        if an is not None:
            gather_copies(of_a, ring, an, a_all, T)
        gather_copies(of_dy, ring, dy_ref, dy_all, T)
        return ring, of_a, of_dy, of_o

    pairs = ((x_ref, stg.at[0]), (dy_ref, stg.at[1]), (c_ref, small.at[0]), (s_ref, small.at[1]), (wo_ref, wo),
             (x_ref, stg.at[0]), (qkv, qkv_ref), (o, o_ref), (ot, ot_ref), (lse, lse_ref))
    copies = [pltpu.make_async_copy(a, b, sl.at[k]) for k, (a, b) in enumerate(pairs)]
    x_in, dy_in, c_in, s_in, wo_in, x_again, *outs = copies
    x_in.start()

    def products(an, w, cos, sin, wt):
        tables = [pltpu.make_async_copy(a, b, so.at[0, k]) for k, (a, b) in enumerate(((cos, cos_ref), (sin, sin_ref)))]
        ring, of_a, of_dy, _ = links(an)
        keep, keep_dy = (pltpu.make_async_copy(a, b.at[ring.me], so.at[1, k]) for k, (a, b) in enumerate(((an, a_all), (stg.at[1], dy_all))))
        place = [upto(NQ), pl.ds(NQ, NK), pl.ds(turned, NK)]
        loads = [dy_in, c_in, s_in, wo_in] + [pltpu.make_async_copy(r, w.at[:, c], sb.at[0, k]) for k, (r, c) in enumerate(zip((wq_ref, wk_ref, wv_ref), place))]
        begin(loads)
        ring.barrier()
        x_in.wait()
        for q, k in ((0, RA), (2, LA), (1, RB), (3, LB)):

            def norm(at):
                at = pl.ds(q * Q + at.start, at.size)
                wide = stg[0, at, :].astype(F32)
                an[at, :] = (wide * norm_scale(wide)).astype(BF)
            chunked(Q, 16, norm)
            of_a.start(k)
        of_a.start(MA)
        keep.start()
        end(loads)
        keep_dy.start()

        def table(at):
            row = pl.ds(HEAD + lax.div(at.start, HEAD), 1)
            c0, s0, c1, s1 = small[0, row, :], small[1, row, :], small[0, :HEAD, :], small[1, :HEAD, :]
            cos[at, :] = c0 * c1 - s0 * s1
            sin[at, :] = s0 * c1 + c0 * s1
        chunked(n * T, HEAD, table)
        begin(tables)
        end([keep, keep_dy])

        def work(u, units, x):
            H = T // 2
            places = [rows_of_unit(u, units, k, H) for k in BOTH]

            def run(c):
                r = dot(x[...], w[:, c]).astype(BF)
                for k, place in enumerate(places):
                    qkv[place, c] = r[k * H:(k + 1) * H]

            chunked(w.shape[1], 2 * HEAD, run)
            for place in places:
                for a in range(0, turned, HEAD):
                    qkv[place, a:a + HEAD] = turn(qkv[place, a:a + HEAD].astype(F32), cos[place, :], sin[place, :]).astype(BF)

        def turned_round(j):
            slot = lax.rem(j, 2)
            put = lambda j: pltpu.make_async_copy(wt.at[slot], wt_ref.at[:, block_rows(j, TILE)], so.at[1, slot])
            pl.when(j > 1)(lambda: put(j - 2).wait())
            wt[slot] = w[block_rows(j, TILE), :].T
            put(j).start()

        def near():
            of_a.passed_on(RA, LA)
            loop(D // TILE, turned_round)
            of_a.passed_on(RB, LB)
            of_a.start(RE, LE, MB, MC)
            of_dy.start(RA, LA, RB, LB, MA)

        stream(ring, of_a, a_all, tile, sb, None, None, None, work, gather_events(of_a, near))
        end([*tables, *[pltpu.make_async_copy(wt.at[k], wt_ref.at[:, upto(TILE)], so.at[1, k]) for k in BOTH]])

    pl.run_scoped(products, V((T, D), BF), V((D, turned + NK), BF), *[V((n * T, HEAD), F32)] * 2, V((2, turned + NK, TILE), BF))
    outs[0].start()
    set_gap(gap)

    def rest(wd):
        ring, _, of_dy, of_o = links()
        wd_in = pltpu.make_async_copy(wd_ref, wd, so.at[0, 0])
        wd_in.start()
        blocks = n * T // BQ

        def attention(iq):
            attend_block(iq, qkv, o, ot, lse, qs, top, mix, gap)
            steps(iq, {blocks - 2: lambda: of_dy.passed_on(RA, LA)})

        loop(blocks, attention)
        begin(outs[1:])
        of_dy.passed_on(RB, LB)
        of_dy.start(RE, LE, MB, MC)

        def product(shard, rows, then):
            at = pl.ds(pl.multiple_of(shard * T + rows.start, T // 2), rows.size)
            chunked(D, D // RUNS, lambda c: then(c, dot(o[at, :], wo[:, c])))

        scatter = Scatter(ring, of_o, product, stg, p, s, acc, tr, fr)
        scatter.send()
        wd_in.wait()

        def work(u, units, x, o):
            def run(c):
                o[:, c] = dot(x[...], wd[c, :], NT).astype(BF)
            chunked(wd.shape[0], 2 * HEAD, run)

        stream(ring, of_dy, dy_all, tile, sb, dhid, dt, so, work, gather_events(of_dy))
        of_o.sent(M3, M4)
        x_again.start()
        scatter.pass_on()
        end([x_again, *outs])

        def last(at, total):
            h = (stg[0, at, :].astype(F32) + total).astype(BF)
            s[0, at, :] = h
            h = h.astype(F32)
            stg[1, at, :] = (h * norm_scale(h)).astype(BF)

        scatter.finish(last, lambda k, at: [pltpu.make_async_copy(a.at[at], b.at[at], sl.at[2 * k + m]) for m, (a, b) in enumerate(((s.at[0], h_ref), (stg.at[1], b_ref)))])
        of_o.sent(R2, L2, R3, L3, R4, L4)

    pl.run_scoped(rest, V(wd_ref.shape, BF))


def front(x, dy, wq, wk, wv, wo, wd, n, cid):
    T, D = x.shape
    NQ, F, tokens = wo.shape[0], wd.shape[0], n * T
    N, cols = NQ + 2 * HEAD, NQ // HEAD * BQ
    stat = (tokens // BQ, 1, cols)
    table, row = S((tokens, HEAD), F32), S((T, D), BF)
    small = angles(jnp.concatenate([jnp.arange(HEAD), jnp.arange(0, tokens, HEAD)]))
    outs = [S((n, T, D), BF), S((tokens, N), BF), S((n, T, D), BF), S((n, T, F), BF), S((tokens, NQ), BF), S(stat, F32), table, table, row, row, S((N, D), BF), S((NQ, tokens), BF)]
    scratch = [V((2, T, D), BF), V((2, *small[0].shape), F32), V((tokens, N), BF), V((tokens, NQ), BF), V((NQ, tokens), BF),
               V(stat, F32), V((cols, HEAD), BF), V((1, cols), F32), V((HEAD + 8, cols), F32), V((BK, BQ), jnp.int32), V((NQ, D), BF), V((2, T, F), BF),
               *scatter_scratch(T, D), DMA((3 * COPIES,)), DMA((3 * COPIES,)), DMA((2, 3)), DMA((2, 3)), DMA((15,))]
    return call(functools.partial(_front, n=n), [x, dy, wq, wk, wv, wo, wd, *small], outs, scratch, 2 * tokens * D * (N + F + NQ), "front", cid)


def _back(t_ref, x_ref, wt_ref, a_ref, dh_all, heads_ref, b_ref, du_ref, dx_ref, by_q, by_k, by_v, by_o, by_up,
          w, t, heads, du, out, ft, stg, p, s, acc, tr, fr, ss, rs, sl, sf, sg, *, n):
    ring, links = Ring(n), Links(ss, rs)
    T, D = x_ref.shape
    NQ, NK = by_q.shape[1], by_k.shape[1]
    columns = [upto(NQ), pl.ds(NQ, NK), pl.ds(NQ + NK, NK)]
    pairs = ((t_ref, t), (wt_ref, w), (du_ref, du), (heads_ref, heads), (x_ref, stg.at[0]), (dh_all.at[ring.me], stg.at[1]))
    *first, du_in, heads_in, x_in, dh_in = [pltpu.make_async_copy(a, b, sl.at[k]) for k, (a, b) in enumerate(pairs)]
    begin(first)
    ring.barrier()
    end(first)
    begin([du_in, heads_in])
    late = lambda j: [(upto(du.shape[2]), by_up.at[block_rows(j - EARLY, TILE)])]
    fill = Fill((([b_ref], du, out, None, [late], EARLY, D // TILE),
                 ([a_ref], t, out, None, [lambda j: [(c, r.at[block_rows(j, TILE)]) for c, r in zip(columns, (by_q, by_k, by_v))]]),
                 ([dh_all], heads, out, NN, [lambda j: [(upto(TILE), by_o.at[:, block_rows(j, TILE)])]])), ft, sf, sg)
    fill.fetch(0)

    def product(shard, rows, then):
        chunked(D, D // RUNS, lambda c: then(c, dot(t[shard, rows, :], w[:, c])))

    scatter = Scatter(ring, links, product, stg, p, s, acc, tr, fr)
    scatter.send()
    end([du_in, heads_in])

    def rows_in():
        links.sent(M3, M4)
        begin([x_in, dh_in])
    def beside(k):
        fill.step(k)
        steps(k, [None, scatter.pass_on, rows_in])
    loop(fill.steps, beside)
    fill.finish()
    end([x_in, dh_in])

    def last(at, total):
        s[0, at, :] = (stg[1, at, :].astype(F32) + unnorm(stg[0, at, :].astype(F32), total)).astype(BF)

    scatter.finish(last, lambda k, at: [pltpu.make_async_copy(s.at[0, at], dx_ref.at[at], sl.at[k])])
    links.sent(R2, L2, R3, L3, R4, L4)


def back(dqkv, x, wt, ws, a, dh_all, heads, b, du, n, cid):
    T, D = x.shape
    K, NQ, F = dqkv.shape[2], heads.shape[0], du.shape[2]
    scratch = [V((K, D), BF), V(dqkv.shape, BF), V(heads.shape, BF), V(du.shape, BF), V((2, TILE, F), BF), V((2, n, T, TILE), BF), *scatter_scratch(T, D),
               DMA((COPIES,)), DMA((COPIES,)), DMA((8,)), DMA((2,)), DMA((2, 3))]
    outs = [S((T, D), BF), *(S(w.shape, BF) for w in ws), S((NQ, D), BF), S((D - EARLY * TILE, F), BF)]
    return call(functools.partial(_back, n=n), [dqkv, x, wt, a, dh_all, heads, b, du], outs, scratch, 6 * n * T * D * K, "back", cid)


def _land(*refs):
    m = (len(refs) - 2) // 3
    ins, outs, tiles, sem = refs[:m], refs[m + 1:2 * m + 1], refs[2 * m + 1:-1], refs[-1]
    outs = [*outs[:-1], outs[-1].at[pl.ds(EARLY * TILE, ins[-1].shape[0])]]
    come = [pltpu.make_async_copy(a, b, sem.at[k]) for k, (a, b) in enumerate(zip(ins, tiles))]
    go = [pltpu.make_async_copy(a, b, sem.at[k]) for k, (a, b) in enumerate(zip(tiles, outs))]
    begin(come)
    for a, b in zip(come, go):
        a.wait()
        b.start()
    end(go)


def land(arrays, whole):
    shapes = [S(t.shape, BF) for t in (*arrays[:-1], whole)]
    return call(_land, [*arrays, whole], shapes, [*(V(t.shape, BF) for t in arrays), DMA((len(arrays),))], 0, "land", aliases={len(arrays): len(arrays) - 1})


def mlp_links(b_ref, bg, frm, stg, s3, s1, p1, p3, tr, fr, ss, rs, n):
    ring, links = Ring(n), Links(ss, rs)
    T = b_ref.shape[0]
    H, Q = T // 2, T // 4
    first = upto(Q)
    frp, frn = fr.at[0], fr.at[1]
    nx, pv, mt = ring.next, ring.prev, ring.mate
    lo, hi = upto(H), pl.ds(H, H)
    gather_copies(links, ring, b_ref, bg, T, True)
    at = lambda ref: [ref.at[k] for k in range(ref.shape[0])]
    pa, pb, pc, pd, sa, sb1, sc, sd1, even, odd, on, off = [*at(p1), *at(s1), *at(stg), *at(tr)]
    for k, src, dst, to in ((M5, odd, frm, mt), (M0, odd.at[hi], pa, mt), (M1, even, p3, mt), (M2, even.at[hi], pb, mt), (M3, odd.at[hi], pc, mt), (M4, even.at[hi], pd, mt),
                            (R1, s3.at[lo], on, nx), (L1, s3.at[hi], off, pv),
                            (L2, sa.at[first], frn.at[first], pv), (L5, sb1.at[first], frn.at[pl.ds(Q, Q)], pv),
                            (R2, sa.at[pl.ds(Q, Q)], frp.at[pl.ds(H, Q)], nx), (R5, sb1.at[pl.ds(Q, Q)], frp.at[pl.ds(H + Q, Q)], nx),
                            (R3, sc.at[first], frp.at[first], nx), (R4, sd1.at[first], frp.at[pl.ds(Q, Q)], nx),
                            (L3, sc.at[pl.ds(Q, Q)], frn.at[pl.ds(H, Q)], pv), (L4, sd1.at[pl.ds(Q, Q)], frn.at[pl.ds(H + Q, Q)], pv)):
        links.put(k, src, dst, to)
    return ring, links


def pair_sum(acc, p1, s1, tr, k, base=0, first=None):
    H = s1.shape[1]

    def add(at, *further):
        v = acc[pl.ds(base + at.start, at.size), :] + p1[k, at, :].astype(F32)
        s1[k, at, :] = sum([tr[t].astype(F32) for t in further], v).astype(BF)

    if first is None:
        chunked(H, 16, add)
    else:
        for side in BOTH:
            chunked(H // 2, 16, lambda at: add(pl.ds(side * (H // 2) + at.start, at.size), (side, pl.ds(first + at.start, at.size))))


def _units(b_ref, dhid_ref, wg_ref, wu_ref, bg, hid, dgo, duo, own, frm, bt, acc, stg, s3, s1, p1, p3, tr, fr, ss, rs, sw, sb, sd, so, sl, n, wg, wu, dht, st):
    ring, links = mlp_links(b_ref, bg, frm, stg, s3, s1, p1, p3, tr, fr, ss, rs, n)
    T, D = b_ref.shape
    F = wg_ref.shape[1]
    H, NC, NB = T // 2, F // 3, D // 2
    me, nx, pv, mt = ring.me, ring.next, ring.prev, ring.mate
    Q0, Q1, Q2, Q3 = range(4)
    quarters = lambda *shards: tuple((shard, q) for shard in shards for q in range(4))
    pvm, nxm = ring.prevm, ring.nextm
    units = [quarters(me), ((pv, Q0), (nx, Q2), (pvm, Q0), (nxm, Q2)), ((pv, Q1), (nx, Q3), (pvm, Q1), (nxm, Q3)), quarters(ring.opp), quarters(ring.oppm),
             ((nx, Q0), (pv, Q2), (nxm, Q0), (pvm, Q2)), ((nx, Q1), (pv, Q3), (nxm, Q1), (pvm, Q3)), quarters(mt)]
    count = len(units)

    def fetch(u, slot):
        return moves(u, units, bg, bt.at[slot], sb.at[slot]) + moves(u, units, dhid_ref, dht.at[slot], sd.at[slot])

    def store(u):
        return [c for m, ref in enumerate((hid, dgo, duo)) for c in moves(u, units, ref, st.at[m], so.at[m], True)]

    def weights(j):
        s = block_rows(j, NC)
        return [pltpu.make_async_copy(a.at[:, s], b.at[:, s], sw.at[k, j]) for k, (a, b) in enumerate(((wg_ref, wg), (wu_ref, wu)))]

    pairs = ((b_ref, bt.at[0]), (dhid_ref.at[me], dht.at[0]), (bt.at[0], bg.at[me]), (acc, own))
    *first, keep, own_out = [pltpu.make_async_copy(a, b, sl.at[k]) for k, (a, b) in enumerate(pairs)]
    begin(first)
    for j in range(F // NC):
        begin(weights(j))
    ring.barrier()
    links.start(RA, LA, RB, LB, MA)
    end(first)
    keep.start()

    pair = functools.partial(pair_sum, acc, p1, s1, tr)

    def late0():
        links.passed_on(RA, LA)
        links.start(MB, MC)

    def post0():
        keep.wait()
        own_out.start()
        links.got(MB, MC)
        begin(fetch(1, 1))

    def mid1():
        own_out.wait()
        links.passed_on(RB)
        links.start(RE)
        links.passed_on(LB)
        links.start(LE, MH, MI)

    def late1():
        links.got(MH, MI)
        begin(fetch(2, 0))

    def mid2():
        links.got(M0)
        pair(0)
        links.start(L2, R2)

    def post2():
        links.start(M2)
        far()
        begin(fetch(3, 1))

    def mid3():
        links.got(M2)
        pair(1)
        links.start(L5, R5)

    def late3():
        links.got(MD, ME)
        begin(fetch(4, 0))
        links.sent(M2)

    def late4():
        links.got(MF, MG)
        begin(fetch(5, 1))

    def mid5():
        links.got(M1)

        def add(at):
            s3[at, :] = (acc[at, :] + p3[at, :].astype(F32)).astype(BF)
        chunked(T, 16, add)
        links.start(R1, L1)
        links.sent(M0)

    def late6():
        links.got(MA)
        begin(fetch(7, 1))

    def pairs_left():
        links.got(M3, R1, L1)
        pair(2, 0, 0)
        links.start(R3, L3)
        links.got(M4)
        pair(3, H, H // 2)
        links.start(R4, L4)

    def post7():
        links.start(M5)
        end(store(7))

    _, _, _, far, _, last, _ = gather_events(links)
    starting = lambda *ks: lambda: links.start(*ks)
    mids = [None, mid1, mid2, mid3, last, mid5, lambda: links.sent(M1), lambda: links.sent(M3)]
    lates = [late0, late1, None, late3, late4, lambda: begin(fetch(6, 0)), late6]
    posts = [post0, starting(M0), post2, None, starting(M1), starting(M3), starting(M4), post7]

    def forth_unit(u, slot):
        @pl.when(u > 0)
        def _():
            end(fetch(u, slot))
            end(store(u - 1))

        def forth(j):
            @pl.when(u == 0)
            def _():
                end(weights(j))
            s = block_rows(j, NC)
            x = bt[slot]
            gate, up = dot(x, wg[:, s]), dot(x, wu[:, s])
            d = dht[slot, :, s].astype(F32)
            sig = jax.nn.sigmoid(gate)
            act = gate * sig
            for m, v in enumerate((act * up, d * up * (sig + act * (1 - sig)), d * act)):
                st[m, :, s] = v.astype(BF)
            pl.when((u == count - 1) & (j == 0))(pairs_left)

        loop(F // NC, forth)
        begin(store(u))

    def unit(u):
        slot = lax.rem(u, 2)
        forth_unit(u, slot)
        steps(u, mids)
        among = lambda *us: functools.reduce(jnp.logical_or, [u == k for k in us])
        side = jnp.where(among(2, 4, 6), 0, 1)

        def back(c):
            v = dot(st[1], wg[c, :], NT) + dot(st[2], wu[c, :], NT)

            @pl.when(among(0, 3))
            def _():
                acc[:, c] = v

            @pl.when(among(4, 7))
            def _():
                stg[side, :, c] = v.astype(BF)

            @pl.when(among(1, 2, 5, 6))
            def _():
                acc[pl.ds(pl.multiple_of(jnp.where(u == 6, H, 0), H), H), c] = v[:H]
                stg[side, H:, c] = v[H:].astype(BF)

        def part(j):
            back(block_rows(j, NB))
            pl.when(j == 0)(lambda: steps(u, lates))

        loop(D // NB, part)
        steps(u, posts)

    loop(count, unit)


def _middle(b_ref, dhid_ref, wg_ref, wu_ref, h_ref, dy_ref, wo_ref, dy_all, bg, hid, dgo, duo, dh_all, out, by_down, by_gate, by_up, own, frm,
            bt, acc, stg, s3, s1, p1, p3, tr, fr, ot, ss, rs, sw, sb, sd, so, sl, sf, sg, *, n):
    T, D = b_ref.shape
    F, NQ = wg_ref.shape[1], wo_ref.shape[0]
    shared = (bt, acc, stg, s3, s1, p1, p3, tr, fr, ss, rs)
    pl.run_scoped(functools.partial(_units, b_ref, dhid_ref, wg_ref, wu_ref, bg, hid, dgo, duo, own, frm, *shared, sw, sb, sd, so, sl, n),
                  V((D, F), BF), V((D, F), BF), V((2, T, F), BF), V((3, T, F), BF))

    def rest(fixed, left, tile, wo):
        ring, links = mlp_links(b_ref, bg, frm, *shared[2:], n)
        of_dh = Links(ss, rs, COPIES)
        gather_copies(of_dh, ring, stg.at[0], dh_all, T)
        pairs = ((hid, fixed.at[1]), (dgo, fixed.at[0]), (duo, fixed.at[1]), (wo_ref, wo), (own, acc), (frm, bt.at[0]), (h_ref, bt.at[1]), (dy_ref, s3),
                 (stg.at[0], dh_all.at[ring.me]))
        hid_in, dg_in, du_in, wo_in, own_in, frm_in, *rows_in, keep = [pltpu.make_async_copy(a, b, sl.at[k]) for k, (a, b) in enumerate(pairs)]
        side = lambda ref: lambda j: [(upto(F), ref.at[block_rows(j, TILE)])]
        fill = Fill((([dy_all], fixed.at[1], left, TN, [lambda j: [(pl.ds(a, TILE), by_down.at[pl.ds(a, TILE), block_rows(j, TILE)]) for a in range(0, F, TILE)]]),
                     ([bg, bg], fixed, left, None, [side(by_gate), side(by_up)], 0, D // TILE + EARLY)), tile, sf, sg)
        hid_in.start()
        fill.fetch(0)
        own_in.start()
        links.sent(R1, L1)
        begin(rows_in)
        hid_in.wait()

        def mates_part():
            links.got(M5)
            frm_in.start()
            own_in.wait()
            add_rows(links, acc, (R2, R5), fr.at[0], T // 2)
            add_rows(links, acc, (L2, L5), fr.at[1], 0)

        def scattered():
            end([frm_in, *rows_in])
            links.sent(M4)

            def add(at):
                acc[at, :] += bt[0, at, :].astype(F32)
            chunked(T, 16, add)

            def last(at, total):
                stg[0, at, :] = (s3[at, :].astype(F32) + unnorm(bt[1, at, :].astype(F32), total)).astype(BF)

            finish(links, acc, fr, last)
            of_dh.start(RA, LA, RB, LB, MA)
            keep.start()

        def near():
            of_dh.passed_on(RB, LB)
            of_dh.start(RE, LE, MB, MC)

        def work(u, units, x, o):
            def run(c):
                o[:, c] = dot(x[...], wo[c, :], NT).astype(BF)
            chunked(NQ, 2 * HEAD, run)

        mate, _, mates, far, fars, last, lasts = gather_events(of_dh)
        events = {0: mates_part, 1: scattered, 3: lambda: begin([dg_in, wo_in]), 5: lambda: (mate(), end([keep, wo_in, dg_in]), of_dh.passed_on(RA, LA)),
                  7: du_in.start, 8: near, 10: mates, 13: far, 14: fars, 15: du_in.wait, fill.steps - 2: last, fill.steps - 1: lasts}
        schedule = (6, 7, 11, 12, 15, 16, fill.steps - 1, fill.steps)
        stream(ring, of_dh, dh_all, bt, sb, out, ot, sd, work, events, schedule, lambda k: pl.when(k < fill.steps)(lambda: fill.step(k)))
        fill.finish()
        links.sent(*GATHER, MH, MI, R2, R3, R4, R5, L2, L3, L4, L5, M5)

    pl.run_scoped(rest, V((2, n, T, F), BF), V((2, TILE, F), BF), V((2, n, T, TILE), BF), V((NQ, D), BF))


def middle(b, dhid, wg, wu, h, dy, wo, dy_all, n, cid):
    T, D = b.shape
    F, NQ = wg.shape[1], wo.shape[0]
    H = T // 2
    row, halves = V((T, D), BF), V((4, H, D), BF)
    scratch = [V((2, T, D), BF), V((T, D), F32), V((2, T, D), BF), row, halves, halves, row, V((2, H, D), BF), V((2, T, D), BF), V((2, T, NQ), BF),
               DMA((2 * COPIES,)), DMA((2 * COPIES,)), DMA((2, 3)), DMA((2, 4)), DMA((2, 4)), DMA((3, 4)), DMA((9,)), DMA((2,)), DMA((2, 3))]
    wide, full, narrow = S((n, T, F), BF), S((n, T, D), BF), S((D, F), BF)
    outs = [full, wide, wide, wide, full, S((n, T, NQ), BF), S((F, D), BF), narrow, narrow, S((T, D), F32), S((T, D), BF)]
    got = call(functools.partial(_middle, n=n), [b, dhid, wg, wu, h, dy, wo, dy_all], outs, scratch, 14 * n * T * D * F, "middle", cid)
    return got[4:9], got[0], got[3]


def solution(mesh):
    n = mesh.shape["tp"]

    def step(x, dy, wq, wk, wv, wo, wg, wu, wd):
        x, dy = x[0], dy[0]
        blocks = lambda t: t.reshape(n, -1, t.shape[1])
        a, qkv, dy_all, dhid, heads, lse, cos, sin, h, b, wt, heads_t = front(x, dy, wq, wk, wv, wo, wd, n, 0)
        (dh_all, d_heads, *by_mlp), b, du = middle(b, dhid, wg, wu, h, dy, wo, dy_all, n, 1)
        dqkv, by_down, by_gate, by_up = attend_bwd(qkv, flat(d_heads), heads, lse, cos, sin, by_mlp)
        dx, *by_qkvo, by_up = land(back(blocks(dqkv), x, wt, [wq, wk, wv], a, dh_all, heads_t, b, du, n, 2), by_up)
        return dx[None], *by_qkvo, by_gate, by_up, by_down

    states, by_columns, by_rows = P("dp", "tp", None), P(None, "tp"), P("tp", None)
    weights = (by_columns, by_columns, by_columns, by_rows, by_columns, by_columns, by_rows)
    own = tuple(P("dp", "tp") if spec == by_columns else P(("dp", "tp"), None) for spec in weights)
    return jax.shard_map(step, mesh=mesh, in_specs=(states, states, *weights), out_specs=(states, *own), check_vma=False)
```
